32 devices in a mesh: grp: 4 (over x, core), tile: 8 (over z, y).
Axes of the slice: x: 2, y: 2, z: 4, core: 2. Of those that a mesh axis runs over, the one named last changes fastest.
Arguments:
- flow_state: float32 [4, 4, 32, 2048], P('grp', None, 'tile'), may hold values from -6 to 6
- line_owner: int32 [8192, 1], replicated, may hold values from 0 to 7; in each aligned block of 8192 rows (0 to 8191, 8192 to 16383, ...) at most 2048 rows name the same one
Outputs:
- record: float32 [4, 8, 32, 2048], P('grp', 'tile')
The draws below stay inside these ranges and needn't reach their ends.
Inputs may be any that keep to these rules, and one draw needn't show every extreme that they name: `line_owner`: no pencil owns more than 2048 lines, some pencil owns exactly 2048, and every pencil owns at least one line.
All inputs are finite; a program needn't handle non-finite values.
Results may differ from the reference program's by a relative error of at most 0.00002.
Values sent between devices are 32-bit elements; how exact they have to be, the bound alone decides.
A program may use at most 64 MiB of HBM per device.

```python
import math
import jax
import jax.numpy as jnp
import numpy as np
from jax import lax

NY = 2048
PLANES = 4
NX = 32
NL = 8192
CAP = 2048
N_GRP = 4
N_TILE = 8


def steps_of(rng, shape, shards, least, largest):
    loudness, own = 1.0, jax.random.fold_in(rng, 6)
    for dim, parts in shards:
        steps = jnp.exp(jax.random.uniform(jax.random.fold_in(own, dim), (parts,), jnp.float32, least / len(shards), largest / len(shards)))
        loudness = loudness * jnp.repeat(steps, shape[dim] // parts).reshape([-1 if axis == dim else 1 for axis in range(len(shape))])
    return loudness


def assign_block(rng, own, number, rows, amount, top, limit, skew):
    ranking = jax.random.permutation(rng, amount)
    crowded, ordinary = portions_of(amount, rows * top, limit, skew, True), portions_of(amount, rows * top, limit, skew, False)
    places = jnp.arange(amount)

    def named(tallies, offset_by):
        used = int((tallies > 0).sum())
        fixed = max(1, used // 4)
        moved = fixed + (places - fixed + offset_by * (used - fixed)) % max(1, amount - fixed)
        return jnp.zeros((amount,), jnp.int32).at[ranking[jnp.where(places < fixed, places, moved)]].set(jnp.asarray(tallies, jnp.int32))

    tallies = jnp.where(number % 4 == 0, named(crowded, number // 4), named(ordinary, number - number // 4 - 1))
    mixed = jax.random.permutation(jax.random.fold_in(own, 3), amount)
    giver, receiver = mixed[0:amount // 2 * 2:2], mixed[1:amount // 2 * 2:2]
    room = jnp.minimum(tallies[giver] - 1, limit - tallies[receiver]) // 2
    room = jnp.where((giver == ranking[0]) | (receiver == ranking[0]) | (tallies[receiver] == 0), 0, jnp.maximum(room, 0))
    moved = jax.random.randint(jax.random.fold_in(own, 4), (amount // 2,), 0, 1 << 20) % (room + 1)
    tallies = tallies.at[giver].add(-moved).at[receiver].add(moved)
    labels = jnp.searchsorted(jnp.cumsum(tallies), jnp.arange(rows * top), side="right").astype(jnp.int32)
    listing = labels.reshape(top, rows).T
    listing = listing[jax.random.permutation(jax.random.fold_in(own, 1), rows)]
    offset_by = jax.random.randint(jax.random.fold_in(own, 2), (rows, 1), 0, top)
    return jnp.take_along_axis(listing, (jnp.arange(top)[None, :] + offset_by) % top, axis=1)


def portions_of(count, total, bound, lean, full):
    loads = [(1 << 20) // math.isqrt(grade ** lean) + 1 for grade in range(1, count + 1)]
    largest = bound if full else min(bound, max(-(-total // count), total * loads[0] // sum(loads)))
    least = 1 if total - largest >= count - 1 else 0
    holding, rest = [largest] + [least] * (count - 1), total - largest - least * (count - 1)
    while rest > 0:
        movable = [i for i in range(1, count) if holding[i] < largest] or [i for i in range(1, count) if holding[i] < bound]
        pool, remaining = sum([loads[i] for i in movable]), rest
        for i in movable:
            addition = min(bound - holding[i], max(1, remaining * loads[i] // pool), rest)
            holding[i] = holding[i] + addition
            rest = rest - addition
    return np.array(holding)


def centred(key, dims, scale, reach, pieces=(), kind=jnp.bfloat16):
    factor_of = steps_of(key, dims, pieces, -0.22, 0.18) if pieces else 1.0
    array = jax.random.normal(key, dims, jnp.float32) * scale * factor_of
    return jnp.minimum(jnp.maximum(array, -reach), reach).astype(kind)


def setup_inputs(seed: int = 0) -> dict:
    key_list = jax.random.split(jax.random.key(seed), 3)
    flow_state = centred(key_list[0], (N_GRP, PLANES, NX, NY), 1.0, 6.0, ((0, 4), (2, 8)), jnp.float32)
    line_owner_keys = jax.random.split(jax.random.fold_in(key_list[1], 1), NL // NL)
    line_owner_turns = jax.random.permutation(jax.random.fold_in(key_list[1], 3), NL // NL)
    line_owner = jax.vmap(lambda own, number: assign_block(jax.random.fold_in(key_list[1], 2), own, number, NL, N_TILE, 1, CAP, 2))(line_owner_keys, line_owner_turns).reshape((NL, 1))
    return {"flow_state": flow_state, "line_owner": line_owner}


time_step = 0.2
viscosity = 0.05
first_coeffs = (0.8, -0.2, 4.0 / 105.0, -1.0 / 280.0)
second_center = -205.0 / 72.0
second_coeffs = (1.6, -0.2, 8.0 / 315.0, -1.0 / 560.0)
lift_alpha = -1.586134342059924
lift_beta = -0.052980118572961
lift_gamma = 0.882911075530934
lift_delta = 0.443506852043971
lift_scale = 1.149604398860241


def first_rolled(field_now, along_axis):
    running = jnp.zeros_like(field_now)
    for offset in range(4):
        forward = jnp.roll(field_now, -(offset + 1), along_axis)
        behind = jnp.roll(field_now, offset + 1, along_axis)
        running = running + first_coeffs[offset] * (forward - behind)
    return running


def second_rolled(field_now, along_axis):
    running = second_center * field_now
    for offset in range(4):
        forward = jnp.roll(field_now, -(offset + 1), along_axis)
        behind = jnp.roll(field_now, offset + 1, along_axis)
        running = running + second_coeffs[offset] * (forward + behind)
    return running


def tendencies(fields):
    pressure = fields[3]
    grad_axes = (1, 2, 0)
    result = []
    for component in range(3):
        field_now = fields[component]
        advect = fields[0] * first_rolled(field_now, 1) + fields[1] * first_rolled(field_now, 2) + fields[2] * first_rolled(field_now, 0)
        laplace = second_rolled(field_now, 1) + second_rolled(field_now, 2) + second_rolled(field_now, 0)
        result.append(-advect - first_rolled(pressure, grad_axes[component]) + viscosity * laplace)
    return jnp.stack(result)


def lift_axis(signal, along_axis):
    length = signal.shape[along_axis]
    even_part = lax.slice_in_dim(signal, 0, length, 2, along_axis)
    odd_part = lax.slice_in_dim(signal, 1, length, 2, along_axis)
    odd_part = odd_part + lift_alpha * (even_part + jnp.roll(even_part, -1, along_axis))
    even_part = even_part + lift_beta * (odd_part + jnp.roll(odd_part, 1, along_axis))
    odd_part = odd_part + lift_gamma * (even_part + jnp.roll(even_part, -1, along_axis))
    even_part = even_part + lift_delta * (odd_part + jnp.roll(odd_part, 1, along_axis))
    return jnp.concatenate([even_part * lift_scale, odd_part / lift_scale], along_axis)


def line_slots(line_owner, pencils, capacity):
    owners = line_owner[:, 0].astype(jnp.int32)
    sorted_lines = jnp.argsort(owners, stable=True).astype(jnp.int32)
    sorted_owner = owners[sorted_lines]
    targets = jnp.arange(pencils, dtype=jnp.int32)
    starts = jnp.searchsorted(sorted_owner, targets, side="left").astype(jnp.int32)
    ends_at = jnp.searchsorted(sorted_owner, targets, side="right").astype(jnp.int32)
    counts = ends_at - starts
    slot_index = jnp.arange(capacity, dtype=jnp.int32)
    position = jnp.minimum(starts[:, None] + slot_index[None, :], owners.shape[0] - 1)
    chosen = sorted_lines[position]
    usable = slot_index[None, :] < counts[:, None]
    return chosen, usable


def reference(flow_state, line_owner):
    velocity = flow_state[:3]
    pressure = flow_state[3:]
    middle = velocity + time_step * tendencies(flow_state)
    finished = 0.5 * ((velocity + middle) + time_step * tendencies(jnp.concatenate([middle, pressure], 0)))
    coeffs = lift_axis(lift_axis(lift_axis(finished, 3), 1), 2)
    planes = coeffs.shape[1]
    line_table = jnp.transpose(coeffs, (0, 1, 3, 2)).reshape(3, planes * coeffs.shape[3], coeffs.shape[2])
    chosen, usable = line_slots(line_owner, N_TILE, CAP)
    picked = jnp.take(line_table, chosen.reshape(-1), axis=1).reshape(3, N_TILE, CAP, line_table.shape[2])
    picked = jnp.where(usable[None, :, :, None], picked, 0.0)
    record = jnp.transpose(picked, (0, 1, 3, 2))
    energy = record[0] * record[0] + record[1] * record[1] + record[2] * record[2]
    return jnp.concatenate([record, energy[None]], 0)
```

```python
import functools

import jax
import jax.numpy as jnp
import numpy as np
from jax import lax
from jax.experimental import pallas as pl
from jax.experimental.pallas import tpu as pltpu
from jax.sharding import PartitionSpec as P

time_step = 0.2
viscosity = 0.05
reach = 4
first_coeffs = (0.8, -0.2, 4.0 / 105.0, -1.0 / 280.0)
second_center = -205.0 / 72.0
second_coeffs = (1.6, -0.2, 8.0 / 315.0, -1.0 / 560.0)
lift_alpha = -1.586134342059924
lift_beta = -0.052980118572961
lift_gamma = 0.882911075530934
lift_delta = 0.443506852043971
lift_scale = 1.149604398860241
LANES = 128
MESH = pl.DeviceIdType.MESH


def lift_numpy(signal):
    even, odd = signal[0::2].copy(), signal[1::2].copy()
    odd += lift_alpha * (even + np.roll(even, -1, 0))
    even += lift_beta * (odd + np.roll(odd, 1, 0))
    odd += lift_gamma * (even + np.roll(even, -1, 0))
    even += lift_delta * (odd + np.roll(odd, 1, 0))
    return np.concatenate([even * lift_scale, odd / lift_scale])


def lift_matrix(length):
    return lift_numpy(np.eye(length))


def band_matrix():
    full = lift_matrix(8 * LANES)
    low = full[LANES : 2 * LANES, LANES : 5 * LANES]
    high = full[4 * LANES + LANES : 4 * LANES + 2 * LANES, LANES : 5 * LANES]
    return np.concatenate([low, high]).T.astype(np.float32)


def band_value(taps_low, taps_high):
    row = lax.broadcasted_iota(jnp.int32, (4 * LANES, 2 * LANES), 0)
    column = lax.broadcasted_iota(jnp.int32, (4 * LANES, 2 * LANES), 1)
    distance = row - LANES - 2 * (column & (LANES - 1))
    is_low = column < LANES
    value = jnp.zeros((4 * LANES, 2 * LANES), jnp.float32)
    for offset in range(-4, 5):
        tap = jnp.where(is_low, taps_low[offset + 4], taps_high[offset + 4])
        value = jnp.where(distance == offset, tap, value)
    return value


def band_taps():
    band = band_matrix()
    rows = slice(LANES + LANES // 2 - 4, LANES + LANES // 2 + 5)
    return [float(x) for x in band[rows, LANES // 4]], [float(x) for x in band[rows, LANES + LANES // 4]]


def shifted_y(value, k):
    return pltpu.roll(value, (-k) % value.shape[-1], value.ndim - 1)


def derivatives(center, shift, want_first=True, want_second=True):
    first, second = None, second_center * center if want_second else None
    for k in range(1, reach + 1):
        ahead, behind = shift(k), shift(-k)
        if want_first:
            term = first_coeffs[k - 1] * (ahead - behind)
            first = term if first is None else first + term
        if want_second:
            second = second + second_coeffs[k - 1] * (ahead + behind)
    return first, second


def slots_of(n_tile, owner_ref, place_ref, base_ref, count_ref):
    owner = owner_ref[...]
    n_blocks = owner.shape[0]
    upper = (lax.broadcasted_iota(jnp.int32, (LANES, LANES), 0) <= lax.broadcasted_iota(jnp.int32, (LANES, LANES), 1)).astype(jnp.float32)
    lower = (lax.broadcasted_iota(jnp.int32, (n_blocks, n_blocks), 0) > lax.broadcasted_iota(jnp.int32, (n_blocks, n_blocks), 1)).astype(jnp.float32)
    lane = lax.broadcasted_iota(jnp.int32, (n_blocks, LANES), 1)

    def step(s, carry):
        place, counts, ahead = carry
        mask = (owner == s).astype(jnp.float32)
        within = jnp.dot(mask, upper, preferred_element_type=jnp.float32)
        total = jnp.sum(mask, axis=1, keepdims=True)
        place = place + mask * (ahead + within - 1.0)
        counts = jnp.where(lane == s, total, counts)
        return place, counts, ahead + total

    zeros = jnp.zeros((n_blocks, LANES), jnp.float32)
    carry = (zeros, zeros, jnp.zeros((n_blocks, 1), jnp.float32))
    if n_tile <= 16:
        for s in range(n_tile):
            carry = step(s, carry)
    else:
        carry = lax.fori_loop(0, n_tile, step, carry)
    place, counts, _ = carry
    place_ref[...] = place
    count_ref[...] = counts.astype(jnp.int32)
    base_ref[...] = jnp.dot(lower, counts, preferred_element_type=jnp.float32).astype(jnp.int32)


def flow_kernel(n_tile, own_ref, owner_ref, out_ref, place_ref, base_ref, count_ref,
                fields, mids, halo, mid_halo, pad, ppad, middle, fin, along_y, along_z, lap, send_sem, recv_sem, hsend_sem, hrecv_sem, msend_sem, mrecv_sem, mhsend_sem, mhrecv_sem, relay_sem, band_ref):
    g, t = lax.axis_index("grp"), lax.axis_index("tile")
    right, left = lax.rem(t + 1, n_tile), lax.rem(t + n_tile - 1, n_tile)
    planes, rows, ny = own_ref.shape[1:]
    own = own_ref.at[0]

    barrier = pltpu.get_barrier_semaphore()
    for k in range(1, 4):
        pl.semaphore_signal(barrier, inc=1, device_id=(lax.rem(g + k, 4), t), device_id_type=MESH)
    for side in (right, left):
        pl.semaphore_signal(barrier, inc=1, device_id=(g, side), device_id_type=MESH)

    @pl.when((g == 0) | (g == 3))
    def _():
        for side in (right, left):
            pl.semaphore_signal(barrier, inc=1, device_id=(3 - g, side), device_id_type=MESH)
        pl.semaphore_wait(barrier, 7)

    @pl.when((g == 1) | (g == 2))
    def _():
        pl.semaphore_wait(barrier, 5)

    def gather_copy(src, dst, ssem, rsem, k, slot):
        return pltpu.make_async_remote_copy(
            src_ref=src, dst_ref=dst.at[slot], send_sem=ssem.at[k], recv_sem=rsem.at[slot],
            device_id=(k, t), device_id_type=MESH)

    half = planes // 2

    def whole_copy(k, slot):
        return pltpu.make_async_remote_copy(
            src_ref=own, dst_ref=fields.at[slot], send_sem=send_sem.at[k], recv_sem=recv_sem.at[slot, 0],
            device_id=(k, t), device_id_type=MESH)

    def half_copy(slot, k):
        part = pl.ds(k * half, half)
        return pltpu.make_async_remote_copy(
            src_ref=own.at[part], dst_ref=fields.at[slot, part], send_sem=send_sem.at[k],
            recv_sem=recv_sem.at[slot, k], device_id=(k, t), device_id_type=MESH)

    def relay_copy(slot, k):
        part = pl.ds(k * half, half)
        return pltpu.make_async_remote_copy(
            src_ref=fields.at[slot, part], dst_ref=fields.at[slot, part], send_sem=relay_sem.at[slot],
            recv_sem=recv_sem.at[slot, k], device_id=(1 - k, t), device_id_type=MESH)

    def halo_copy(src, dst, ssem, rsem, side, slot, group):
        return pltpu.make_async_remote_copy(
            src_ref=src, dst_ref=dst.at[slot + side], send_sem=ssem.at[side], recv_sem=rsem.at[slot + side],
            device_id=(group, right if side == 0 else left), device_id_type=MESH)

    @pl.when(g < 3)
    def _():
        for side in range(2):
            halo_copy(own, halo, hsend_sem, hrecv_sem, side, 0, g).start()

    for k in range(3):
        @pl.when((g < 2) & (g != k))
        def _(k=k):
            whole_copy(k, g).start()

    @pl.when(g >= 2)
    def _():
        for k in range(2):
            half_copy(g, k).start()

    @pl.when(g == 3)
    def _():
        whole_copy(2, 3).start()
        for side in range(2):
            halo_copy(own, halo, hsend_sem, hrecv_sem, side, 2, 0).start()

    def local_terms():
        for z in range(planes):
            center = pad[z, reach : reach + rows]
            fy, sy = derivatives(center, lambda k: shifted_y(center, k))
            fz, sz = derivatives(center, lambda k: pad[(z + k) % planes, reach : reach + rows])
            along_y[z], along_z[z], lap[z] = fy, fz, sy + sz

    slots_of(n_tile, owner_ref, place_ref, base_ref, count_ref)
    band_ref[...] = band_value(*band_taps())

    @pl.when(g < 3)
    def _():
        for k in range(3):
            @pl.when(g == k)
            def _(k=k):
                fields[k] = own_ref[0]

        for z in range(planes):
            pad[z, reach : reach + rows] = own_ref[0, z]
        local_terms()

        @pl.when(g < 2)
        def _():
            for slot in (2, 3):
                half_copy(slot, g).wait_recv()
                relay_copy(slot, g).start()
            whole_copy(0, 1 - g).wait_recv()
            for slot in (2, 3):
                half_copy(slot, 1 - g).wait_recv()

        @pl.when(g == 2)
        def _():
            for slot in (0, 1, 3):
                whole_copy(0, slot).wait_recv()

        for side in range(2):
            halo_copy(own, halo, hsend_sem, hrecv_sem, side, 0, g).wait_recv()

        @pl.when(g == 0)
        def _():
            for side in range(2):
                halo_copy(own, halo, hsend_sem, hrecv_sem, side, 2, 0).wait_recv()
            for z in range(planes):
                ppad[z, 0:reach] = halo[2, z, rows - reach : rows]
                ppad[z, reach : reach + rows] = fields[3, z]
                ppad[z, reach + rows : 2 * reach + rows] = halo[3, z, 0:reach]
            for z in range(planes):
                middle[z], _ = derivatives(None, lambda k: ppad[z, reach + k : reach + k + rows], True, False)

        @pl.when(g == 1)
        def _():
            for z in range(planes):
                value = fields[3, z]
                middle[z], _ = derivatives(None, lambda k: shifted_y(value, k), True, False)

        @pl.when(g == 2)
        def _():
            for z in range(planes):
                middle[z], _ = derivatives(None, lambda k: fields[3, (z + k) % planes], True, False)

        def tendency(z, vel, press):
            center = pad[z, reach : reach + rows]
            fx, sx = derivatives(center, lambda k: pad[z, reach + k : reach + k + rows])
            advect = vel[0, z] * fx + vel[1, z] * along_y[z] + vel[2, z] * along_z[z]
            return viscosity * (sx + lap[z]) - advect - press

        for z in range(planes):
            pad[z, 0:reach] = halo[0, z, rows - reach : rows]
            pad[z, reach + rows : 2 * reach + rows] = halo[1, z, 0:reach]
        for z in range(planes):
            press = middle[z]
            ppad[z, 0:rows] = press
        for z in range(planes):
            middle[z] = own_ref[0, z] + time_step * tendency(z, fields, ppad[z, 0:rows])

        for side in range(2):
            halo_copy(middle, mid_halo, mhsend_sem, mhrecv_sem, side, 0, g).start()
        for k in range(3):
            @pl.when(g != k)
            def _(k=k):
                gather_copy(middle, mids, msend_sem, mrecv_sem, k, g).start()

            @pl.when(g == k)
            def _(k=k):
                mids[k] = middle[...]

        for z in range(planes):
            pad[z, reach : reach + rows] = middle[z]
        local_terms()
        for k in range(3):
            @pl.when(g != k)
            def _(k=k):
                gather_copy(middle, mids, msend_sem, mrecv_sem, 0, k).wait_recv()
        for side in range(2):
            halo_copy(middle, mid_halo, mhsend_sem, mhrecv_sem, side, 0, g).wait_recv()
        for z in range(planes):
            pad[z, 0:reach] = mid_halo[0, z, rows - reach : rows]
            pad[z, reach + rows : 2 * reach + rows] = mid_halo[1, z, 0:reach]
        for z in range(planes):
            fin[z] = 0.5 * ((own_ref[0, z] + middle[z]) + time_step * tendency(z, mids, ppad[z, 0:rows]))

        blocks = ny // (2 * LANES)
        groups = ny // LANES
        for z in range(planes):
            value = fin[z]
            pieces = []
            for b in range(blocks):
                window = [value[:, ((2 * b + j) % groups) * LANES : ((2 * b + j) % groups + 1) * LANES] for j in (-1, 0, 1, 2)]
                pieces.append(jnp.concatenate(window, axis=1))
            stacked = jnp.concatenate(pieces, axis=0)
            lifted = jnp.dot(stacked, band_ref[...], precision=lax.Precision.HIGHEST, preferred_element_type=jnp.float32)
            for b in range(blocks):
                piece = lifted[b * rows : (b + 1) * rows]
                fin[z, :, b * LANES : (b + 1) * LANES] = piece[:, 0:LANES]
                fin[z, :, ny // 2 + b * LANES : ny // 2 + (b + 1) * LANES] = piece[:, LANES:]

        even = [fin[2 * i] for i in range(half)]
        odd = [fin[2 * i + 1] for i in range(half)]
        odd = [odd[i] + lift_alpha * (even[i] + even[(i + 1) % half]) for i in range(half)]
        even = [even[i] + lift_beta * (odd[i] + odd[(i - 1) % half]) for i in range(half)]
        odd = [odd[i] + lift_gamma * (even[i] + even[(i + 1) % half]) for i in range(half)]
        even = [even[i] + lift_delta * (odd[i] + odd[(i - 1) % half]) for i in range(half)]
        for i in range(half):
            out_ref[i] = even[i] * lift_scale
            out_ref[half + i] = odd[i] * (1.0 / lift_scale)

        for side in range(2):
            halo_copy(middle, mid_halo, mhsend_sem, mhrecv_sem, side, 0, g).wait_send()
        for k in range(3):
            @pl.when(g != k)
            def _(k=k):
                gather_copy(middle, mids, msend_sem, mrecv_sem, k, g).wait_send()

    @pl.when(g == 3)
    def _():
        out_ref[...] = jnp.zeros_like(out_ref)

    for side in range(2):
        halo_copy(own, halo, hsend_sem, hrecv_sem, side, 0, g).wait_send()
    for k in range(3):
        @pl.when((g < 2) & (g != k))
        def _(k=k):
            whole_copy(k, g).wait_send()

    @pl.when(g < 2)
    def _():
        for slot in (2, 3):
            relay_copy(slot, g).wait_send()

    @pl.when(g >= 2)
    def _():
        for k in range(2):
            half_copy(g, k).wait_send()

    @pl.when(g == 3)
    def _():
        whole_copy(2, 3).wait_send()


def compact_kernel(n_tile, base_ref, count_ref, coeff_ref, place_ref, out_ref, current):
    planes, rows, ny = coeff_ref.shape
    groups = ny // LANES
    out_ref[...] = jnp.zeros_like(out_ref)
    current[...] = jnp.zeros_like(current)
    rank = lax.broadcasted_iota(jnp.int32, (LANES, LANES), 0).astype(jnp.float32)
    lane = lax.broadcasted_iota(jnp.int32, (rows, LANES), 1)

    def sort(b):
        z, y = b // groups, b % groups
        value = coeff_ref[z, :, pl.ds(pl.multiple_of(y * LANES, LANES), LANES)]
        high = value.astype(jnp.bfloat16).astype(jnp.float32)
        rest = value - high
        mid = rest.astype(jnp.bfloat16).astype(jnp.float32)
        low = rest - mid
        parts = jnp.concatenate([high, mid, low], axis=0).astype(jnp.bfloat16)
        chosen = jnp.where(rank == place_ref[pl.ds(b, 1), :], 1.0, 0.0).astype(jnp.bfloat16)
        ordered = lax.dot_general(parts, chosen, (((1,), (1,)), ((), ())), preferred_element_type=jnp.float32)
        return (ordered[0:rows] + ordered[rows : 2 * rows]) + ordered[2 * rows : 3 * rows]

    def pencil(b, ordered, s, ahead):
        base, count = base_ref[b, s], count_ref[b, s]
        start = base & (LANES - 1)
        end = start + count
        turned = pltpu.roll(ordered, (start - ahead) & (LANES - 1), 1)
        now = current[s] + jnp.where((lane >= start) & (lane < end), turned, 0.0)
        group = pl.multiple_of(base - start, LANES)
        after = jnp.where(lane < end - LANES, turned, 0.0)
        current[s] = jnp.where(end >= LANES, after, now)
        out_ref[s, :, pl.ds(group, 2 * LANES)] = jnp.concatenate([now, after], axis=1)
        return ahead + count

    n_blocks = planes * groups
    batch = 8 if n_blocks % 8 == 0 and n_tile <= 16 else 1

    def blocks(i, _):
        ordered = [sort(i * batch + j) for j in range(batch)]
        for j in range(batch):
            b = i * batch + j
            if n_tile <= 16:
                ahead = jnp.int32(0)
                for s in range(n_tile):
                    ahead = pencil(b, ordered[j], s, ahead)
            else:
                lax.fori_loop(0, n_tile, lambda s, ahead: pencil(b, ordered[j], s, ahead), jnp.int32(0))
        return 0

    lax.fori_loop(0, n_blocks // batch, blocks, 0)


def record_kernel(n_tile, chunks, sent_ref, matrix_ref, out_ref, got, records, send_sem, recv_sem, rsend_sem, rrecv_sem):
    g, t = lax.axis_index("grp"), lax.axis_index("tile")
    rows, nx, cap = sent_ref.shape[1], out_ref.shape[0], out_ref.shape[1]
    width = cap // chunks

    barrier = pltpu.get_barrier_semaphore()

    @pl.when(g < 3)
    def _():
        for k in range(1, n_tile):
            pl.semaphore_signal(barrier, inc=1, device_id=(g, lax.rem(t + k, n_tile)), device_id_type=MESH)
        pl.semaphore_signal(barrier, inc=1, device_id=(3, t), device_id_type=MESH)
        pl.semaphore_wait(barrier, n_tile)

    @pl.when(g == 3)
    def _():
        for k in range(3):
            pl.semaphore_signal(barrier, inc=1, device_id=(k, t), device_id_type=MESH)
        pl.semaphore_wait(barrier, 3)

    def exchange(s, slot, c):
        part = pl.ds(c * width, width)
        return pltpu.make_async_remote_copy(
            src_ref=sent_ref.at[s, :, part], dst_ref=got.at[slot, :, part], send_sem=send_sem.at[s, c],
            recv_sem=recv_sem.at[slot, c], device_id=(g, s), device_id_type=MESH)

    def report(c, slot):
        part = pl.ds(c * width, width)
        return pltpu.make_async_remote_copy(
            src_ref=out_ref.at[:, part], dst_ref=records.at[slot, :, part], send_sem=rsend_sem.at[c],
            recv_sem=rrecv_sem.at[slot, c], device_id=(3, t), device_id_type=MESH)

    @pl.when(g < 3)
    def _():
        for c in range(chunks):
            for k in range(1, n_tile):
                exchange(lax.rem(t + k, n_tile), t, c).start()
        got[t] = sent_ref[t, :, 0:cap]
        matrix = matrix_ref[...]
        for c in range(chunks):
            for k in range(1, n_tile):
                exchange(lax.rem(t + k, n_tile), lax.rem(t + k, n_tile), c).wait_recv()
            value = got[:, :, c * width : (c + 1) * width].reshape(nx, width)
            out_ref[:, c * width : (c + 1) * width] = jnp.dot(
                matrix, value, precision=lax.Precision.HIGHEST, preferred_element_type=jnp.float32)
            report(c, g).start()
        for c in range(chunks):
            for k in range(1, n_tile):
                exchange(lax.rem(t + k, n_tile), t, c).wait_send()
            report(c, g).wait_send()

    @pl.when(g == 3)
    def _():
        for c in range(chunks):
            for k in range(3):
                report(c, k).wait_recv()
            part = slice(c * width, (c + 1) * width)
            first, second, third = records[0, :, part], records[1, :, part], records[2, :, part]
            out_ref[:, part] = first * first + second * second + third * third


def tiled_body(flow_state, line_owner, *, n_tile):
    _, planes, rows, ny = flow_state.shape
    n_lines = line_owner.shape[0]
    n_blocks = n_lines // LANES
    nx = rows * n_tile
    cap = 2 * planes * ny // n_tile
    vmem = pl.BlockSpec(memory_space=pltpu.VMEM)
    smem = pl.BlockSpec(memory_space=pltpu.SMEM)
    f32 = jnp.float32
    shape = jax.ShapeDtypeStruct
    limit = 16 * 1024 * 1024
    dma = pltpu.SemaphoreType.DMA
    owner = line_owner.reshape(n_blocks, LANES)
    tile = (planes, rows, ny)
    ints = shape((n_blocks, LANES), jnp.int32)
    coeffs, place, base, count = pl.pallas_call(
        functools.partial(flow_kernel, n_tile),
        out_shape=(shape(tile, f32), shape((n_blocks, LANES), f32), ints, ints),
        in_specs=[vmem, vmem], out_specs=(vmem, vmem, vmem, vmem),
        scratch_shapes=[
            pltpu.VMEM((4,) + tile, f32), pltpu.VMEM((3,) + tile, f32),
            pltpu.VMEM((4,) + tile, f32), pltpu.VMEM((2,) + tile, f32),
            pltpu.VMEM((planes, rows + 2 * reach, ny), f32), pltpu.VMEM((planes, rows + 2 * reach, ny), f32),
            pltpu.VMEM(tile, f32), pltpu.VMEM(tile, f32), pltpu.VMEM(tile, f32), pltpu.VMEM(tile, f32), pltpu.VMEM(tile, f32),
            dma((4,)), dma((4, 2)), dma((2,)), dma((4,)), dma((4,)), dma((4,)), dma((2,)), dma((2,)), dma((4,)),
            pltpu.VMEM((4 * LANES, 2 * LANES), f32),
        ],
        compiler_params=pltpu.CompilerParams(has_side_effects=True, collective_id=0, vmem_limit_bytes=limit), name="flow",
    )(flow_state, owner)
    sent = pl.pallas_call(
        functools.partial(compact_kernel, n_tile),
        out_shape=shape((n_tile, rows, cap + 2 * LANES), f32),
        in_specs=[smem, smem, vmem, vmem], out_specs=vmem,
        scratch_shapes=[pltpu.VMEM((n_tile, rows, LANES), f32)],
        compiler_params=pltpu.CompilerParams(vmem_limit_bytes=limit), name="compact",
    )(base, count, coeffs, place)
    chunks = 4 if cap % (4 * LANES) == 0 else 1
    record = pl.pallas_call(
        functools.partial(record_kernel, n_tile, chunks),
        out_shape=shape((nx, cap), f32),
        in_specs=[vmem, vmem], out_specs=vmem,
        scratch_shapes=[
            pltpu.VMEM((n_tile, rows, cap), f32), pltpu.VMEM((3, nx, cap), f32),
            dma((n_tile, chunks)), dma((n_tile, chunks)), dma((chunks,)), dma((3, chunks)),
        ],
        compiler_params=pltpu.CompilerParams(has_side_effects=True, collective_id=1, vmem_limit_bytes=limit), name="record",
    )(sent, jnp.asarray(lift_matrix(nx).astype(np.float32)))
    return record[None, None]


CHUNK = 64
SIDE = (LANES - CHUNK) // 2
SUB = 8


def planes_taps(planes):
    first, second = [0.0] * planes, [0.0] * planes
    second[0] = 3.0 * second_center
    for k in range(1, reach + 1):
        first[k % planes] += first_coeffs[k - 1]
        first[-k % planes] -= first_coeffs[k - 1]
        second[k % planes] += second_coeffs[k - 1]
        second[-k % planes] += second_coeffs[k - 1]
    return first, second


def column_taps():
    full = lift_matrix(8 * CHUNK)
    middle = 4 * CHUNK
    low = full[middle // 2, middle - 4 : middle + 5]
    high = full[8 * CHUNK // 2 + middle // 2, middle + 1 - 4 : middle + 1 + 5]
    return [float(x) for x in low], [float(x) for x in high]


def column_band(planes):
    taps_low, taps_high = column_taps()
    part = CHUNK // 2
    row = lax.broadcasted_iota(jnp.int32, (planes * LANES, 2 * LANES), 0)
    column = lax.broadcasted_iota(jnp.int32, (planes * LANES, 2 * LANES), 1)
    is_low = column < LANES
    spot = SIDE + 2 * (column & (part - 1)) + jnp.where(is_low, 0, 1)
    same = (row // LANES) == ((column & (LANES - 1)) // part)
    distance = jnp.where(same, (row & (LANES - 1)) - spot, LANES)
    value = jnp.zeros((planes * LANES, 2 * LANES), jnp.float32)
    for offset in range(-4, 5):
        tap = jnp.where(is_low, taps_low[offset + 4], taps_high[offset + 4])
        value = jnp.where(distance == offset, tap, value)
    return value


def chunk_kernel(n_tile, own_hbm, owner_ref, out_ref, place_ref, base_ref, count_ref,
                 own, windows, arrived, fields, mids, slope, final, parts, returned, band_ref,
                 own_sem, send_sem, recv_sem, send_two, recv_two):
    g, t = lax.axis_index("grp"), lax.axis_index("tile")
    planes, rows, ny = own.shape
    n_grp = 4
    n_dev = n_grp * n_tile
    nx = rows * n_tile
    half = nx // 2
    me = t * n_grp + g

    load = pltpu.make_async_copy(own_hbm.at[0], own, own_sem)
    load.start()
    peers = [(lax.rem(g + k % n_grp, n_grp), lax.rem(t + k // n_grp, n_tile)) for k in range(1, n_dev)]
    barrier = pltpu.get_barrier_semaphore()
    for peer in peers:
        pl.semaphore_signal(barrier, inc=1, device_id=peer, device_id_type=MESH)
    load.wait()
    for z in range(planes):
        value = own[z]
        for odd in range(2):
            turned = pltpu.roll(value, SIDE if odd == 0 else ny - SIDE, 1)
            for m in range(n_dev // 2):
                windows[2 * m + odd, z * rows : (z + 1) * rows] = turned[:, m * LANES : (m + 1) * LANES]
    pl.semaphore_wait(barrier, n_dev - 1)

    def deal(peer, source):
        to = peer[1] * n_grp + peer[0]
        return pltpu.make_async_remote_copy(
            src_ref=windows.at[to], dst_ref=arrived.at[source], send_sem=send_sem.at[to], recv_sem=recv_sem.at[source],
            device_id=peer, device_id_type=MESH)

    def give_back(peer, source):
        to = peer[1] * n_grp + peer[0]
        return pltpu.make_async_remote_copy(
            src_ref=parts.at[to], dst_ref=returned.at[source], send_sem=send_two.at[to], recv_sem=recv_two.at[source],
            device_id=peer, device_id_type=MESH)

    for peer in peers:
        deal(peer, me).start()
    arrived[me] = windows[me]

    slots_of(n_tile, owner_ref, place_ref, base_ref, count_ref)
    band_ref[...] = column_band(planes)

    for peer in peers:
        deal(peer, peer[1] * n_grp + peer[0]).wait_recv()

    sublane = lax.broadcasted_iota(jnp.int32, (reach, SUB, LANES), 1)

    def flip(value):
        return jnp.where((sublane & 1) == 0, pltpu.roll(value, SUB - 1, 1), pltpu.roll(value, 1, 1))

    def wrap(ref, c):
        ref[c, 0:reach] = flip(ref[c, half : half + reach])
        ref[c, half + reach : half + 2 * reach] = flip(ref[c, reach : 2 * reach])

    for f in range(n_grp):
        for tile in range(n_tile):
            side, first = tile // (n_tile // 2), (tile % (n_tile // 2)) * rows
            for r in range(rows):
                fields[f, reach + first + r, pl.ds(side, planes, stride=2), :] = arrived[tile * n_grp + f, pl.ds(r, planes, stride=rows), :]
        wrap(fields, f)

    z_first, z_second = planes_taps(planes)
    step = rows

    def turn_z(value, m):
        return value if m == 0 else pltpu.roll(value, (-2 * m) % SUB, 1)

    def turn_y(value, k):
        return pltpu.roll(value, (-k) % LANES, 2)

    def gradient(i, direction):
        if direction == 0:
            shift = lambda k: fields[3, reach + i + k : reach + i + k + step]
        else:
            center = fields[3, reach + i : reach + i + step]
            if direction == 1:
                shift = lambda k: turn_y(center, k)
            else:
                total = None
                for m in range(1, planes):
                    if z_first[m] != 0.0:
                        term = z_first[m] * turn_z(center, m)
                        total = term if total is None else total + term
                return total
        value, _ = derivatives(None, shift, True, False)
        return value

    def tendency(ref, c, i, speed, press):
        center = ref[c, reach + i : reach + i + step]
        total = z_second[0] * center
        slope_z = None
        for m in range(1, planes):
            turned = turn_z(center, m)
            total = total + z_second[m] * turned
            if z_first[m] != 0.0:
                term = z_first[m] * turned
                slope_z = term if slope_z is None else slope_z + term
        slope_x, slope_y = None, None
        for k in range(1, reach + 1):
            ahead, behind = ref[c, reach + i + k : reach + i + k + step], ref[c, reach + i - k : reach + i - k + step]
            up, down = turn_y(center, k), turn_y(center, -k)
            term_x, term_y = first_coeffs[k - 1] * (ahead - behind), first_coeffs[k - 1] * (up - down)
            slope_x = term_x if slope_x is None else slope_x + term_x
            slope_y = term_y if slope_y is None else slope_y + term_y
            total = total + second_coeffs[k - 1] * ((ahead + behind) + (up + down))
        advect = speed[0] * slope_x + speed[1] * slope_y + speed[2] * slope_z
        return viscosity * total - advect - press, center

    def first_section(b, _):
        i = b * step
        speed = [fields[f, reach + i : reach + i + step] if isinstance(i, int) else fields[f, pl.ds(reach + i, step)] for f in range(3)]
        for c in range(3):
            press = gradient(i, c)
            slope[c, i : i + step] = press
            change, center = tendency(fields, c, i, speed, press)
            mids[c, reach + i : reach + i + step] = center + time_step * change
        return 0

    def second_section(b, _):
        i = b * step
        speed = [mids[f, reach + i : reach + i + step] for f in range(3)]
        for c in range(3):
            change, center = tendency(mids, c, i, speed, slope[c, i : i + step])
            final[c, i : i + step] = 0.5 * ((fields[c, reach + i : reach + i + step] + center) + time_step * change)
        return 0

    for b in range(half // step):
        first_section(b, 0)
    for c in range(3):
        wrap(mids, c)
    for b in range(half // step):
        second_section(b, 0)

    flat = lax.broadcasted_iota(jnp.int32, (SUB, LANES), 0)

    def flip_one(value):
        return jnp.where((flat & 1) == 0, pltpu.roll(value, SUB - 1, 0), pltpu.roll(value, 1, 0))

    matrix = lift_matrix(planes)
    z_coeffs = []
    for m in range(planes):
        column = jnp.zeros((SUB, LANES), jnp.float32)
        for z in range(planes):
            column = jnp.where(flat // 2 == z, float(matrix[z, (z + m) % planes]), column)
        z_coeffs.append(column)

    def lift_z(value):
        total = z_coeffs[0] * value
        for m in range(1, planes):
            total = total + z_coeffs[m] * pltpu.roll(value, (-2 * m) % SUB, 0)
        return total

    pairs = half // 2
    for c in range(3):
        even = [lift_z(final[c, 2 * i]) for i in range(pairs)]
        odd = [lift_z(final[c, 2 * i + 1]) for i in range(pairs)]
        for odd_tap, even_tap in ((lift_alpha, lift_beta), (lift_gamma, lift_delta)):
            after = even[1:] + [flip_one(even[0])]
            odd = [odd[i] + odd_tap * (even[i] + after[i]) for i in range(pairs)]
            before = [flip_one(odd[-1])] + odd[:-1]
            even = [even[i] + even_tap * (odd[i] + before[i]) for i in range(pairs)]
        for i in range(pairs):
            final[c, i] = even[i] * lift_scale
            final[c, pairs + i] = odd[i] * (1.0 / lift_scale)

    stacked = []
    for c in range(3):
        flat_ref = final.at[c].reshape(half * SUB, LANES)
        for high in range(2):
            for a in range(2):
                stacked.append(jnp.concatenate([flat_ref[pl.ds(high * pairs * SUB + 2 * z + a, pairs, stride=SUB), :] for z in range(planes)], axis=1))
    lines = jnp.dot(jnp.concatenate(stacked, axis=0), band_ref[...], precision=lax.Precision.HIGHEST, preferred_element_type=jnp.float32)
    lines = [lines[c * nx : (c + 1) * nx] for c in range(3)]
    lines.append(lines[0] * lines[0] + lines[1] * lines[1] + lines[2] * lines[2])
    for c in range(4):
        for tile in range(n_tile):
            part = lines[c][tile * rows : (tile + 1) * rows]
            parts[tile * n_grp + c, 0:rows] = part[:, 0:LANES]
            parts[tile * n_grp + c, rows : 2 * rows] = part[:, LANES:]

    for peer in peers:
        give_back(peer, me).start()
    returned[me] = parts[me]
    for peer in peers:
        give_back(peer, peer[1] * n_grp + peer[0]).wait_recv()

    group = lax.broadcasted_iota(jnp.int32, (SUB, LANES), 1) // (CHUNK // 2)
    for b in range(n_dev // 4):
        tiles = [returned[4 * b + m] for m in range(4)]
        for bit in range(2):
            distance = (CHUNK // 2) << bit
            is_low = (group & (1 << bit)) == 0
            turned = list(tiles)
            for m in range(4):
                if not m & (1 << bit):
                    other = m | (1 << bit)
                    turned[m] = jnp.where(is_low, tiles[m], pltpu.roll(tiles[other], distance, 1))
                    turned[other] = jnp.where(is_low, pltpu.roll(tiles[m], LANES - distance, 1), tiles[other])
            tiles = turned
        for z in range(planes):
            for high in range(2):
                out_ref[(z * 2 + high) * (n_dev // 4) + b] = tiles[z][high * rows : (high + 1) * rows]

    for peer in peers:
        deal(peer, me).wait_send()
        give_back(peer, me).wait_send()


def sort_kernel(n_tile, base_ref, count_ref, coeff_ref, place_ref, out_ref, current):
    n_blocks, rows, _ = coeff_ref.shape
    out_ref[...] = jnp.zeros_like(out_ref)
    current[...] = jnp.zeros_like(current)
    rank = lax.broadcasted_iota(jnp.int32, (LANES, LANES), 0).astype(jnp.float32)
    lane = lax.broadcasted_iota(jnp.int32, (rows, LANES), 1)

    def sort(b):
        value = coeff_ref[b]
        high = value.astype(jnp.bfloat16).astype(jnp.float32)
        rest = value - high
        mid = rest.astype(jnp.bfloat16).astype(jnp.float32)
        low = rest - mid
        pieces = jnp.concatenate([high, mid, low], axis=0).astype(jnp.bfloat16)
        chosen = jnp.where(rank == place_ref[pl.ds(b, 1), :], 1.0, 0.0).astype(jnp.bfloat16)
        ordered = lax.dot_general(pieces, chosen, (((1,), (1,)), ((), ())), preferred_element_type=jnp.float32)
        return (ordered[0:rows] + ordered[rows : 2 * rows]) + ordered[2 * rows : 3 * rows]

    def pencil(b, ordered, s, ahead):
        base, count = base_ref[b, s], count_ref[b, s]
        start = base & (LANES - 1)
        end = start + count
        turned = pltpu.roll(ordered, (start - ahead) & (LANES - 1), 1)
        now = current[s] + jnp.where((lane >= start) & (lane < end), turned, 0.0)
        group = pl.multiple_of(base - start, LANES)
        after = jnp.where(lane < end - LANES, turned, 0.0)
        current[s] = jnp.where(end >= LANES, after, now)
        out_ref[s, :, pl.ds(group, 2 * LANES)] = jnp.concatenate([now, after], axis=1)
        return ahead + count

    batch = 8

    def blocks(i, _):
        ordered = [sort(i * batch + j) for j in range(batch)]
        for j in range(batch):
            ahead = jnp.int32(0)
            for s in range(n_tile):
                ahead = pencil(i * batch + j, ordered[j], s, ahead)
        return 0

    lax.fori_loop(0, n_blocks // batch, blocks, 0)


def exchange_kernel(n_tile, sent_ref, out_ref, got, send_sem, recv_sem):
    g, t = lax.axis_index("grp"), lax.axis_index("tile")
    rows, cap = got.shape[1:]

    barrier = pltpu.get_barrier_semaphore()
    others = [lax.rem(t + k, n_tile) for k in range(1, n_tile)]
    for s in others:
        pl.semaphore_signal(barrier, inc=1, device_id=(g, s), device_id_type=MESH)
    pl.semaphore_wait(barrier, n_tile - 1)

    def exchange(s, slot):
        return pltpu.make_async_remote_copy(
            src_ref=sent_ref.at[s, :, pl.ds(0, cap)], dst_ref=got.at[slot], send_sem=send_sem.at[s],
            recv_sem=recv_sem.at[slot], device_id=(g, s), device_id_type=MESH)

    for s in others:
        exchange(s, t).start()
    got[t] = sent_ref[t, :, 0:cap]
    for s in others:
        exchange(s, s).wait_recv()
    for tile in range(n_tile):
        out_ref[tile * rows : (tile + 1) * rows] = got[tile]
    for s in others:
        exchange(s, t).wait_send()


def chunk_body(flow_state, line_owner, *, n_tile):
    _, planes, rows, ny = flow_state.shape
    n_lines = line_owner.shape[0]
    n_blocks = n_lines // LANES
    nx = rows * n_tile
    half = nx // 2
    n_dev = 4 * n_tile
    cap = 2 * planes * ny // n_tile
    vmem = pl.BlockSpec(memory_space=pltpu.VMEM)
    smem = pl.BlockSpec(memory_space=pltpu.SMEM)
    f32 = jnp.float32
    shape = jax.ShapeDtypeStruct
    limit = 16 * 1024 * 1024
    dma = pltpu.SemaphoreType.DMA
    owner = line_owner.reshape(n_blocks, LANES)
    ints = shape((n_blocks, LANES), jnp.int32)
    padded = (half + 2 * reach, SUB, LANES)
    coeffs, place, base, count = pl.pallas_call(
        functools.partial(chunk_kernel, n_tile),
        out_shape=(shape((n_blocks, rows, LANES), f32), shape((n_blocks, LANES), f32), ints, ints),
        in_specs=[pl.BlockSpec(memory_space=pl.ANY), vmem], out_specs=(vmem, vmem, vmem, vmem),
        scratch_shapes=[
            pltpu.VMEM((planes, rows, ny), f32), pltpu.VMEM((n_dev, planes * rows, LANES), f32), pltpu.VMEM((n_dev, planes * rows, LANES), f32),
            pltpu.VMEM((4,) + padded, f32), pltpu.VMEM((3,) + padded, f32),
            pltpu.VMEM((3, half, SUB, LANES), f32), pltpu.VMEM((3, half, SUB, LANES), f32),
            pltpu.VMEM((n_dev, 2 * rows, LANES), f32), pltpu.VMEM((n_dev, 2 * rows, LANES), f32),
            pltpu.VMEM((planes * LANES, 2 * LANES), f32),
            dma, dma((n_dev,)), dma((n_dev,)), dma((n_dev,)), dma((n_dev,)),
        ],
        compiler_params=pltpu.CompilerParams(has_side_effects=True, collective_id=0, vmem_limit_bytes=limit), name="flow",
    )(flow_state, owner)
    sent = pl.pallas_call(
        functools.partial(sort_kernel, n_tile),
        out_shape=shape((n_tile, rows, cap + 2 * LANES), f32),
        in_specs=[smem, smem, vmem, vmem], out_specs=vmem,
        scratch_shapes=[pltpu.VMEM((n_tile, rows, LANES), f32)],
        compiler_params=pltpu.CompilerParams(vmem_limit_bytes=limit), name="compact",
    )(base, count, coeffs, place)
    record = pl.pallas_call(
        functools.partial(exchange_kernel, n_tile),
        out_shape=shape((nx, cap), f32),
        in_specs=[vmem], out_specs=vmem,
        scratch_shapes=[pltpu.VMEM((n_tile, rows, cap), f32), dma((n_tile,)), dma((n_tile,))],
        compiler_params=pltpu.CompilerParams(has_side_effects=True, collective_id=1, vmem_limit_bytes=limit), name="record",
    )(sent)
    return record[None, None]


def fits_chunks(mesh, planes, rows, ny):
    n_tile = mesh.shape["tile"]
    return 2 * planes == SUB and 2 * rows == SUB and mesh.shape["grp"] == 4 and ny == 4 * n_tile * CHUNK and n_tile % 4 == 0


def solution(mesh):
    in_specs = (P("grp", None, "tile", None), P())
    out_specs = P("grp", "tile", None, None)
    n_tile = mesh.shape["tile"]

    def run(flow_state, line_owner):
        _, planes, rows, ny = flow_state.shape
        chosen = chunk_body if fits_chunks(mesh, planes, rows, ny) else tiled_body
        return chosen(flow_state, line_owner, n_tile=n_tile)

    return jax.shard_map(run, mesh=mesh, in_specs=in_specs, out_specs=out_specs, check_vma=False)
```

```python
import functools

import jax
import jax.numpy as jnp
import numpy as np
from jax import lax
from jax.experimental import pallas as pl
from jax.experimental.pallas import tpu as pltpu
from jax.sharding import PartitionSpec as P

time_step = 0.2
viscosity = 0.05
reach = 4
first_coeffs = (0.8, -0.2, 4.0 / 105.0, -1.0 / 280.0)
second_center = -205.0 / 72.0
second_coeffs = (1.6, -0.2, 8.0 / 315.0, -1.0 / 560.0)
lift_alpha = -1.586134342059924
lift_beta = -0.052980118572961
lift_gamma = 0.882911075530934
lift_delta = 0.443506852043971
lift_scale = 1.149604398860241
LANES = 128
MESH = pl.DeviceIdType.MESH


def lift_numpy(signal):
    even, odd = signal[0::2].copy(), signal[1::2].copy()
    odd += lift_alpha * (even + np.roll(even, -1, 0))
    even += lift_beta * (odd + np.roll(odd, 1, 0))
    odd += lift_gamma * (even + np.roll(even, -1, 0))
    even += lift_delta * (odd + np.roll(odd, 1, 0))
    return np.concatenate([even * lift_scale, odd / lift_scale])


def lift_matrix(length):
    return lift_numpy(np.eye(length))


def band_matrix():
    full = lift_matrix(8 * LANES)
    low = full[LANES : 2 * LANES, LANES : 5 * LANES]
    high = full[4 * LANES + LANES : 4 * LANES + 2 * LANES, LANES : 5 * LANES]
    return np.concatenate([low, high]).T.astype(np.float32)


def band_value(taps_low, taps_high):
    row = lax.broadcasted_iota(jnp.int32, (4 * LANES, 2 * LANES), 0)
    column = lax.broadcasted_iota(jnp.int32, (4 * LANES, 2 * LANES), 1)
    distance = row - LANES - 2 * (column & (LANES - 1))
    is_low = column < LANES
    value = jnp.zeros((4 * LANES, 2 * LANES), jnp.float32)
    for offset in range(-4, 5):
        tap = jnp.where(is_low, taps_low[offset + 4], taps_high[offset + 4])
        value = jnp.where(distance == offset, tap, value)
    return value


def band_taps():
    band = band_matrix()
    rows = slice(LANES + LANES // 2 - 4, LANES + LANES // 2 + 5)
    return [float(x) for x in band[rows, LANES // 4]], [float(x) for x in band[rows, LANES + LANES // 4]]


def shifted_y(value, k):
    return pltpu.roll(value, (-k) % value.shape[-1], value.ndim - 1)


def derivatives(center, shift, want_first=True, want_second=True):
    first, second = None, second_center * center if want_second else None
    for k in range(1, reach + 1):
        ahead, behind = shift(k), shift(-k)
        if want_first:
            term = first_coeffs[k - 1] * (ahead - behind)
            first = term if first is None else first + term
        if want_second:
            second = second + second_coeffs[k - 1] * (ahead + behind)
    return first, second


def slots_of(n_tile, owner_ref, place_ref, base_ref, count_ref):
    owner = owner_ref[...]
    n_blocks = owner.shape[0]
    upper = (lax.broadcasted_iota(jnp.int32, (LANES, LANES), 0) <= lax.broadcasted_iota(jnp.int32, (LANES, LANES), 1)).astype(jnp.float32)
    lower = (lax.broadcasted_iota(jnp.int32, (n_blocks, n_blocks), 0) > lax.broadcasted_iota(jnp.int32, (n_blocks, n_blocks), 1)).astype(jnp.float32)
    lane = lax.broadcasted_iota(jnp.int32, (n_blocks, LANES), 1)

    def step(s, carry):
        place, counts, ahead = carry
        mask = (owner == s).astype(jnp.float32)
        within = jnp.dot(mask, upper, preferred_element_type=jnp.float32)
        total = jnp.sum(mask, axis=1, keepdims=True)
        place = place + mask * (ahead + within - 1.0)
        counts = jnp.where(lane == s, total, counts)
        return place, counts, ahead + total

    zeros = jnp.zeros((n_blocks, LANES), jnp.float32)
    carry = (zeros, zeros, jnp.zeros((n_blocks, 1), jnp.float32))
    if n_tile <= 16:
        for s in range(n_tile):
            carry = step(s, carry)
    else:
        carry = lax.fori_loop(0, n_tile, step, carry)
    place, counts, _ = carry
    place_ref[...] = place
    count_ref[...] = counts.astype(jnp.int32)
    base_ref[...] = jnp.dot(lower, counts, preferred_element_type=jnp.float32).astype(jnp.int32)


def flow_kernel(n_tile, own_ref, owner_ref, out_ref, place_ref, base_ref, count_ref,
                fields, mids, halo, mid_halo, pad, ppad, middle, fin, along_y, along_z, lap, send_sem, recv_sem, hsend_sem, hrecv_sem, msend_sem, mrecv_sem, mhsend_sem, mhrecv_sem, relay_sem, band_ref):
    g, t = lax.axis_index("grp"), lax.axis_index("tile")
    right, left = lax.rem(t + 1, n_tile), lax.rem(t + n_tile - 1, n_tile)
    planes, rows, ny = own_ref.shape[1:]
    own = own_ref.at[0]

    barrier = pltpu.get_barrier_semaphore()
    for k in range(1, 4):
        pl.semaphore_signal(barrier, inc=1, device_id=(lax.rem(g + k, 4), t), device_id_type=MESH)
    for side in (right, left):
        pl.semaphore_signal(barrier, inc=1, device_id=(g, side), device_id_type=MESH)

    @pl.when((g == 0) | (g == 3))
    def _():
        for side in (right, left):
            pl.semaphore_signal(barrier, inc=1, device_id=(3 - g, side), device_id_type=MESH)
        pl.semaphore_wait(barrier, 7)

    @pl.when((g == 1) | (g == 2))
    def _():
        pl.semaphore_wait(barrier, 5)

    def gather_copy(src, dst, ssem, rsem, k, slot):
        return pltpu.make_async_remote_copy(
            src_ref=src, dst_ref=dst.at[slot], send_sem=ssem.at[k], recv_sem=rsem.at[slot],
            device_id=(k, t), device_id_type=MESH)

    half = planes // 2

    def whole_copy(k, slot):
        return pltpu.make_async_remote_copy(
            src_ref=own, dst_ref=fields.at[slot], send_sem=send_sem.at[k], recv_sem=recv_sem.at[slot, 0],
            device_id=(k, t), device_id_type=MESH)

    def half_copy(slot, k):
        part = pl.ds(k * half, half)
        return pltpu.make_async_remote_copy(
            src_ref=own.at[part], dst_ref=fields.at[slot, part], send_sem=send_sem.at[k],
            recv_sem=recv_sem.at[slot, k], device_id=(k, t), device_id_type=MESH)

    def relay_copy(slot, k):
        part = pl.ds(k * half, half)
        return pltpu.make_async_remote_copy(
            src_ref=fields.at[slot, part], dst_ref=fields.at[slot, part], send_sem=relay_sem.at[slot],
            recv_sem=recv_sem.at[slot, k], device_id=(1 - k, t), device_id_type=MESH)

    def halo_copy(src, dst, ssem, rsem, side, slot, group):
        return pltpu.make_async_remote_copy(
            src_ref=src, dst_ref=dst.at[slot + side], send_sem=ssem.at[side], recv_sem=rsem.at[slot + side],
            device_id=(group, right if side == 0 else left), device_id_type=MESH)

    @pl.when(g < 3)
    def _():
        for side in range(2):
            halo_copy(own, halo, hsend_sem, hrecv_sem, side, 0, g).start()

    for k in range(3):
        @pl.when((g < 2) & (g != k))
        def _(k=k):
            whole_copy(k, g).start()

    @pl.when(g >= 2)
    def _():
        for k in range(2):
            half_copy(g, k).start()

    @pl.when(g == 3)
    def _():
        whole_copy(2, 3).start()
        for side in range(2):
            halo_copy(own, halo, hsend_sem, hrecv_sem, side, 2, 0).start()

    def local_terms():
        for z in range(planes):
            center = pad[z, reach : reach + rows]
            fy, sy = derivatives(center, lambda k: shifted_y(center, k))
            fz, sz = derivatives(center, lambda k: pad[(z + k) % planes, reach : reach + rows])
            along_y[z], along_z[z], lap[z] = fy, fz, sy + sz

    slots_of(n_tile, owner_ref, place_ref, base_ref, count_ref)
    band_ref[...] = band_value(*band_taps())

    @pl.when(g < 3)
    def _():
        for k in range(3):
            @pl.when(g == k)
            def _(k=k):
                fields[k] = own_ref[0]

        for z in range(planes):
            pad[z, reach : reach + rows] = own_ref[0, z]
        local_terms()

        @pl.when(g < 2)
        def _():
            for slot in (2, 3):
                half_copy(slot, g).wait_recv()
                relay_copy(slot, g).start()
            whole_copy(0, 1 - g).wait_recv()
            for slot in (2, 3):
                half_copy(slot, 1 - g).wait_recv()

        @pl.when(g == 2)
        def _():
            for slot in (0, 1, 3):
                whole_copy(0, slot).wait_recv()

        for side in range(2):
            halo_copy(own, halo, hsend_sem, hrecv_sem, side, 0, g).wait_recv()

        @pl.when(g == 0)
        def _():
            for side in range(2):
                halo_copy(own, halo, hsend_sem, hrecv_sem, side, 2, 0).wait_recv()
            for z in range(planes):
                ppad[z, 0:reach] = halo[2, z, rows - reach : rows]
                ppad[z, reach : reach + rows] = fields[3, z]
                ppad[z, reach + rows : 2 * reach + rows] = halo[3, z, 0:reach]
            for z in range(planes):
                middle[z], _ = derivatives(None, lambda k: ppad[z, reach + k : reach + k + rows], True, False)

        @pl.when(g == 1)
        def _():
            for z in range(planes):
                value = fields[3, z]
                middle[z], _ = derivatives(None, lambda k: shifted_y(value, k), True, False)

        @pl.when(g == 2)
        def _():
            for z in range(planes):
                middle[z], _ = derivatives(None, lambda k: fields[3, (z + k) % planes], True, False)

        def tendency(z, vel, press):
            center = pad[z, reach : reach + rows]
            fx, sx = derivatives(center, lambda k: pad[z, reach + k : reach + k + rows])
            advect = vel[0, z] * fx + vel[1, z] * along_y[z] + vel[2, z] * along_z[z]
            return viscosity * (sx + lap[z]) - advect - press

        for z in range(planes):
            pad[z, 0:reach] = halo[0, z, rows - reach : rows]
            pad[z, reach + rows : 2 * reach + rows] = halo[1, z, 0:reach]
        for z in range(planes):
            press = middle[z]
            ppad[z, 0:rows] = press
        for z in range(planes):
            middle[z] = own_ref[0, z] + time_step * tendency(z, fields, ppad[z, 0:rows])

        for side in range(2):
            halo_copy(middle, mid_halo, mhsend_sem, mhrecv_sem, side, 0, g).start()
        for k in range(3):
            @pl.when(g != k)
            def _(k=k):
                gather_copy(middle, mids, msend_sem, mrecv_sem, k, g).start()

            @pl.when(g == k)
            def _(k=k):
                mids[k] = middle[...]

        for z in range(planes):
            pad[z, reach : reach + rows] = middle[z]
        local_terms()
        for k in range(3):
            @pl.when(g != k)
            def _(k=k):
                gather_copy(middle, mids, msend_sem, mrecv_sem, 0, k).wait_recv()
        for side in range(2):
            halo_copy(middle, mid_halo, mhsend_sem, mhrecv_sem, side, 0, g).wait_recv()
        for z in range(planes):
            pad[z, 0:reach] = mid_halo[0, z, rows - reach : rows]
            pad[z, reach + rows : 2 * reach + rows] = mid_halo[1, z, 0:reach]
        for z in range(planes):
            fin[z] = 0.5 * ((own_ref[0, z] + middle[z]) + time_step * tendency(z, mids, ppad[z, 0:rows]))

        blocks = ny // (2 * LANES)
        groups = ny // LANES
        for z in range(planes):
            value = fin[z]
            pieces = []
            for b in range(blocks):
                window = [value[:, ((2 * b + j) % groups) * LANES : ((2 * b + j) % groups + 1) * LANES] for j in (-1, 0, 1, 2)]
                pieces.append(jnp.concatenate(window, axis=1))
            stacked = jnp.concatenate(pieces, axis=0)
            lifted = jnp.dot(stacked, band_ref[...], precision=lax.Precision.HIGHEST, preferred_element_type=jnp.float32)
            for b in range(blocks):
                piece = lifted[b * rows : (b + 1) * rows]
                fin[z, :, b * LANES : (b + 1) * LANES] = piece[:, 0:LANES]
                fin[z, :, ny // 2 + b * LANES : ny // 2 + (b + 1) * LANES] = piece[:, LANES:]

        even = [fin[2 * i] for i in range(half)]
        odd = [fin[2 * i + 1] for i in range(half)]
        odd = [odd[i] + lift_alpha * (even[i] + even[(i + 1) % half]) for i in range(half)]
        even = [even[i] + lift_beta * (odd[i] + odd[(i - 1) % half]) for i in range(half)]
        odd = [odd[i] + lift_gamma * (even[i] + even[(i + 1) % half]) for i in range(half)]
        even = [even[i] + lift_delta * (odd[i] + odd[(i - 1) % half]) for i in range(half)]
        for i in range(half):
            out_ref[i] = even[i] * lift_scale
            out_ref[half + i] = odd[i] * (1.0 / lift_scale)

        for side in range(2):
            halo_copy(middle, mid_halo, mhsend_sem, mhrecv_sem, side, 0, g).wait_send()
        for k in range(3):
            @pl.when(g != k)
            def _(k=k):
                gather_copy(middle, mids, msend_sem, mrecv_sem, k, g).wait_send()

    @pl.when(g == 3)
    def _():
        out_ref[...] = jnp.zeros_like(out_ref)

    for side in range(2):
        halo_copy(own, halo, hsend_sem, hrecv_sem, side, 0, g).wait_send()
    for k in range(3):
        @pl.when((g < 2) & (g != k))
        def _(k=k):
            whole_copy(k, g).wait_send()

    @pl.when(g < 2)
    def _():
        for slot in (2, 3):
            relay_copy(slot, g).wait_send()

    @pl.when(g >= 2)
    def _():
        for k in range(2):
            half_copy(g, k).wait_send()

    @pl.when(g == 3)
    def _():
        whole_copy(2, 3).wait_send()


def compact_kernel(n_tile, base_ref, count_ref, coeff_ref, place_ref, out_ref, current):
    planes, rows, ny = coeff_ref.shape
    groups = ny // LANES
    out_ref[...] = jnp.zeros_like(out_ref)
    current[...] = jnp.zeros_like(current)
    rank = lax.broadcasted_iota(jnp.int32, (LANES, LANES), 0).astype(jnp.float32)
    lane = lax.broadcasted_iota(jnp.int32, (rows, LANES), 1)

    def sort(b):
        z, y = b // groups, b % groups
        value = coeff_ref[z, :, pl.ds(pl.multiple_of(y * LANES, LANES), LANES)]
        high = value.astype(jnp.bfloat16).astype(jnp.float32)
        rest = value - high
        mid = rest.astype(jnp.bfloat16).astype(jnp.float32)
        low = rest - mid
        parts = jnp.concatenate([high, mid, low], axis=0).astype(jnp.bfloat16)
        chosen = jnp.where(rank == place_ref[pl.ds(b, 1), :], 1.0, 0.0).astype(jnp.bfloat16)
        ordered = lax.dot_general(parts, chosen, (((1,), (1,)), ((), ())), preferred_element_type=jnp.float32)
        return (ordered[0:rows] + ordered[rows : 2 * rows]) + ordered[2 * rows : 3 * rows]

    def pencil(b, ordered, s, ahead):
        base, count = base_ref[b, s], count_ref[b, s]
        start = base & (LANES - 1)
        end = start + count
        turned = pltpu.roll(ordered, (start - ahead) & (LANES - 1), 1)
        now = current[s] + jnp.where((lane >= start) & (lane < end), turned, 0.0)
        group = pl.multiple_of(base - start, LANES)
        after = jnp.where(lane < end - LANES, turned, 0.0)
        current[s] = jnp.where(end >= LANES, after, now)
        out_ref[s, :, pl.ds(group, 2 * LANES)] = jnp.concatenate([now, after], axis=1)
        return ahead + count

    n_blocks = planes * groups
    batch = 8 if n_blocks % 8 == 0 and n_tile <= 16 else 1

    def blocks(i, _):
        ordered = [sort(i * batch + j) for j in range(batch)]
        for j in range(batch):
            b = i * batch + j
            if n_tile <= 16:
                ahead = jnp.int32(0)
                for s in range(n_tile):
                    ahead = pencil(b, ordered[j], s, ahead)
            else:
                lax.fori_loop(0, n_tile, lambda s, ahead: pencil(b, ordered[j], s, ahead), jnp.int32(0))
        return 0

    lax.fori_loop(0, n_blocks // batch, blocks, 0)


def record_kernel(n_tile, chunks, sent_ref, matrix_ref, out_ref, got, records, send_sem, recv_sem, rsend_sem, rrecv_sem):
    g, t = lax.axis_index("grp"), lax.axis_index("tile")
    rows, nx, cap = sent_ref.shape[1], out_ref.shape[0], out_ref.shape[1]
    width = cap // chunks

    barrier = pltpu.get_barrier_semaphore()

    @pl.when(g < 3)
    def _():
        for k in range(1, n_tile):
            pl.semaphore_signal(barrier, inc=1, device_id=(g, lax.rem(t + k, n_tile)), device_id_type=MESH)
        pl.semaphore_signal(barrier, inc=1, device_id=(3, t), device_id_type=MESH)
        pl.semaphore_wait(barrier, n_tile)

    @pl.when(g == 3)
    def _():
        for k in range(3):
            pl.semaphore_signal(barrier, inc=1, device_id=(k, t), device_id_type=MESH)
        pl.semaphore_wait(barrier, 3)

    def exchange(s, slot, c):
        part = pl.ds(c * width, width)
        return pltpu.make_async_remote_copy(
            src_ref=sent_ref.at[s, :, part], dst_ref=got.at[slot, :, part], send_sem=send_sem.at[s, c],
            recv_sem=recv_sem.at[slot, c], device_id=(g, s), device_id_type=MESH)

    def report(c, slot):
        part = pl.ds(c * width, width)
        return pltpu.make_async_remote_copy(
            src_ref=out_ref.at[:, part], dst_ref=records.at[slot, :, part], send_sem=rsend_sem.at[c],
            recv_sem=rrecv_sem.at[slot, c], device_id=(3, t), device_id_type=MESH)

    @pl.when(g < 3)
    def _():
        for c in range(chunks):
            for k in range(1, n_tile):
                exchange(lax.rem(t + k, n_tile), t, c).start()
        got[t] = sent_ref[t, :, 0:cap]
        matrix = matrix_ref[...]
        for c in range(chunks):
            for k in range(1, n_tile):
                exchange(lax.rem(t + k, n_tile), lax.rem(t + k, n_tile), c).wait_recv()
            value = got[:, :, c * width : (c + 1) * width].reshape(nx, width)
            out_ref[:, c * width : (c + 1) * width] = jnp.dot(
                matrix, value, precision=lax.Precision.HIGHEST, preferred_element_type=jnp.float32)
            report(c, g).start()
        for c in range(chunks):
            for k in range(1, n_tile):
                exchange(lax.rem(t + k, n_tile), t, c).wait_send()
            report(c, g).wait_send()

    @pl.when(g == 3)
    def _():
        for c in range(chunks):
            for k in range(3):
                report(c, k).wait_recv()
            part = slice(c * width, (c + 1) * width)
            first, second, third = records[0, :, part], records[1, :, part], records[2, :, part]
            out_ref[:, part] = first * first + second * second + third * third


def tiled_body(flow_state, line_owner, *, n_tile):
    _, planes, rows, ny = flow_state.shape
    n_lines = line_owner.shape[0]
    n_blocks = n_lines // LANES
    nx = rows * n_tile
    cap = 2 * planes * ny // n_tile
    vmem = pl.BlockSpec(memory_space=pltpu.VMEM)
    smem = pl.BlockSpec(memory_space=pltpu.SMEM)
    f32 = jnp.float32
    shape = jax.ShapeDtypeStruct
    limit = 16 * 1024 * 1024
    dma = pltpu.SemaphoreType.DMA
    owner = line_owner.reshape(n_blocks, LANES)
    tile = (planes, rows, ny)
    ints = shape((n_blocks, LANES), jnp.int32)
    coeffs, place, base, count = pl.pallas_call(
        functools.partial(flow_kernel, n_tile),
        out_shape=(shape(tile, f32), shape((n_blocks, LANES), f32), ints, ints),
        in_specs=[vmem, vmem], out_specs=(vmem, vmem, vmem, vmem),
        scratch_shapes=[
            pltpu.VMEM((4,) + tile, f32), pltpu.VMEM((3,) + tile, f32),
            pltpu.VMEM((4,) + tile, f32), pltpu.VMEM((2,) + tile, f32),
            pltpu.VMEM((planes, rows + 2 * reach, ny), f32), pltpu.VMEM((planes, rows + 2 * reach, ny), f32),
            pltpu.VMEM(tile, f32), pltpu.VMEM(tile, f32), pltpu.VMEM(tile, f32), pltpu.VMEM(tile, f32), pltpu.VMEM(tile, f32),
            dma((4,)), dma((4, 2)), dma((2,)), dma((4,)), dma((4,)), dma((4,)), dma((2,)), dma((2,)), dma((4,)),
            pltpu.VMEM((4 * LANES, 2 * LANES), f32),
        ],
        compiler_params=pltpu.CompilerParams(has_side_effects=True, collective_id=0, vmem_limit_bytes=limit), name="flow",
    )(flow_state, owner)
    sent = pl.pallas_call(
        functools.partial(compact_kernel, n_tile),
        out_shape=shape((n_tile, rows, cap + 2 * LANES), f32),
        in_specs=[smem, smem, vmem, vmem], out_specs=vmem,
        scratch_shapes=[pltpu.VMEM((n_tile, rows, LANES), f32)],
        compiler_params=pltpu.CompilerParams(vmem_limit_bytes=limit), name="compact",
    )(base, count, coeffs, place)
    chunks = 4 if cap % (4 * LANES) == 0 else 1
    record = pl.pallas_call(
        functools.partial(record_kernel, n_tile, chunks),
        out_shape=shape((nx, cap), f32),
        in_specs=[vmem, vmem], out_specs=vmem,
        scratch_shapes=[
            pltpu.VMEM((n_tile, rows, cap), f32), pltpu.VMEM((3, nx, cap), f32),
            dma((n_tile, chunks)), dma((n_tile, chunks)), dma((chunks,)), dma((3, chunks)),
        ],
        compiler_params=pltpu.CompilerParams(has_side_effects=True, collective_id=1, vmem_limit_bytes=limit), name="record",
    )(sent, jnp.asarray(lift_matrix(nx).astype(np.float32)))
    return record[None, None]


CHUNK = 64
SIDE = (LANES - CHUNK) // 2
SUB = 8


def planes_taps(planes):
    first, second = [0.0] * planes, [0.0] * planes
    second[0] = 3.0 * second_center
    for k in range(1, reach + 1):
        first[k % planes] += first_coeffs[k - 1]
        first[-k % planes] -= first_coeffs[k - 1]
        second[k % planes] += second_coeffs[k - 1]
        second[-k % planes] += second_coeffs[k - 1]
    return first, second


def column_taps():
    full = lift_matrix(8 * CHUNK)
    middle = 4 * CHUNK
    low = full[middle // 2, middle - 4 : middle + 5]
    high = full[8 * CHUNK // 2 + middle // 2, middle + 1 - 4 : middle + 1 + 5]
    return [float(x) for x in low], [float(x) for x in high]


def column_band(planes):
    taps_low, taps_high = column_taps()
    part = CHUNK // 2
    row = lax.broadcasted_iota(jnp.int32, (planes * LANES, 2 * LANES), 0)
    column = lax.broadcasted_iota(jnp.int32, (planes * LANES, 2 * LANES), 1)
    is_low = column < LANES
    spot = SIDE + 2 * (column & (part - 1)) + jnp.where(is_low, 0, 1)
    same = (row // LANES) == ((column & (LANES - 1)) // part)
    distance = jnp.where(same, (row & (LANES - 1)) - spot, LANES)
    value = jnp.zeros((planes * LANES, 2 * LANES), jnp.float32)
    for offset in range(-4, 5):
        tap = jnp.where(is_low, taps_low[offset + 4], taps_high[offset + 4])
        value = jnp.where(distance == offset, tap, value)
    return value


def pencil_slots(pencil, owner, spot_ref, group_ref):
    n_blocks = owner.shape[0]
    upper = (lax.broadcasted_iota(jnp.int32, (LANES, LANES), 0) <= lax.broadcasted_iota(jnp.int32, (LANES, LANES), 1)).astype(jnp.float32)
    lower = (lax.broadcasted_iota(jnp.int32, (n_blocks, n_blocks), 0) > lax.broadcasted_iota(jnp.int32, (n_blocks, n_blocks), 1)).astype(jnp.float32)
    lane = lax.broadcasted_iota(jnp.int32, (n_blocks, LANES), 1)
    mine = owner == pencil
    mask = mine.astype(jnp.float32)
    within = jnp.dot(mask, upper, preferred_element_type=jnp.float32)
    total = jnp.broadcast_to(jnp.sum(mask, axis=1, keepdims=True), (n_blocks, LANES))
    base = jnp.dot(lower, total, preferred_element_type=jnp.float32).astype(jnp.int32)
    slot = base + within.astype(jnp.int32) - 1
    spot_ref[...] = jnp.where(mine, slot & (LANES - 1), -1)
    group_ref[...] = base // LANES + jnp.where(lane < (base & (LANES - 1)), 1, 0)


def chunk_kernel(n_tile, own_hbm, owner_hbm, out_ref,
                 own, owner_ref, windows, arrived, fields, mids, slope, final, pieces, landed, spot_ref, group_ref, ordered, band_ref,
                 own_sem, owner_sem, send_sem, recv_sem, recv_two, hand_sem, side_sem, up_sem, down_sem, cross_sem):
    g, t = lax.axis_index("grp"), lax.axis_index("tile")
    planes, rows, ny = own.shape
    n_grp = 4
    n_dev = n_grp * n_tile
    nx = rows * n_tile
    half = nx // 2
    me = t * n_grp + g

    load = pltpu.make_async_copy(own_hbm.at[0], own, own_sem)
    load.start()
    load_owner = pltpu.make_async_copy(owner_hbm, owner_ref, owner_sem)
    load_owner.start()
    peers = [(lax.rem(g + k % n_grp, n_grp), lax.rem(t + k // n_grp, n_tile)) for k in range(1, n_dev)]
    barrier = pltpu.get_barrier_semaphore()
    for peer in peers:
        pl.semaphore_signal(barrier, inc=1, device_id=peer, device_id_type=MESH)
    load.wait()
    for z in range(planes):
        value = own[z]
        for odd in range(2):
            turned = pltpu.roll(value, SIDE if odd == 0 else ny - SIDE, 1)
            for m in range(n_dev // 2):
                windows[2 * m + odd, z * rows : (z + 1) * rows] = turned[:, m * LANES : (m + 1) * LANES]
    pl.semaphore_wait(barrier, n_dev - 1)

    def deal(peer, source):
        to = peer[1] * n_grp + peer[0]
        return pltpu.make_async_remote_copy(
            src_ref=windows.at[to], dst_ref=arrived.at[source], send_sem=send_sem.at[to], recv_sem=recv_sem.at[source],
            device_id=peer, device_id_type=MESH)

    for peer in peers:
        deal(peer, me).start()
    arrived[me] = windows[me]

    load_owner.wait()
    pencil_slots(t, owner_ref[...], spot_ref, group_ref)
    out_ref[...] = jnp.zeros_like(out_ref)
    band_ref[...] = column_band(planes)

    for peer in peers:
        deal(peer, peer[1] * n_grp + peer[0]).wait_recv()

    sublane = lax.broadcasted_iota(jnp.int32, (reach, SUB, LANES), 1)

    def flip(value):
        return jnp.where((sublane & 1) == 0, pltpu.roll(value, SUB - 1, 1), pltpu.roll(value, 1, 1))

    def wrap(ref, c):
        ref[c, 0:reach] = flip(ref[c, half : half + reach])
        ref[c, half + reach : half + 2 * reach] = flip(ref[c, reach : 2 * reach])

    for f in range(n_grp):
        for tile in range(n_tile):
            side, first = tile // (n_tile // 2), (tile % (n_tile // 2)) * rows
            for r in range(rows):
                fields[f, reach + first + r, pl.ds(side, planes, stride=2), :] = arrived[tile * n_grp + f, pl.ds(r, planes, stride=rows), :]
        wrap(fields, f)

    z_first, z_second = planes_taps(planes)
    step = rows

    def turn_z(value, m):
        return value if m == 0 else pltpu.roll(value, (-2 * m) % SUB, 1)

    def turn_y(value, k):
        return pltpu.roll(value, (-k) % LANES, 2)

    def gradient(i, direction):
        if direction == 0:
            shift = lambda k: fields[3, reach + i + k : reach + i + k + step]
        else:
            center = fields[3, reach + i : reach + i + step]
            if direction == 1:
                shift = lambda k: turn_y(center, k)
            else:
                total = None
                for m in range(1, planes):
                    if z_first[m] != 0.0:
                        term = z_first[m] * turn_z(center, m)
                        total = term if total is None else total + term
                return total
        value, _ = derivatives(None, shift, True, False)
        return value

    def tendency(ref, c, i, speed, press):
        center = ref[c, reach + i : reach + i + step]
        total = z_second[0] * center
        slope_z = None
        for m in range(1, planes):
            turned = turn_z(center, m)
            total = total + z_second[m] * turned
            if z_first[m] != 0.0:
                term = z_first[m] * turned
                slope_z = term if slope_z is None else slope_z + term
        slope_x, slope_y = None, None
        for k in range(1, reach + 1):
            ahead, behind = ref[c, reach + i + k : reach + i + k + step], ref[c, reach + i - k : reach + i - k + step]
            up, down = turn_y(center, k), turn_y(center, -k)
            term_x, term_y = first_coeffs[k - 1] * (ahead - behind), first_coeffs[k - 1] * (up - down)
            slope_x = term_x if slope_x is None else slope_x + term_x
            slope_y = term_y if slope_y is None else slope_y + term_y
            total = total + second_coeffs[k - 1] * ((ahead + behind) + (up + down))
        advect = speed[0] * slope_x + speed[1] * slope_y + speed[2] * slope_z
        return viscosity * total - advect - press, center

    def first_section(b, _):
        i = b * step
        speed = [fields[f, reach + i : reach + i + step] if isinstance(i, int) else fields[f, pl.ds(reach + i, step)] for f in range(3)]
        for c in range(3):
            press = gradient(i, c)
            slope[c, i : i + step] = press
            change, center = tendency(fields, c, i, speed, press)
            mids[c, reach + i : reach + i + step] = center + time_step * change
        return 0

    def second_section(b, _):
        i = b * step
        speed = [mids[f, reach + i : reach + i + step] for f in range(3)]
        for c in range(3):
            change, center = tendency(mids, c, i, speed, slope[c, i : i + step])
            final[c, i : i + step] = 0.5 * ((fields[c, reach + i : reach + i + step] + center) + time_step * change)
        return 0

    for b in range(half // step):
        first_section(b, 0)
    for c in range(3):
        wrap(mids, c)
    for b in range(half // step):
        second_section(b, 0)

    flat = lax.broadcasted_iota(jnp.int32, (SUB, LANES), 0)

    def flip_one(value):
        return jnp.where((flat & 1) == 0, pltpu.roll(value, SUB - 1, 0), pltpu.roll(value, 1, 0))

    matrix = lift_matrix(planes)
    z_coeffs = []
    for m in range(planes):
        column = jnp.zeros((SUB, LANES), jnp.float32)
        for z in range(planes):
            column = jnp.where(flat // 2 == z, float(matrix[z, (z + m) % planes]), column)
        z_coeffs.append(column)

    def lift_z(value):
        total = z_coeffs[0] * value
        for m in range(1, planes):
            total = total + z_coeffs[m] * pltpu.roll(value, (-2 * m) % SUB, 0)
        return total

    pairs = half // 2
    for c in range(3):
        even = [lift_z(final[c, 2 * i]) for i in range(pairs)]
        odd = [lift_z(final[c, 2 * i + 1]) for i in range(pairs)]
        for odd_tap, even_tap in ((lift_alpha, lift_beta), (lift_gamma, lift_delta)):
            after = even[1:] + [flip_one(even[0])]
            odd = [odd[i] + odd_tap * (even[i] + after[i]) for i in range(pairs)]
            before = [flip_one(odd[-1])] + odd[:-1]
            even = [even[i] + even_tap * (odd[i] + before[i]) for i in range(pairs)]
        for i in range(pairs):
            final[c, i] = even[i] * lift_scale
            final[c, pairs + i] = odd[i] * (1.0 / lift_scale)

    stacked = []
    for c in range(3):
        flat_ref = final.at[c].reshape(half * SUB, LANES)
        for high in range(2):
            for a in range(2):
                stacked.append(jnp.concatenate([flat_ref[pl.ds(high * pairs * SUB + 2 * z + a, pairs, stride=SUB), :] for z in range(planes)], axis=1))
    lines = jnp.dot(jnp.concatenate(stacked, axis=0), band_ref[...], precision=lax.Precision.HIGHEST, preferred_element_type=jnp.float32)
    lines = [lines[c * nx : (c + 1) * nx] for c in range(3)]
    lines.append(lines[0] * lines[0] + lines[1] * lines[1] + lines[2] * lines[2])
    for c in range(n_grp):
        pieces[c] = lines[c]

    z, y = t // 2, t % 2
    n_z = n_tile // 2

    def flipped(value, bits):
        result, place = 0, 1
        while place < n_z:
            result = result + place * lax.rem(value // place + bits // place, 2)
            place *= 2
        return result

    partner = flipped(z, 1)

    def source_of(level, column, group):
        return (level * 2 + column) * n_grp + group

    def send(origin, source, sem, group, level, column):
        return pltpu.make_async_remote_copy(
            src_ref=origin, dst_ref=landed.at[source], send_sem=sem, recv_sem=recv_two.at[source],
            device_id=(group, level * 2 + column), device_id_type=MESH)

    kin = [g, g + 1 - 2 * lax.rem(g, 2), lax.rem(g + 2, n_grp), n_grp - 1 - g]

    def hand(k):
        group = kin[k]
        return send(pieces.at[group], me, hand_sem.at[k], group, z, y)

    def climb(origin, source):
        return send(origin, source, up_sem.at[source], g, z + 1, y)

    def sink(origin, source):
        return send(origin, source, down_sem.at[source], g, z - 1, y)

    def side(origin, source):
        return send(origin, source, side_sem.at[source], g, z, 1 - y)

    def cross(source):
        return send(landed.at[source], source, cross_sem.at[source], g, partner, y)

    def await_piece(source):
        send(pieces.at[g], source, hand_sem.at[0], g, z, 1 - y).wait_recv()

    def spread(origin, source):
        side(origin, source).start()

        @pl.when(z + 1 < n_z)
        def _():
            climb(origin, source).start()

        @pl.when(z > 0)
        def _():
            sink(origin, source).start()

    for k in (2, 3, 1):
        hand(k).start()
    spread(pieces.at[g], me)
    landed[me] = pieces[g]
    for k in range(1, n_grp):
        source = source_of(z, y, kin[k])
        await_piece(source)
        spread(landed.at[source], source)

    def relay(distance):
        for k in range(n_grp):
            for up in (True, False):
                level = z - distance if up else z + distance

                @pl.when(level >= 0 if up else level < n_z)
                def _(up=up, level=level):
                    source = source_of(level, y, kin[k])
                    await_piece(source)

                    @pl.when(z + 1 < n_z if up else z > 0)
                    def _():
                        (climb if up else sink)(landed.at[source], source).start()

                    @pl.when((level != partner) | (k < n_grp // 2))
                    def _():
                        side(landed.at[source], source).start()

    relay(1)
    for k in range(n_grp):
        source = source_of(z, 1 - y, kin[k])
        await_piece(source)
        if k >= n_grp // 2:
            cross(source).start()
    for distance in range(2, n_z):
        relay(distance)

    rank = lax.broadcasted_iota(jnp.int32, (LANES, LANES), 0)
    n_groups = n_tile
    lane_part = lax.broadcasted_iota(jnp.int32, (nx, LANES), 1) // (CHUNK // 2)

    def select(tile):
        for high in range(2):
            tiles = [landed[tile * n_grp + m, :, high * LANES : (high + 1) * LANES] for m in range(4)]
            for bit in range(2):
                distance = (CHUNK // 2) << bit
                is_low = (lane_part & (1 << bit)) == 0
                turned = list(tiles)
                for m in range(4):
                    if not m & (1 << bit):
                        other = m | (1 << bit)
                        turned[m] = jnp.where(is_low, tiles[m], pltpu.roll(tiles[other], distance, 1))
                        turned[other] = jnp.where(is_low, pltpu.roll(tiles[m], LANES - distance, 1), tiles[other])
                tiles = turned
            for plane in range(planes):
                block = (plane * 2 + high) * n_groups + tile
                value = tiles[plane]
                first = value.astype(jnp.bfloat16).astype(jnp.float32)
                rest = value - first
                second = rest.astype(jnp.bfloat16).astype(jnp.float32)
                stack = jnp.concatenate([first, second, rest - second], axis=0).astype(jnp.bfloat16)
                chosen = jnp.where(rank == spot_ref[pl.ds(block, 1), :], 1.0, 0.0).astype(jnp.bfloat16)
                placed = lax.dot_general(stack, chosen, (((1,), (1,)), ((), ())), preferred_element_type=jnp.float32)
                ordered[plane * 2 + high] = (placed[0:nx] + placed[nx : 2 * nx]) + placed[2 * nx : 3 * nx]
        labels = [group_ref[pl.ds((plane * 2 + high) * n_groups + tile, 1), :] for plane in range(planes) for high in range(2)]
        for q in range(out_ref.shape[1] // LANES):
            total = out_ref[:, q * LANES : (q + 1) * LANES]
            for n, label in enumerate(labels):
                total = total + jnp.where(label == q, ordered[n], 0.0)
            out_ref[:, q * LANES : (q + 1) * LANES] = total

    def own_column(k, _):
        select(flipped(z, k) * 2 + y)
        return 0

    lax.fori_loop(0, n_z, own_column, 0)
    select(z * 2 + 1 - y)

    def other_column(k, _):
        level = flipped(z, k)
        for group in range(n_grp):
            await_piece(source_of(level, 1 - y, group))
        select(level * 2 + 1 - y)
        return 0

    lax.fori_loop(1, n_z, other_column, 0)

    for peer in peers:
        deal(peer, me).wait_send()
    for k in range(1, n_grp):
        hand(k).wait_send()
    for k in range(n_grp // 2, n_grp):
        cross(source_of(z, 1 - y, kin[k])).wait_send()
    for level in range(n_z):
        for k in range(n_grp):
            source = source_of(level, y, kin[k])

            @pl.when((level != partner) | (k < n_grp // 2))
            def _():
                side(landed.at[source], source).wait_send()

            @pl.when((level <= z) & (z + 1 < n_z))
            def _():
                climb(landed.at[source], source).wait_send()

            @pl.when((level >= z) & (z > 0))
            def _():
                sink(landed.at[source], source).wait_send()


def chunk_body(flow_state, line_owner, *, n_tile):
    _, planes, rows, ny = flow_state.shape
    n_lines = line_owner.shape[0]
    n_blocks = n_lines // LANES
    nx = rows * n_tile
    half = nx // 2
    n_dev = 4 * n_tile
    cap = 2 * planes * ny // n_tile
    f32 = jnp.float32
    dma = pltpu.SemaphoreType.DMA
    hbm = pl.BlockSpec(memory_space=pltpu.HBM)
    padded = (half + 2 * reach, SUB, LANES)
    record = pl.pallas_call(
        functools.partial(chunk_kernel, n_tile),
        out_shape=jax.ShapeDtypeStruct((nx, cap), f32),
        in_specs=[hbm, hbm], out_specs=pl.BlockSpec(memory_space=pltpu.VMEM),
        scratch_shapes=[
            pltpu.VMEM((planes, rows, ny), f32), pltpu.VMEM((n_blocks, LANES), jnp.int32),
            pltpu.VMEM((n_dev, planes * rows, LANES), f32), pltpu.VMEM((n_dev, planes * rows, LANES), f32),
            pltpu.VMEM((4,) + padded, f32), pltpu.VMEM((3,) + padded, f32),
            pltpu.VMEM((3, half, SUB, LANES), f32), pltpu.VMEM((3, half, SUB, LANES), f32),
            pltpu.VMEM((4, nx, 2 * LANES), f32), pltpu.VMEM((n_dev, nx, 2 * LANES), f32),
            pltpu.VMEM((n_blocks, LANES), jnp.int32), pltpu.VMEM((n_blocks, LANES), jnp.int32),
            pltpu.VMEM((2 * planes, nx, LANES), f32), pltpu.VMEM((planes * LANES, 2 * LANES), f32),
            dma, dma, dma((n_dev,)), dma((n_dev,)), dma((n_dev,)), dma((4,)), dma((n_dev,)), dma((n_dev,)), dma((n_dev,)), dma((n_dev,)),
        ],
        compiler_params=pltpu.CompilerParams(has_side_effects=True, collective_id=0, vmem_limit_bytes=60 * 1024 * 1024), name="record",
    )(flow_state, line_owner.reshape(n_blocks, LANES))
    return record[None, None]


def fits_chunks(mesh, planes, rows, ny):
    n_tile = mesh.shape["tile"]
    return 2 * planes == SUB and 2 * rows == SUB and mesh.shape["grp"] == 4 and ny == 4 * n_tile * CHUNK and n_tile & (n_tile - 1) == 0 and n_tile >= 4


def solution(mesh):
    in_specs = (P("grp", None, "tile", None), P())
    out_specs = P("grp", "tile", None, None)
    n_tile = mesh.shape["tile"]

    def run(flow_state, line_owner):
        _, planes, rows, ny = flow_state.shape
        chosen = chunk_body if fits_chunks(mesh, planes, rows, ny) else tiled_body
        return chosen(flow_state, line_owner, n_tile=n_tile)

    return jax.shard_map(run, mesh=mesh, in_specs=in_specs, out_specs=out_specs, check_vma=False)
```

```python
import functools

import jax
import jax.numpy as jnp
import numpy as np
from jax import lax
from jax.experimental import pallas as pl
from jax.experimental.pallas import tpu as pltpu
from jax.sharding import PartitionSpec as P

time_step = 0.2
viscosity = 0.05
reach = 4
first_coeffs = (0.8, -0.2, 4.0 / 105.0, -1.0 / 280.0)
second_center = -205.0 / 72.0
second_coeffs = (1.6, -0.2, 8.0 / 315.0, -1.0 / 560.0)
lift_alpha = -1.586134342059924
lift_beta = -0.052980118572961
lift_gamma = 0.882911075530934
lift_delta = 0.443506852043971
lift_scale = 1.149604398860241
LANES = 128
MESH = pl.DeviceIdType.MESH


def lift_numpy(signal):
    even, odd = signal[0::2].copy(), signal[1::2].copy()
    odd += lift_alpha * (even + np.roll(even, -1, 0))
    even += lift_beta * (odd + np.roll(odd, 1, 0))
    odd += lift_gamma * (even + np.roll(even, -1, 0))
    even += lift_delta * (odd + np.roll(odd, 1, 0))
    return np.concatenate([even * lift_scale, odd / lift_scale])


def lift_matrix(length):
    return lift_numpy(np.eye(length))


def band_matrix():
    full = lift_matrix(8 * LANES)
    low = full[LANES : 2 * LANES, LANES : 5 * LANES]
    high = full[4 * LANES + LANES : 4 * LANES + 2 * LANES, LANES : 5 * LANES]
    return np.concatenate([low, high]).T.astype(np.float32)


def band_value(taps_low, taps_high):
    row = lax.broadcasted_iota(jnp.int32, (4 * LANES, 2 * LANES), 0)
    column = lax.broadcasted_iota(jnp.int32, (4 * LANES, 2 * LANES), 1)
    distance = row - LANES - 2 * (column & (LANES - 1))
    is_low = column < LANES
    value = jnp.zeros((4 * LANES, 2 * LANES), jnp.float32)
    for offset in range(-4, 5):
        tap = jnp.where(is_low, taps_low[offset + 4], taps_high[offset + 4])
        value = jnp.where(distance == offset, tap, value)
    return value


def band_taps():
    band = band_matrix()
    rows = slice(LANES + LANES // 2 - 4, LANES + LANES // 2 + 5)
    return [float(x) for x in band[rows, LANES // 4]], [float(x) for x in band[rows, LANES + LANES // 4]]


def shifted_y(value, k):
    return pltpu.roll(value, (-k) % value.shape[-1], value.ndim - 1)


def derivatives(center, shift, want_first=True, want_second=True):
    first, second = None, second_center * center if want_second else None
    for k in range(1, reach + 1):
        ahead, behind = shift(k), shift(-k)
        if want_first:
            term = first_coeffs[k - 1] * (ahead - behind)
            first = term if first is None else first + term
        if want_second:
            second = second + second_coeffs[k - 1] * (ahead + behind)
    return first, second


def slots_of(n_tile, owner_ref, place_ref, base_ref, count_ref):
    owner = owner_ref[...]
    n_blocks = owner.shape[0]
    upper = (lax.broadcasted_iota(jnp.int32, (LANES, LANES), 0) <= lax.broadcasted_iota(jnp.int32, (LANES, LANES), 1)).astype(jnp.float32)
    lower = (lax.broadcasted_iota(jnp.int32, (n_blocks, n_blocks), 0) > lax.broadcasted_iota(jnp.int32, (n_blocks, n_blocks), 1)).astype(jnp.float32)
    lane = lax.broadcasted_iota(jnp.int32, (n_blocks, LANES), 1)

    def step(s, carry):
        place, counts, ahead = carry
        mask = (owner == s).astype(jnp.float32)
        within = jnp.dot(mask, upper, preferred_element_type=jnp.float32)
        total = jnp.sum(mask, axis=1, keepdims=True)
        place = place + mask * (ahead + within - 1.0)
        counts = jnp.where(lane == s, total, counts)
        return place, counts, ahead + total

    zeros = jnp.zeros((n_blocks, LANES), jnp.float32)
    carry = (zeros, zeros, jnp.zeros((n_blocks, 1), jnp.float32))
    if n_tile <= 16:
        for s in range(n_tile):
            carry = step(s, carry)
    else:
        carry = lax.fori_loop(0, n_tile, step, carry)
    place, counts, _ = carry
    place_ref[...] = place
    count_ref[...] = counts.astype(jnp.int32)
    base_ref[...] = jnp.dot(lower, counts, preferred_element_type=jnp.float32).astype(jnp.int32)


def flow_kernel(n_tile, own_ref, owner_ref, out_ref, place_ref, base_ref, count_ref,
                fields, mids, halo, mid_halo, pad, ppad, middle, fin, along_y, along_z, lap, send_sem, recv_sem, hsend_sem, hrecv_sem, msend_sem, mrecv_sem, mhsend_sem, mhrecv_sem, relay_sem, band_ref):
    g, t = lax.axis_index("grp"), lax.axis_index("tile")
    right, left = lax.rem(t + 1, n_tile), lax.rem(t + n_tile - 1, n_tile)
    planes, rows, ny = own_ref.shape[1:]
    own = own_ref.at[0]

    barrier = pltpu.get_barrier_semaphore()
    for k in range(1, 4):
        pl.semaphore_signal(barrier, inc=1, device_id=(lax.rem(g + k, 4), t), device_id_type=MESH)
    for side in (right, left):
        pl.semaphore_signal(barrier, inc=1, device_id=(g, side), device_id_type=MESH)

    @pl.when((g == 0) | (g == 3))
    def _():
        for side in (right, left):
            pl.semaphore_signal(barrier, inc=1, device_id=(3 - g, side), device_id_type=MESH)
        pl.semaphore_wait(barrier, 7)

    @pl.when((g == 1) | (g == 2))
    def _():
        pl.semaphore_wait(barrier, 5)

    def gather_copy(src, dst, ssem, rsem, k, slot):
        return pltpu.make_async_remote_copy(
            src_ref=src, dst_ref=dst.at[slot], send_sem=ssem.at[k], recv_sem=rsem.at[slot],
            device_id=(k, t), device_id_type=MESH)

    half = planes // 2

    def whole_copy(k, slot):
        return pltpu.make_async_remote_copy(
            src_ref=own, dst_ref=fields.at[slot], send_sem=send_sem.at[k], recv_sem=recv_sem.at[slot, 0],
            device_id=(k, t), device_id_type=MESH)

    def half_copy(slot, k):
        part = pl.ds(k * half, half)
        return pltpu.make_async_remote_copy(
            src_ref=own.at[part], dst_ref=fields.at[slot, part], send_sem=send_sem.at[k],
            recv_sem=recv_sem.at[slot, k], device_id=(k, t), device_id_type=MESH)

    def relay_copy(slot, k):
        part = pl.ds(k * half, half)
        return pltpu.make_async_remote_copy(
            src_ref=fields.at[slot, part], dst_ref=fields.at[slot, part], send_sem=relay_sem.at[slot],
            recv_sem=recv_sem.at[slot, k], device_id=(1 - k, t), device_id_type=MESH)

    def halo_copy(src, dst, ssem, rsem, side, slot, group):
        return pltpu.make_async_remote_copy(
            src_ref=src, dst_ref=dst.at[slot + side], send_sem=ssem.at[side], recv_sem=rsem.at[slot + side],
            device_id=(group, right if side == 0 else left), device_id_type=MESH)

    @pl.when(g < 3)
    def _():
        for side in range(2):
            halo_copy(own, halo, hsend_sem, hrecv_sem, side, 0, g).start()

    for k in range(3):
        @pl.when((g < 2) & (g != k))
        def _(k=k):
            whole_copy(k, g).start()

    @pl.when(g >= 2)
    def _():
        for k in range(2):
            half_copy(g, k).start()

    @pl.when(g == 3)
    def _():
        whole_copy(2, 3).start()
        for side in range(2):
            halo_copy(own, halo, hsend_sem, hrecv_sem, side, 2, 0).start()

    def local_terms():
        for z in range(planes):
            center = pad[z, reach : reach + rows]
            fy, sy = derivatives(center, lambda k: shifted_y(center, k))
            fz, sz = derivatives(center, lambda k: pad[(z + k) % planes, reach : reach + rows])
            along_y[z], along_z[z], lap[z] = fy, fz, sy + sz

    slots_of(n_tile, owner_ref, place_ref, base_ref, count_ref)
    band_ref[...] = band_value(*band_taps())

    @pl.when(g < 3)
    def _():
        for k in range(3):
            @pl.when(g == k)
            def _(k=k):
                fields[k] = own_ref[0]

        for z in range(planes):
            pad[z, reach : reach + rows] = own_ref[0, z]
        local_terms()

        @pl.when(g < 2)
        def _():
            for slot in (2, 3):
                half_copy(slot, g).wait_recv()
                relay_copy(slot, g).start()
            whole_copy(0, 1 - g).wait_recv()
            for slot in (2, 3):
                half_copy(slot, 1 - g).wait_recv()

        @pl.when(g == 2)
        def _():
            for slot in (0, 1, 3):
                whole_copy(0, slot).wait_recv()

        for side in range(2):
            halo_copy(own, halo, hsend_sem, hrecv_sem, side, 0, g).wait_recv()

        @pl.when(g == 0)
        def _():
            for side in range(2):
                halo_copy(own, halo, hsend_sem, hrecv_sem, side, 2, 0).wait_recv()
            for z in range(planes):
                ppad[z, 0:reach] = halo[2, z, rows - reach : rows]
                ppad[z, reach : reach + rows] = fields[3, z]
                ppad[z, reach + rows : 2 * reach + rows] = halo[3, z, 0:reach]
            for z in range(planes):
                middle[z], _ = derivatives(None, lambda k: ppad[z, reach + k : reach + k + rows], True, False)

        @pl.when(g == 1)
        def _():
            for z in range(planes):
                value = fields[3, z]
                middle[z], _ = derivatives(None, lambda k: shifted_y(value, k), True, False)

        @pl.when(g == 2)
        def _():
            for z in range(planes):
                middle[z], _ = derivatives(None, lambda k: fields[3, (z + k) % planes], True, False)

        def tendency(z, vel, press):
            center = pad[z, reach : reach + rows]
            fx, sx = derivatives(center, lambda k: pad[z, reach + k : reach + k + rows])
            advect = vel[0, z] * fx + vel[1, z] * along_y[z] + vel[2, z] * along_z[z]
            return viscosity * (sx + lap[z]) - advect - press

        for z in range(planes):
            pad[z, 0:reach] = halo[0, z, rows - reach : rows]
            pad[z, reach + rows : 2 * reach + rows] = halo[1, z, 0:reach]
        for z in range(planes):
            press = middle[z]
            ppad[z, 0:rows] = press
        for z in range(planes):
            middle[z] = own_ref[0, z] + time_step * tendency(z, fields, ppad[z, 0:rows])

        for side in range(2):
            halo_copy(middle, mid_halo, mhsend_sem, mhrecv_sem, side, 0, g).start()
        for k in range(3):
            @pl.when(g != k)
            def _(k=k):
                gather_copy(middle, mids, msend_sem, mrecv_sem, k, g).start()

            @pl.when(g == k)
            def _(k=k):
                mids[k] = middle[...]

        for z in range(planes):
            pad[z, reach : reach + rows] = middle[z]
        local_terms()
        for k in range(3):
            @pl.when(g != k)
            def _(k=k):
                gather_copy(middle, mids, msend_sem, mrecv_sem, 0, k).wait_recv()
        for side in range(2):
            halo_copy(middle, mid_halo, mhsend_sem, mhrecv_sem, side, 0, g).wait_recv()
        for z in range(planes):
            pad[z, 0:reach] = mid_halo[0, z, rows - reach : rows]
            pad[z, reach + rows : 2 * reach + rows] = mid_halo[1, z, 0:reach]
        for z in range(planes):
            fin[z] = 0.5 * ((own_ref[0, z] + middle[z]) + time_step * tendency(z, mids, ppad[z, 0:rows]))

        blocks = ny // (2 * LANES)
        groups = ny // LANES
        for z in range(planes):
            value = fin[z]
            pieces = []
            for b in range(blocks):
                window = [value[:, ((2 * b + j) % groups) * LANES : ((2 * b + j) % groups + 1) * LANES] for j in (-1, 0, 1, 2)]
                pieces.append(jnp.concatenate(window, axis=1))
            stacked = jnp.concatenate(pieces, axis=0)
            lifted = jnp.dot(stacked, band_ref[...], precision=lax.Precision.HIGHEST, preferred_element_type=jnp.float32)
            for b in range(blocks):
                piece = lifted[b * rows : (b + 1) * rows]
                fin[z, :, b * LANES : (b + 1) * LANES] = piece[:, 0:LANES]
                fin[z, :, ny // 2 + b * LANES : ny // 2 + (b + 1) * LANES] = piece[:, LANES:]

        even = [fin[2 * i] for i in range(half)]
        odd = [fin[2 * i + 1] for i in range(half)]
        odd = [odd[i] + lift_alpha * (even[i] + even[(i + 1) % half]) for i in range(half)]
        even = [even[i] + lift_beta * (odd[i] + odd[(i - 1) % half]) for i in range(half)]
        odd = [odd[i] + lift_gamma * (even[i] + even[(i + 1) % half]) for i in range(half)]
        even = [even[i] + lift_delta * (odd[i] + odd[(i - 1) % half]) for i in range(half)]
        for i in range(half):
            out_ref[i] = even[i] * lift_scale
            out_ref[half + i] = odd[i] * (1.0 / lift_scale)

        for side in range(2):
            halo_copy(middle, mid_halo, mhsend_sem, mhrecv_sem, side, 0, g).wait_send()
        for k in range(3):
            @pl.when(g != k)
            def _(k=k):
                gather_copy(middle, mids, msend_sem, mrecv_sem, k, g).wait_send()

    @pl.when(g == 3)
    def _():
        out_ref[...] = jnp.zeros_like(out_ref)

    for side in range(2):
        halo_copy(own, halo, hsend_sem, hrecv_sem, side, 0, g).wait_send()
    for k in range(3):
        @pl.when((g < 2) & (g != k))
        def _(k=k):
            whole_copy(k, g).wait_send()

    @pl.when(g < 2)
    def _():
        for slot in (2, 3):
            relay_copy(slot, g).wait_send()

    @pl.when(g >= 2)
    def _():
        for k in range(2):
            half_copy(g, k).wait_send()

    @pl.when(g == 3)
    def _():
        whole_copy(2, 3).wait_send()


def compact_kernel(n_tile, base_ref, count_ref, coeff_ref, place_ref, out_ref, current):
    planes, rows, ny = coeff_ref.shape
    groups = ny // LANES
    out_ref[...] = jnp.zeros_like(out_ref)
    current[...] = jnp.zeros_like(current)
    rank = lax.broadcasted_iota(jnp.int32, (LANES, LANES), 0).astype(jnp.float32)
    lane = lax.broadcasted_iota(jnp.int32, (rows, LANES), 1)

    def sort(b):
        z, y = b // groups, b % groups
        value = coeff_ref[z, :, pl.ds(pl.multiple_of(y * LANES, LANES), LANES)]
        high = value.astype(jnp.bfloat16).astype(jnp.float32)
        rest = value - high
        mid = rest.astype(jnp.bfloat16).astype(jnp.float32)
        low = rest - mid
        parts = jnp.concatenate([high, mid, low], axis=0).astype(jnp.bfloat16)
        chosen = jnp.where(rank == place_ref[pl.ds(b, 1), :], 1.0, 0.0).astype(jnp.bfloat16)
        ordered = lax.dot_general(parts, chosen, (((1,), (1,)), ((), ())), preferred_element_type=jnp.float32)
        return (ordered[0:rows] + ordered[rows : 2 * rows]) + ordered[2 * rows : 3 * rows]

    def pencil(b, ordered, s, ahead):
        base, count = base_ref[b, s], count_ref[b, s]
        start = base & (LANES - 1)
        end = start + count
        turned = pltpu.roll(ordered, (start - ahead) & (LANES - 1), 1)
        now = current[s] + jnp.where((lane >= start) & (lane < end), turned, 0.0)
        group = pl.multiple_of(base - start, LANES)
        after = jnp.where(lane < end - LANES, turned, 0.0)
        current[s] = jnp.where(end >= LANES, after, now)
        out_ref[s, :, pl.ds(group, 2 * LANES)] = jnp.concatenate([now, after], axis=1)
        return ahead + count

    n_blocks = planes * groups
    batch = 8 if n_blocks % 8 == 0 and n_tile <= 16 else 1

    def blocks(i, _):
        ordered = [sort(i * batch + j) for j in range(batch)]
        for j in range(batch):
            b = i * batch + j
            if n_tile <= 16:
                ahead = jnp.int32(0)
                for s in range(n_tile):
                    ahead = pencil(b, ordered[j], s, ahead)
            else:
                lax.fori_loop(0, n_tile, lambda s, ahead: pencil(b, ordered[j], s, ahead), jnp.int32(0))
        return 0

    lax.fori_loop(0, n_blocks // batch, blocks, 0)


def record_kernel(n_tile, chunks, sent_ref, matrix_ref, out_ref, got, records, send_sem, recv_sem, rsend_sem, rrecv_sem):
    g, t = lax.axis_index("grp"), lax.axis_index("tile")
    rows, nx, cap = sent_ref.shape[1], out_ref.shape[0], out_ref.shape[1]
    width = cap // chunks

    barrier = pltpu.get_barrier_semaphore()

    @pl.when(g < 3)
    def _():
        for k in range(1, n_tile):
            pl.semaphore_signal(barrier, inc=1, device_id=(g, lax.rem(t + k, n_tile)), device_id_type=MESH)
        pl.semaphore_signal(barrier, inc=1, device_id=(3, t), device_id_type=MESH)
        pl.semaphore_wait(barrier, n_tile)

    @pl.when(g == 3)
    def _():
        for k in range(3):
            pl.semaphore_signal(barrier, inc=1, device_id=(k, t), device_id_type=MESH)
        pl.semaphore_wait(barrier, 3)

    def exchange(s, slot, c):
        part = pl.ds(c * width, width)
        return pltpu.make_async_remote_copy(
            src_ref=sent_ref.at[s, :, part], dst_ref=got.at[slot, :, part], send_sem=send_sem.at[s, c],
            recv_sem=recv_sem.at[slot, c], device_id=(g, s), device_id_type=MESH)

    def report(c, slot):
        part = pl.ds(c * width, width)
        return pltpu.make_async_remote_copy(
            src_ref=out_ref.at[:, part], dst_ref=records.at[slot, :, part], send_sem=rsend_sem.at[c],
            recv_sem=rrecv_sem.at[slot, c], device_id=(3, t), device_id_type=MESH)

    @pl.when(g < 3)
    def _():
        for c in range(chunks):
            for k in range(1, n_tile):
                exchange(lax.rem(t + k, n_tile), t, c).start()
        got[t] = sent_ref[t, :, 0:cap]
        matrix = matrix_ref[...]
        for c in range(chunks):
            for k in range(1, n_tile):
                exchange(lax.rem(t + k, n_tile), lax.rem(t + k, n_tile), c).wait_recv()
            value = got[:, :, c * width : (c + 1) * width].reshape(nx, width)
            out_ref[:, c * width : (c + 1) * width] = jnp.dot(
                matrix, value, precision=lax.Precision.HIGHEST, preferred_element_type=jnp.float32)
            report(c, g).start()
        for c in range(chunks):
            for k in range(1, n_tile):
                exchange(lax.rem(t + k, n_tile), t, c).wait_send()
            report(c, g).wait_send()

    @pl.when(g == 3)
    def _():
        for c in range(chunks):
            for k in range(3):
                report(c, k).wait_recv()
            part = slice(c * width, (c + 1) * width)
            first, second, third = records[0, :, part], records[1, :, part], records[2, :, part]
            out_ref[:, part] = first * first + second * second + third * third


def tiled_body(flow_state, line_owner, *, n_tile):
    _, planes, rows, ny = flow_state.shape
    n_lines = line_owner.shape[0]
    n_blocks = n_lines // LANES
    nx = rows * n_tile
    cap = 2 * planes * ny // n_tile
    vmem = pl.BlockSpec(memory_space=pltpu.VMEM)
    smem = pl.BlockSpec(memory_space=pltpu.SMEM)
    f32 = jnp.float32
    shape = jax.ShapeDtypeStruct
    limit = 16 * 1024 * 1024
    dma = pltpu.SemaphoreType.DMA
    owner = line_owner.reshape(n_blocks, LANES)
    tile = (planes, rows, ny)
    ints = shape((n_blocks, LANES), jnp.int32)
    coeffs, place, base, count = pl.pallas_call(
        functools.partial(flow_kernel, n_tile),
        out_shape=(shape(tile, f32), shape((n_blocks, LANES), f32), ints, ints),
        in_specs=[vmem, vmem], out_specs=(vmem, vmem, vmem, vmem),
        scratch_shapes=[
            pltpu.VMEM((4,) + tile, f32), pltpu.VMEM((3,) + tile, f32),
            pltpu.VMEM((4,) + tile, f32), pltpu.VMEM((2,) + tile, f32),
            pltpu.VMEM((planes, rows + 2 * reach, ny), f32), pltpu.VMEM((planes, rows + 2 * reach, ny), f32),
            pltpu.VMEM(tile, f32), pltpu.VMEM(tile, f32), pltpu.VMEM(tile, f32), pltpu.VMEM(tile, f32), pltpu.VMEM(tile, f32),
            dma((4,)), dma((4, 2)), dma((2,)), dma((4,)), dma((4,)), dma((4,)), dma((2,)), dma((2,)), dma((4,)),
            pltpu.VMEM((4 * LANES, 2 * LANES), f32),
        ],
        compiler_params=pltpu.CompilerParams(has_side_effects=True, collective_id=0, vmem_limit_bytes=limit), name="flow",
    )(flow_state, owner)
    sent = pl.pallas_call(
        functools.partial(compact_kernel, n_tile),
        out_shape=shape((n_tile, rows, cap + 2 * LANES), f32),
        in_specs=[smem, smem, vmem, vmem], out_specs=vmem,
        scratch_shapes=[pltpu.VMEM((n_tile, rows, LANES), f32)],
        compiler_params=pltpu.CompilerParams(vmem_limit_bytes=limit), name="compact",
    )(base, count, coeffs, place)
    chunks = 4 if cap % (4 * LANES) == 0 else 1
    record = pl.pallas_call(
        functools.partial(record_kernel, n_tile, chunks),
        out_shape=shape((nx, cap), f32),
        in_specs=[vmem, vmem], out_specs=vmem,
        scratch_shapes=[
            pltpu.VMEM((n_tile, rows, cap), f32), pltpu.VMEM((3, nx, cap), f32),
            dma((n_tile, chunks)), dma((n_tile, chunks)), dma((chunks,)), dma((3, chunks)),
        ],
        compiler_params=pltpu.CompilerParams(has_side_effects=True, collective_id=1, vmem_limit_bytes=limit), name="record",
    )(sent, jnp.asarray(lift_matrix(nx).astype(np.float32)))
    return record[None, None]


CHUNK = 64
SIDE = (LANES - CHUNK) // 2
SUB = 8


def planes_taps(planes):
    first, second = [0.0] * planes, [0.0] * planes
    second[0] = 3.0 * second_center
    for k in range(1, reach + 1):
        first[k % planes] += first_coeffs[k - 1]
        first[-k % planes] -= first_coeffs[k - 1]
        second[k % planes] += second_coeffs[k - 1]
        second[-k % planes] += second_coeffs[k - 1]
    return first, second


def column_taps():
    full = lift_matrix(8 * CHUNK)
    middle = 4 * CHUNK
    low = full[middle // 2, middle - 4 : middle + 5]
    high = full[8 * CHUNK // 2 + middle // 2, middle + 1 - 4 : middle + 1 + 5]
    return [float(x) for x in low], [float(x) for x in high]


def column_band(planes):
    taps_low, taps_high = column_taps()
    part = CHUNK // 2
    row = lax.broadcasted_iota(jnp.int32, (planes * LANES, 2 * LANES), 0)
    column = lax.broadcasted_iota(jnp.int32, (planes * LANES, 2 * LANES), 1)
    is_low = column < LANES
    spot = SIDE + 2 * (column & (part - 1)) + jnp.where(is_low, 0, 1)
    same = (row // LANES) == ((column & (LANES - 1)) // part)
    distance = jnp.where(same, (row & (LANES - 1)) - spot, LANES)
    value = jnp.zeros((planes * LANES, 2 * LANES), jnp.float32)
    for offset in range(-4, 5):
        tap = jnp.where(is_low, taps_low[offset + 4], taps_high[offset + 4])
        value = jnp.where(distance == offset, tap, value)
    return value


def pencil_slots(pencil, owner, spot_ref, group_ref):
    n_blocks = owner.shape[0]
    upper = (lax.broadcasted_iota(jnp.int32, (LANES, LANES), 0) <= lax.broadcasted_iota(jnp.int32, (LANES, LANES), 1)).astype(jnp.float32)
    lower = (lax.broadcasted_iota(jnp.int32, (n_blocks, n_blocks), 0) > lax.broadcasted_iota(jnp.int32, (n_blocks, n_blocks), 1)).astype(jnp.float32)
    lane = lax.broadcasted_iota(jnp.int32, (n_blocks, LANES), 1)
    mine = owner == pencil
    mask = mine.astype(jnp.float32)
    within = jnp.dot(mask, upper, preferred_element_type=jnp.float32)
    total = jnp.broadcast_to(jnp.sum(mask, axis=1, keepdims=True), (n_blocks, LANES))
    base = jnp.dot(lower, total, preferred_element_type=jnp.float32).astype(jnp.int32)
    slot = base + within.astype(jnp.int32) - 1
    spot_ref[...] = jnp.where(mine, slot & (LANES - 1), -1)
    group_ref[...] = base // LANES + jnp.where(lane < (base & (LANES - 1)), 1, 0)


def chunk_kernel(n_tile, own_hbm, owner_hbm, out_ref,
                 own, owner_ref, windows, arrived, fields, mids, slope, final, pieces, landed, spot_ref, group_ref, ordered, band_ref,
                 own_sem, owner_sem, send_sem, recv_sem, recv_two, hand_sem, side_sem, onward_sem):
    g, t = lax.axis_index("grp"), lax.axis_index("tile")
    planes, rows, ny = own.shape
    n_grp = 4
    n_dev = n_grp * n_tile
    nx = rows * n_tile
    half = nx // 2
    me = t * n_grp + g

    load = pltpu.make_async_copy(own_hbm.at[0], own, own_sem)
    load.start()
    load_owner = pltpu.make_async_copy(owner_hbm, owner_ref, owner_sem)
    load_owner.start()
    peers = [(lax.rem(g + k % n_grp, n_grp), lax.rem(t + k // n_grp, n_tile)) for k in range(1, n_dev)]
    barrier = pltpu.get_barrier_semaphore()
    for peer in peers:
        pl.semaphore_signal(barrier, inc=1, device_id=peer, device_id_type=MESH)
    load.wait()
    for z in range(planes):
        value = own[z]
        for odd in range(2):
            turned = pltpu.roll(value, SIDE if odd == 0 else ny - SIDE, 1)
            for m in range(n_dev // 2):
                windows[2 * m + odd, z * rows : (z + 1) * rows] = turned[:, m * LANES : (m + 1) * LANES]
    pl.semaphore_wait(barrier, n_dev - 1)

    def deal(peer, source):
        to = peer[1] * n_grp + peer[0]
        return pltpu.make_async_remote_copy(
            src_ref=windows.at[to], dst_ref=arrived.at[source], send_sem=send_sem.at[to], recv_sem=recv_sem.at[source],
            device_id=peer, device_id_type=MESH)

    for peer in peers:
        deal(peer, me).start()
    arrived[me] = windows[me]

    load_owner.wait()
    pencil_slots(t, owner_ref[...], spot_ref, group_ref)
    out_ref[...] = jnp.zeros_like(out_ref)
    band_ref[...] = column_band(planes)

    for peer in peers:
        deal(peer, peer[1] * n_grp + peer[0]).wait_recv()

    sublane = lax.broadcasted_iota(jnp.int32, (reach, SUB, LANES), 1)

    def flip(value):
        return jnp.where((sublane & 1) == 0, pltpu.roll(value, SUB - 1, 1), pltpu.roll(value, 1, 1))

    def wrap(ref, c):
        ref[c, 0:reach] = flip(ref[c, half : half + reach])
        ref[c, half + reach : half + 2 * reach] = flip(ref[c, reach : 2 * reach])

    for f in range(n_grp):
        for tile in range(n_tile):
            side, first = tile // (n_tile // 2), (tile % (n_tile // 2)) * rows
            for r in range(rows):
                fields[f, reach + first + r, pl.ds(side, planes, stride=2), :] = arrived[tile * n_grp + f, pl.ds(r, planes, stride=rows), :]
        wrap(fields, f)

    z_first, z_second = planes_taps(planes)
    step = rows

    def turn_z(value, m):
        return value if m == 0 else pltpu.roll(value, (-2 * m) % SUB, 1)

    def turn_y(value, k):
        return pltpu.roll(value, (-k) % LANES, 2)

    def gradient(i, direction):
        if direction == 0:
            shift = lambda k: fields[3, reach + i + k : reach + i + k + step]
        else:
            center = fields[3, reach + i : reach + i + step]
            if direction == 1:
                shift = lambda k: turn_y(center, k)
            else:
                total = None
                for m in range(1, planes):
                    if z_first[m] != 0.0:
                        term = z_first[m] * turn_z(center, m)
                        total = term if total is None else total + term
                return total
        value, _ = derivatives(None, shift, True, False)
        return value

    def tendency(ref, c, i, speed, press):
        center = ref[c, reach + i : reach + i + step]
        total = z_second[0] * center
        slope_z = None
        for m in range(1, planes):
            turned = turn_z(center, m)
            total = total + z_second[m] * turned
            if z_first[m] != 0.0:
                term = z_first[m] * turned
                slope_z = term if slope_z is None else slope_z + term
        slope_x, slope_y = None, None
        for k in range(1, reach + 1):
            ahead, behind = ref[c, reach + i + k : reach + i + k + step], ref[c, reach + i - k : reach + i - k + step]
            up, down = turn_y(center, k), turn_y(center, -k)
            term_x, term_y = first_coeffs[k - 1] * (ahead - behind), first_coeffs[k - 1] * (up - down)
            slope_x = term_x if slope_x is None else slope_x + term_x
            slope_y = term_y if slope_y is None else slope_y + term_y
            total = total + second_coeffs[k - 1] * ((ahead + behind) + (up + down))
        advect = speed[0] * slope_x + speed[1] * slope_y + speed[2] * slope_z
        return viscosity * total - advect - press, center

    def first_section(b, _):
        i = b * step
        speed = [fields[f, reach + i : reach + i + step] if isinstance(i, int) else fields[f, pl.ds(reach + i, step)] for f in range(3)]
        for c in range(3):
            press = gradient(i, c)
            slope[c, i : i + step] = press
            change, center = tendency(fields, c, i, speed, press)
            mids[c, reach + i : reach + i + step] = center + time_step * change
        return 0

    def second_section(b, _):
        i = b * step
        speed = [mids[f, reach + i : reach + i + step] for f in range(3)]
        for c in range(3):
            change, center = tendency(mids, c, i, speed, slope[c, i : i + step])
            final[c, i : i + step] = 0.5 * ((fields[c, reach + i : reach + i + step] + center) + time_step * change)
        return 0

    for b in range(half // step):
        first_section(b, 0)
    for c in range(3):
        wrap(mids, c)
    for b in range(half // step):
        second_section(b, 0)

    flat = lax.broadcasted_iota(jnp.int32, (SUB, LANES), 0)

    def flip_one(value):
        return jnp.where((flat & 1) == 0, pltpu.roll(value, SUB - 1, 0), pltpu.roll(value, 1, 0))

    matrix = lift_matrix(planes)
    z_coeffs = []
    for m in range(planes):
        column = jnp.zeros((SUB, LANES), jnp.float32)
        for z in range(planes):
            column = jnp.where(flat // 2 == z, float(matrix[z, (z + m) % planes]), column)
        z_coeffs.append(column)

    def lift_z(value):
        total = z_coeffs[0] * value
        for m in range(1, planes):
            total = total + z_coeffs[m] * pltpu.roll(value, (-2 * m) % SUB, 0)
        return total

    pairs = half // 2
    for c in range(3):
        even = [lift_z(final[c, 2 * i]) for i in range(pairs)]
        odd = [lift_z(final[c, 2 * i + 1]) for i in range(pairs)]
        for odd_tap, even_tap in ((lift_alpha, lift_beta), (lift_gamma, lift_delta)):
            after = even[1:] + [flip_one(even[0])]
            odd = [odd[i] + odd_tap * (even[i] + after[i]) for i in range(pairs)]
            before = [flip_one(odd[-1])] + odd[:-1]
            even = [even[i] + even_tap * (odd[i] + before[i]) for i in range(pairs)]
        for i in range(pairs):
            final[c, i] = even[i] * lift_scale
            final[c, pairs + i] = odd[i] * (1.0 / lift_scale)

    stacked = []
    for c in range(3):
        flat_ref = final.at[c].reshape(half * SUB, LANES)
        for high in range(2):
            for a in range(2):
                stacked.append(jnp.concatenate([flat_ref[pl.ds(high * pairs * SUB + 2 * z + a, pairs, stride=SUB), :] for z in range(planes)], axis=1))
    lines = jnp.dot(jnp.concatenate(stacked, axis=0), band_ref[...], precision=lax.Precision.HIGHEST, preferred_element_type=jnp.float32)
    lines = [lines[c * nx : (c + 1) * nx] for c in range(3)]
    lines.append(lines[0] * lines[0] + lines[1] * lines[1] + lines[2] * lines[2])
    for c in range(n_grp):
        pieces[c] = lines[c]

    z, y = t // 2, t % 2
    n_z = n_tile // 2

    def flipped(value, bits):
        result, place = 0, 1
        while place < n_z:
            result = result + place * lax.rem(value // place + bits // place, 2)
            place *= 2
        return result

    partner = flipped(z, 1)

    def source_of(level, column, group):
        return (level * 2 + column) * n_grp + group

    def send(origin, source, sem, group, level, column):
        return pltpu.make_async_remote_copy(
            src_ref=origin, dst_ref=landed.at[source], send_sem=sem, recv_sem=recv_two.at[source],
            device_id=(group, level * 2 + column), device_id_type=MESH)

    kin = [g, g + 1 - 2 * lax.rem(g, 2), lax.rem(g + 2, n_grp), n_grp - 1 - g]
    across = (0, 2, 3, 1)
    routes = ((3, 0), (0, 1), (0, 0), (1, 0))

    def hand(bits, other, k):
        group = kin[k]
        return send(pieces.at[group], me, hand_sem.at[bits + 2 * other, k], group, flipped(z, bits), lax.rem(y + other, 2))

    def side(source):
        return send(landed.at[source], source, side_sem.at[source], g, z, 1 - y)

    def onward(source):
        return send(landed.at[source], source, onward_sem.at[source], g, partner, y)

    def await_piece(source):
        send(pieces.at[g], source, hand_sem.at[0, 0], g, z, 1 - y).wait_recv()

    for bits, other in routes:
        for k in across:
            if bits or other or k:
                hand(bits, other, k).start()
    landed[me] = pieces[g]

    def sideways(bits, k):
        return bits > 0 and not (bits == 1 and k >= n_grp // 2)

    for bits in (3, 0, 1, 2):
        for k in across:
            source = source_of(flipped(z, bits), y, kin[k])
            if bits or k:
                await_piece(source)
            if bits == 3:
                onward(source).start()
            if sideways(bits, k):
                side(source).start()
        if bits == 0:
            for k in across:
                source = source_of(z, 1 - y, kin[k])
                await_piece(source)
                if k >= n_grp // 2:
                    onward(source).start()

    rank = lax.broadcasted_iota(jnp.int32, (LANES, LANES), 0)
    n_groups = n_tile
    lane_part = lax.broadcasted_iota(jnp.int32, (nx, LANES), 1) // (CHUNK // 2)

    def select(tile):
        for high in range(2):
            tiles = [landed[tile * n_grp + m, :, high * LANES : (high + 1) * LANES] for m in range(4)]
            for bit in range(2):
                distance = (CHUNK // 2) << bit
                is_low = (lane_part & (1 << bit)) == 0
                turned = list(tiles)
                for m in range(4):
                    if not m & (1 << bit):
                        other = m | (1 << bit)
                        turned[m] = jnp.where(is_low, tiles[m], pltpu.roll(tiles[other], distance, 1))
                        turned[other] = jnp.where(is_low, pltpu.roll(tiles[m], LANES - distance, 1), tiles[other])
                tiles = turned
            for plane in range(planes):
                block = (plane * 2 + high) * n_groups + tile
                value = tiles[plane]
                first = value.astype(jnp.bfloat16).astype(jnp.float32)
                rest = value - first
                second = rest.astype(jnp.bfloat16).astype(jnp.float32)
                stack = jnp.concatenate([first, second, rest - second], axis=0).astype(jnp.bfloat16)
                chosen = jnp.where(rank == spot_ref[pl.ds(block, 1), :], 1.0, 0.0).astype(jnp.bfloat16)
                placed = lax.dot_general(stack, chosen, (((1,), (1,)), ((), ())), preferred_element_type=jnp.float32)
                ordered[plane * 2 + high] = (placed[0:nx] + placed[nx : 2 * nx]) + placed[2 * nx : 3 * nx]
        labels = [group_ref[pl.ds((plane * 2 + high) * n_groups + tile, 1), :] for plane in range(planes) for high in range(2)]
        for q in range(out_ref.shape[1] // LANES):
            total = out_ref[:, q * LANES : (q + 1) * LANES]
            for n, label in enumerate(labels):
                total = total + jnp.where(label == q, ordered[n], 0.0)
            out_ref[:, q * LANES : (q + 1) * LANES] = total

    def own_column(k, _):
        select(flipped(z, k) * 2 + y)
        return 0

    lax.fori_loop(0, n_z, own_column, 0)
    select(z * 2 + 1 - y)

    def other_column(k, _):
        level = flipped(z, k)
        for group in range(n_grp):
            await_piece(source_of(level, 1 - y, group))
        select(level * 2 + 1 - y)
        return 0

    lax.fori_loop(1, n_z, other_column, 0)

    for peer in peers:
        deal(peer, me).wait_send()
    for bits, other in routes:
        for k in across:
            if bits or other or k:
                hand(bits, other, k).wait_send()
    for k in across:
        for bits in range(1, n_z):
            source = source_of(flipped(z, bits), y, kin[k])
            if sideways(bits, k):
                side(source).wait_send()
        onward(source_of(flipped(z, 3), y, kin[k])).wait_send()
        if k >= n_grp // 2:
            onward(source_of(z, 1 - y, kin[k])).wait_send()


def chunk_body(flow_state, line_owner, *, n_tile):
    _, planes, rows, ny = flow_state.shape
    n_lines = line_owner.shape[0]
    n_blocks = n_lines // LANES
    nx = rows * n_tile
    half = nx // 2
    n_dev = 4 * n_tile
    cap = 2 * planes * ny // n_tile
    f32 = jnp.float32
    dma = pltpu.SemaphoreType.DMA
    hbm = pl.BlockSpec(memory_space=pltpu.HBM)
    padded = (half + 2 * reach, SUB, LANES)
    record = pl.pallas_call(
        functools.partial(chunk_kernel, n_tile),
        out_shape=jax.ShapeDtypeStruct((nx, cap), f32),
        in_specs=[hbm, hbm], out_specs=pl.BlockSpec(memory_space=pltpu.VMEM),
        scratch_shapes=[
            pltpu.VMEM((planes, rows, ny), f32), pltpu.VMEM((n_blocks, LANES), jnp.int32),
            pltpu.VMEM((n_dev, planes * rows, LANES), f32), pltpu.VMEM((n_dev, planes * rows, LANES), f32),
            pltpu.VMEM((4,) + padded, f32), pltpu.VMEM((3,) + padded, f32),
            pltpu.VMEM((3, half, SUB, LANES), f32), pltpu.VMEM((3, half, SUB, LANES), f32),
            pltpu.VMEM((4, nx, 2 * LANES), f32), pltpu.VMEM((n_dev, nx, 2 * LANES), f32),
            pltpu.VMEM((n_blocks, LANES), jnp.int32), pltpu.VMEM((n_blocks, LANES), jnp.int32),
            pltpu.VMEM((2 * planes, nx, LANES), f32), pltpu.VMEM((planes * LANES, 2 * LANES), f32),
            dma, dma, dma((n_dev,)), dma((n_dev,)), dma((n_dev,)), dma((4, 4)), dma((n_dev,)), dma((n_dev,)),
        ],
        compiler_params=pltpu.CompilerParams(has_side_effects=True, collective_id=0, vmem_limit_bytes=16 * 1024 * 1024), name="record",
    )(pltpu.with_memory_space_constraint(flow_state, pltpu.HBM), pltpu.with_memory_space_constraint(line_owner.reshape(n_blocks, LANES), pltpu.HBM))
    return record[None, None]


def fits_chunks(mesh, planes, rows, ny):
    n_tile = mesh.shape["tile"]
    return 2 * planes == SUB and 2 * rows == SUB and mesh.shape["grp"] == 4 and ny == 4 * n_tile * CHUNK and n_tile == 8


def solution(mesh):
    in_specs = (P("grp", None, "tile", None), P())
    out_specs = P("grp", "tile", None, None)
    n_tile = mesh.shape["tile"]

    def run(flow_state, line_owner):
        _, planes, rows, ny = flow_state.shape
        chosen = chunk_body if fits_chunks(mesh, planes, rows, ny) else tiled_body
        return chosen(flow_state, line_owner, n_tile=n_tile)

    return jax.shard_map(run, mesh=mesh, in_specs=in_specs, out_specs=out_specs, check_vma=False)
```

```python
import functools

import jax
import jax.numpy as jnp
import numpy as np
from jax import lax
from jax.experimental import pallas as pl
from jax.experimental.pallas import tpu as pltpu
from jax.sharding import PartitionSpec as P

time_step = 0.2
viscosity = 0.05
reach = 4
first_coeffs = (0.8, -0.2, 4.0 / 105.0, -1.0 / 280.0)
second_center = -205.0 / 72.0
second_coeffs = (1.6, -0.2, 8.0 / 315.0, -1.0 / 560.0)
lift_alpha = -1.586134342059924
lift_beta = -0.052980118572961
lift_gamma = 0.882911075530934
lift_delta = 0.443506852043971
lift_scale = 1.149604398860241
LANES = 128
MESH = pl.DeviceIdType.MESH


def lift_numpy(signal):
    even, odd = signal[0::2].copy(), signal[1::2].copy()
    odd += lift_alpha * (even + np.roll(even, -1, 0))
    even += lift_beta * (odd + np.roll(odd, 1, 0))
    odd += lift_gamma * (even + np.roll(even, -1, 0))
    even += lift_delta * (odd + np.roll(odd, 1, 0))
    return np.concatenate([even * lift_scale, odd / lift_scale])


def lift_matrix(length):
    return lift_numpy(np.eye(length))


def band_matrix():
    full = lift_matrix(8 * LANES)
    low = full[LANES : 2 * LANES, LANES : 5 * LANES]
    high = full[4 * LANES + LANES : 4 * LANES + 2 * LANES, LANES : 5 * LANES]
    return np.concatenate([low, high]).T.astype(np.float32)


def band_value(taps_low, taps_high):
    row = lax.broadcasted_iota(jnp.int32, (4 * LANES, 2 * LANES), 0)
    column = lax.broadcasted_iota(jnp.int32, (4 * LANES, 2 * LANES), 1)
    distance = row - LANES - 2 * (column & (LANES - 1))
    is_low = column < LANES
    value = jnp.zeros((4 * LANES, 2 * LANES), jnp.float32)
    for offset in range(-4, 5):
        tap = jnp.where(is_low, taps_low[offset + 4], taps_high[offset + 4])
        value = jnp.where(distance == offset, tap, value)
    return value


def band_taps():
    band = band_matrix()
    rows = slice(LANES + LANES // 2 - 4, LANES + LANES // 2 + 5)
    return [float(x) for x in band[rows, LANES // 4]], [float(x) for x in band[rows, LANES + LANES // 4]]


def shifted_y(value, k):
    return pltpu.roll(value, (-k) % value.shape[-1], value.ndim - 1)


def derivatives(center, shift, want_first=True, want_second=True):
    first, second = None, second_center * center if want_second else None
    for k in range(1, reach + 1):
        ahead, behind = shift(k), shift(-k)
        if want_first:
            term = first_coeffs[k - 1] * (ahead - behind)
            first = term if first is None else first + term
        if want_second:
            second = second + second_coeffs[k - 1] * (ahead + behind)
    return first, second


def slots_of(n_tile, owner_ref, place_ref, base_ref, count_ref):
    owner = owner_ref[...]
    n_blocks = owner.shape[0]
    upper = (lax.broadcasted_iota(jnp.int32, (LANES, LANES), 0) <= lax.broadcasted_iota(jnp.int32, (LANES, LANES), 1)).astype(jnp.float32)
    lower = (lax.broadcasted_iota(jnp.int32, (n_blocks, n_blocks), 0) > lax.broadcasted_iota(jnp.int32, (n_blocks, n_blocks), 1)).astype(jnp.float32)
    lane = lax.broadcasted_iota(jnp.int32, (n_blocks, LANES), 1)

    def step(s, carry):
        place, counts, ahead = carry
        mask = (owner == s).astype(jnp.float32)
        within = jnp.dot(mask, upper, preferred_element_type=jnp.float32)
        total = jnp.sum(mask, axis=1, keepdims=True)
        place = place + mask * (ahead + within - 1.0)
        counts = jnp.where(lane == s, total, counts)
        return place, counts, ahead + total

    zeros = jnp.zeros((n_blocks, LANES), jnp.float32)
    carry = (zeros, zeros, jnp.zeros((n_blocks, 1), jnp.float32))
    if n_tile <= 16:
        for s in range(n_tile):
            carry = step(s, carry)
    else:
        carry = lax.fori_loop(0, n_tile, step, carry)
    place, counts, _ = carry
    place_ref[...] = place
    count_ref[...] = counts.astype(jnp.int32)
    base_ref[...] = jnp.dot(lower, counts, preferred_element_type=jnp.float32).astype(jnp.int32)


def flow_kernel(n_tile, own_ref, owner_ref, out_ref, place_ref, base_ref, count_ref,
                fields, mids, halo, mid_halo, pad, ppad, middle, fin, along_y, along_z, lap, send_sem, recv_sem, hsend_sem, hrecv_sem, msend_sem, mrecv_sem, mhsend_sem, mhrecv_sem, relay_sem, band_ref):
    g, t = lax.axis_index("grp"), lax.axis_index("tile")
    right, left = lax.rem(t + 1, n_tile), lax.rem(t + n_tile - 1, n_tile)
    planes, rows, ny = own_ref.shape[1:]
    own = own_ref.at[0]

    barrier = pltpu.get_barrier_semaphore()
    for k in range(1, 4):
        pl.semaphore_signal(barrier, inc=1, device_id=(lax.rem(g + k, 4), t), device_id_type=MESH)
    for side in (right, left):
        pl.semaphore_signal(barrier, inc=1, device_id=(g, side), device_id_type=MESH)

    @pl.when((g == 0) | (g == 3))
    def _():
        for side in (right, left):
            pl.semaphore_signal(barrier, inc=1, device_id=(3 - g, side), device_id_type=MESH)
        pl.semaphore_wait(barrier, 7)

    @pl.when((g == 1) | (g == 2))
    def _():
        pl.semaphore_wait(barrier, 5)

    def gather_copy(src, dst, ssem, rsem, k, slot):
        return pltpu.make_async_remote_copy(
            src_ref=src, dst_ref=dst.at[slot], send_sem=ssem.at[k], recv_sem=rsem.at[slot],
            device_id=(k, t), device_id_type=MESH)

    half = planes // 2

    def whole_copy(k, slot):
        return pltpu.make_async_remote_copy(
            src_ref=own, dst_ref=fields.at[slot], send_sem=send_sem.at[k], recv_sem=recv_sem.at[slot, 0],
            device_id=(k, t), device_id_type=MESH)

    def half_copy(slot, k):
        part = pl.ds(k * half, half)
        return pltpu.make_async_remote_copy(
            src_ref=own.at[part], dst_ref=fields.at[slot, part], send_sem=send_sem.at[k],
            recv_sem=recv_sem.at[slot, k], device_id=(k, t), device_id_type=MESH)

    def relay_copy(slot, k):
        part = pl.ds(k * half, half)
        return pltpu.make_async_remote_copy(
            src_ref=fields.at[slot, part], dst_ref=fields.at[slot, part], send_sem=relay_sem.at[slot],
            recv_sem=recv_sem.at[slot, k], device_id=(1 - k, t), device_id_type=MESH)

    def halo_copy(src, dst, ssem, rsem, side, slot, group):
        return pltpu.make_async_remote_copy(
            src_ref=src, dst_ref=dst.at[slot + side], send_sem=ssem.at[side], recv_sem=rsem.at[slot + side],
            device_id=(group, right if side == 0 else left), device_id_type=MESH)

    @pl.when(g < 3)
    def _():
        for side in range(2):
            halo_copy(own, halo, hsend_sem, hrecv_sem, side, 0, g).start()

    for k in range(3):
        @pl.when((g < 2) & (g != k))
        def _(k=k):
            whole_copy(k, g).start()

    @pl.when(g >= 2)
    def _():
        for k in range(2):
            half_copy(g, k).start()

    @pl.when(g == 3)
    def _():
        whole_copy(2, 3).start()
        for side in range(2):
            halo_copy(own, halo, hsend_sem, hrecv_sem, side, 2, 0).start()

    def local_terms():
        for z in range(planes):
            center = pad[z, reach : reach + rows]
            fy, sy = derivatives(center, lambda k: shifted_y(center, k))
            fz, sz = derivatives(center, lambda k: pad[(z + k) % planes, reach : reach + rows])
            along_y[z], along_z[z], lap[z] = fy, fz, sy + sz

    slots_of(n_tile, owner_ref, place_ref, base_ref, count_ref)
    band_ref[...] = band_value(*band_taps())

    @pl.when(g < 3)
    def _():
        for k in range(3):
            @pl.when(g == k)
            def _(k=k):
                fields[k] = own_ref[0]

        for z in range(planes):
            pad[z, reach : reach + rows] = own_ref[0, z]
        local_terms()

        @pl.when(g < 2)
        def _():
            for slot in (2, 3):
                half_copy(slot, g).wait_recv()
                relay_copy(slot, g).start()
            whole_copy(0, 1 - g).wait_recv()
            for slot in (2, 3):
                half_copy(slot, 1 - g).wait_recv()

        @pl.when(g == 2)
        def _():
            for slot in (0, 1, 3):
                whole_copy(0, slot).wait_recv()

        for side in range(2):
            halo_copy(own, halo, hsend_sem, hrecv_sem, side, 0, g).wait_recv()

        @pl.when(g == 0)
        def _():
            for side in range(2):
                halo_copy(own, halo, hsend_sem, hrecv_sem, side, 2, 0).wait_recv()
            for z in range(planes):
                ppad[z, 0:reach] = halo[2, z, rows - reach : rows]
                ppad[z, reach : reach + rows] = fields[3, z]
                ppad[z, reach + rows : 2 * reach + rows] = halo[3, z, 0:reach]
            for z in range(planes):
                middle[z], _ = derivatives(None, lambda k: ppad[z, reach + k : reach + k + rows], True, False)

        @pl.when(g == 1)
        def _():
            for z in range(planes):
                value = fields[3, z]
                middle[z], _ = derivatives(None, lambda k: shifted_y(value, k), True, False)

        @pl.when(g == 2)
        def _():
            for z in range(planes):
                middle[z], _ = derivatives(None, lambda k: fields[3, (z + k) % planes], True, False)

        def tendency(z, vel, press):
            center = pad[z, reach : reach + rows]
            fx, sx = derivatives(center, lambda k: pad[z, reach + k : reach + k + rows])
            advect = vel[0, z] * fx + vel[1, z] * along_y[z] + vel[2, z] * along_z[z]
            return viscosity * (sx + lap[z]) - advect - press

        for z in range(planes):
            pad[z, 0:reach] = halo[0, z, rows - reach : rows]
            pad[z, reach + rows : 2 * reach + rows] = halo[1, z, 0:reach]
        for z in range(planes):
            press = middle[z]
            ppad[z, 0:rows] = press
        for z in range(planes):
            middle[z] = own_ref[0, z] + time_step * tendency(z, fields, ppad[z, 0:rows])

        for side in range(2):
            halo_copy(middle, mid_halo, mhsend_sem, mhrecv_sem, side, 0, g).start()
        for k in range(3):
            @pl.when(g != k)
            def _(k=k):
                gather_copy(middle, mids, msend_sem, mrecv_sem, k, g).start()

            @pl.when(g == k)
            def _(k=k):
                mids[k] = middle[...]

        for z in range(planes):
            pad[z, reach : reach + rows] = middle[z]
        local_terms()
        for k in range(3):
            @pl.when(g != k)
            def _(k=k):
                gather_copy(middle, mids, msend_sem, mrecv_sem, 0, k).wait_recv()
        for side in range(2):
            halo_copy(middle, mid_halo, mhsend_sem, mhrecv_sem, side, 0, g).wait_recv()
        for z in range(planes):
            pad[z, 0:reach] = mid_halo[0, z, rows - reach : rows]
            pad[z, reach + rows : 2 * reach + rows] = mid_halo[1, z, 0:reach]
        for z in range(planes):
            fin[z] = 0.5 * ((own_ref[0, z] + middle[z]) + time_step * tendency(z, mids, ppad[z, 0:rows]))

        blocks = ny // (2 * LANES)
        groups = ny // LANES
        for z in range(planes):
            value = fin[z]
            pieces = []
            for b in range(blocks):
                window = [value[:, ((2 * b + j) % groups) * LANES : ((2 * b + j) % groups + 1) * LANES] for j in (-1, 0, 1, 2)]
                pieces.append(jnp.concatenate(window, axis=1))
            stacked = jnp.concatenate(pieces, axis=0)
            lifted = jnp.dot(stacked, band_ref[...], precision=lax.Precision.HIGHEST, preferred_element_type=jnp.float32)
            for b in range(blocks):
                piece = lifted[b * rows : (b + 1) * rows]
                fin[z, :, b * LANES : (b + 1) * LANES] = piece[:, 0:LANES]
                fin[z, :, ny // 2 + b * LANES : ny // 2 + (b + 1) * LANES] = piece[:, LANES:]

        even = [fin[2 * i] for i in range(half)]
        odd = [fin[2 * i + 1] for i in range(half)]
        odd = [odd[i] + lift_alpha * (even[i] + even[(i + 1) % half]) for i in range(half)]
        even = [even[i] + lift_beta * (odd[i] + odd[(i - 1) % half]) for i in range(half)]
        odd = [odd[i] + lift_gamma * (even[i] + even[(i + 1) % half]) for i in range(half)]
        even = [even[i] + lift_delta * (odd[i] + odd[(i - 1) % half]) for i in range(half)]
        for i in range(half):
            out_ref[i] = even[i] * lift_scale
            out_ref[half + i] = odd[i] * (1.0 / lift_scale)

        for side in range(2):
            halo_copy(middle, mid_halo, mhsend_sem, mhrecv_sem, side, 0, g).wait_send()
        for k in range(3):
            @pl.when(g != k)
            def _(k=k):
                gather_copy(middle, mids, msend_sem, mrecv_sem, k, g).wait_send()

    @pl.when(g == 3)
    def _():
        out_ref[...] = jnp.zeros_like(out_ref)

    for side in range(2):
        halo_copy(own, halo, hsend_sem, hrecv_sem, side, 0, g).wait_send()
    for k in range(3):
        @pl.when((g < 2) & (g != k))
        def _(k=k):
            whole_copy(k, g).wait_send()

    @pl.when(g < 2)
    def _():
        for slot in (2, 3):
            relay_copy(slot, g).wait_send()

    @pl.when(g >= 2)
    def _():
        for k in range(2):
            half_copy(g, k).wait_send()

    @pl.when(g == 3)
    def _():
        whole_copy(2, 3).wait_send()


def compact_kernel(n_tile, base_ref, count_ref, coeff_ref, place_ref, out_ref, current):
    planes, rows, ny = coeff_ref.shape
    groups = ny // LANES
    out_ref[...] = jnp.zeros_like(out_ref)
    current[...] = jnp.zeros_like(current)
    rank = lax.broadcasted_iota(jnp.int32, (LANES, LANES), 0).astype(jnp.float32)
    lane = lax.broadcasted_iota(jnp.int32, (rows, LANES), 1)

    def sort(b):
        z, y = b // groups, b % groups
        value = coeff_ref[z, :, pl.ds(pl.multiple_of(y * LANES, LANES), LANES)]
        high = value.astype(jnp.bfloat16).astype(jnp.float32)
        rest = value - high
        mid = rest.astype(jnp.bfloat16).astype(jnp.float32)
        low = rest - mid
        parts = jnp.concatenate([high, mid, low], axis=0).astype(jnp.bfloat16)
        chosen = jnp.where(rank == place_ref[pl.ds(b, 1), :], 1.0, 0.0).astype(jnp.bfloat16)
        ordered = lax.dot_general(parts, chosen, (((1,), (1,)), ((), ())), preferred_element_type=jnp.float32)
        return (ordered[0:rows] + ordered[rows : 2 * rows]) + ordered[2 * rows : 3 * rows]

    def pencil(b, ordered, s, ahead):
        base, count = base_ref[b, s], count_ref[b, s]
        start = base & (LANES - 1)
        end = start + count
        turned = pltpu.roll(ordered, (start - ahead) & (LANES - 1), 1)
        now = current[s] + jnp.where((lane >= start) & (lane < end), turned, 0.0)
        group = pl.multiple_of(base - start, LANES)
        after = jnp.where(lane < end - LANES, turned, 0.0)
        current[s] = jnp.where(end >= LANES, after, now)
        out_ref[s, :, pl.ds(group, 2 * LANES)] = jnp.concatenate([now, after], axis=1)
        return ahead + count

    n_blocks = planes * groups
    batch = 8 if n_blocks % 8 == 0 and n_tile <= 16 else 1

    def blocks(i, _):
        ordered = [sort(i * batch + j) for j in range(batch)]
        for j in range(batch):
            b = i * batch + j
            if n_tile <= 16:
                ahead = jnp.int32(0)
                for s in range(n_tile):
                    ahead = pencil(b, ordered[j], s, ahead)
            else:
                lax.fori_loop(0, n_tile, lambda s, ahead: pencil(b, ordered[j], s, ahead), jnp.int32(0))
        return 0

    lax.fori_loop(0, n_blocks // batch, blocks, 0)


def record_kernel(n_tile, chunks, sent_ref, matrix_ref, out_ref, got, records, send_sem, recv_sem, rsend_sem, rrecv_sem):
    g, t = lax.axis_index("grp"), lax.axis_index("tile")
    rows, nx, cap = sent_ref.shape[1], out_ref.shape[0], out_ref.shape[1]
    width = cap // chunks

    barrier = pltpu.get_barrier_semaphore()

    @pl.when(g < 3)
    def _():
        for k in range(1, n_tile):
            pl.semaphore_signal(barrier, inc=1, device_id=(g, lax.rem(t + k, n_tile)), device_id_type=MESH)
        pl.semaphore_signal(barrier, inc=1, device_id=(3, t), device_id_type=MESH)
        pl.semaphore_wait(barrier, n_tile)

    @pl.when(g == 3)
    def _():
        for k in range(3):
            pl.semaphore_signal(barrier, inc=1, device_id=(k, t), device_id_type=MESH)
        pl.semaphore_wait(barrier, 3)

    def exchange(s, slot, c):
        part = pl.ds(c * width, width)
        return pltpu.make_async_remote_copy(
            src_ref=sent_ref.at[s, :, part], dst_ref=got.at[slot, :, part], send_sem=send_sem.at[s, c],
            recv_sem=recv_sem.at[slot, c], device_id=(g, s), device_id_type=MESH)

    def report(c, slot):
        part = pl.ds(c * width, width)
        return pltpu.make_async_remote_copy(
            src_ref=out_ref.at[:, part], dst_ref=records.at[slot, :, part], send_sem=rsend_sem.at[c],
            recv_sem=rrecv_sem.at[slot, c], device_id=(3, t), device_id_type=MESH)

    @pl.when(g < 3)
    def _():
        for c in range(chunks):
            for k in range(1, n_tile):
                exchange(lax.rem(t + k, n_tile), t, c).start()
        got[t] = sent_ref[t, :, 0:cap]
        matrix = matrix_ref[...]
        for c in range(chunks):
            for k in range(1, n_tile):
                exchange(lax.rem(t + k, n_tile), lax.rem(t + k, n_tile), c).wait_recv()
            value = got[:, :, c * width : (c + 1) * width].reshape(nx, width)
            out_ref[:, c * width : (c + 1) * width] = jnp.dot(
                matrix, value, precision=lax.Precision.HIGHEST, preferred_element_type=jnp.float32)
            report(c, g).start()
        for c in range(chunks):
            for k in range(1, n_tile):
                exchange(lax.rem(t + k, n_tile), t, c).wait_send()
            report(c, g).wait_send()

    @pl.when(g == 3)
    def _():
        for c in range(chunks):
            for k in range(3):
                report(c, k).wait_recv()
            part = slice(c * width, (c + 1) * width)
            first, second, third = records[0, :, part], records[1, :, part], records[2, :, part]
            out_ref[:, part] = first * first + second * second + third * third


def tiled_body(flow_state, line_owner, *, n_tile):
    _, planes, rows, ny = flow_state.shape
    n_lines = line_owner.shape[0]
    n_blocks = n_lines // LANES
    nx = rows * n_tile
    cap = 2 * planes * ny // n_tile
    vmem = pl.BlockSpec(memory_space=pltpu.VMEM)
    smem = pl.BlockSpec(memory_space=pltpu.SMEM)
    f32 = jnp.float32
    shape = jax.ShapeDtypeStruct
    limit = 16 * 1024 * 1024
    dma = pltpu.SemaphoreType.DMA
    owner = line_owner.reshape(n_blocks, LANES)
    tile = (planes, rows, ny)
    ints = shape((n_blocks, LANES), jnp.int32)
    coeffs, place, base, count = pl.pallas_call(
        functools.partial(flow_kernel, n_tile),
        out_shape=(shape(tile, f32), shape((n_blocks, LANES), f32), ints, ints),
        in_specs=[vmem, vmem], out_specs=(vmem, vmem, vmem, vmem),
        scratch_shapes=[
            pltpu.VMEM((4,) + tile, f32), pltpu.VMEM((3,) + tile, f32),
            pltpu.VMEM((4,) + tile, f32), pltpu.VMEM((2,) + tile, f32),
            pltpu.VMEM((planes, rows + 2 * reach, ny), f32), pltpu.VMEM((planes, rows + 2 * reach, ny), f32),
            pltpu.VMEM(tile, f32), pltpu.VMEM(tile, f32), pltpu.VMEM(tile, f32), pltpu.VMEM(tile, f32), pltpu.VMEM(tile, f32),
            dma((4,)), dma((4, 2)), dma((2,)), dma((4,)), dma((4,)), dma((4,)), dma((2,)), dma((2,)), dma((4,)),
            pltpu.VMEM((4 * LANES, 2 * LANES), f32),
        ],
        compiler_params=pltpu.CompilerParams(has_side_effects=True, collective_id=0, vmem_limit_bytes=limit), name="flow",
    )(flow_state, owner)
    sent = pl.pallas_call(
        functools.partial(compact_kernel, n_tile),
        out_shape=shape((n_tile, rows, cap + 2 * LANES), f32),
        in_specs=[smem, smem, vmem, vmem], out_specs=vmem,
        scratch_shapes=[pltpu.VMEM((n_tile, rows, LANES), f32)],
        compiler_params=pltpu.CompilerParams(vmem_limit_bytes=limit), name="compact",
    )(base, count, coeffs, place)
    chunks = 4 if cap % (4 * LANES) == 0 else 1
    record = pl.pallas_call(
        functools.partial(record_kernel, n_tile, chunks),
        out_shape=shape((nx, cap), f32),
        in_specs=[vmem, vmem], out_specs=vmem,
        scratch_shapes=[
            pltpu.VMEM((n_tile, rows, cap), f32), pltpu.VMEM((3, nx, cap), f32),
            dma((n_tile, chunks)), dma((n_tile, chunks)), dma((chunks,)), dma((3, chunks)),
        ],
        compiler_params=pltpu.CompilerParams(has_side_effects=True, collective_id=1, vmem_limit_bytes=limit), name="record",
    )(sent, jnp.asarray(lift_matrix(nx).astype(np.float32)))
    return record[None, None]


CHUNK = 64
SIDE = (LANES - CHUNK) // 2
SUB = 8


def planes_taps(planes):
    first, second = [0.0] * planes, [0.0] * planes
    second[0] = 3.0 * second_center
    for k in range(1, reach + 1):
        first[k % planes] += first_coeffs[k - 1]
        first[-k % planes] -= first_coeffs[k - 1]
        second[k % planes] += second_coeffs[k - 1]
        second[-k % planes] += second_coeffs[k - 1]
    return first, second


def column_taps():
    full = lift_matrix(8 * CHUNK)
    middle = 4 * CHUNK
    low = full[middle // 2, middle - 4 : middle + 5]
    high = full[8 * CHUNK // 2 + middle // 2, middle + 1 - 4 : middle + 1 + 5]
    return [float(x) for x in low], [float(x) for x in high]


def column_band(planes):
    taps_low, taps_high = column_taps()
    part = CHUNK // 2
    row = lax.broadcasted_iota(jnp.int32, (planes * LANES, 2 * LANES), 0)
    column = lax.broadcasted_iota(jnp.int32, (planes * LANES, 2 * LANES), 1)
    is_low = column < LANES
    spot = SIDE + 2 * (column & (part - 1)) + jnp.where(is_low, 0, 1)
    same = (row // LANES) == ((column & (LANES - 1)) // part)
    distance = jnp.where(same, (row & (LANES - 1)) - spot, LANES)
    value = jnp.zeros((planes * LANES, 2 * LANES), jnp.float32)
    for offset in range(-4, 5):
        tap = jnp.where(is_low, taps_low[offset + 4], taps_high[offset + 4])
        value = jnp.where(distance == offset, tap, value)
    return value


def pencil_slots(pencil, owner, spot_ref, group_ref):
    n_blocks = owner.shape[0]
    upper = (lax.broadcasted_iota(jnp.int32, (LANES, LANES), 0) <= lax.broadcasted_iota(jnp.int32, (LANES, LANES), 1)).astype(jnp.float32)
    lower = (lax.broadcasted_iota(jnp.int32, (n_blocks, n_blocks), 0) > lax.broadcasted_iota(jnp.int32, (n_blocks, n_blocks), 1)).astype(jnp.float32)
    lane = lax.broadcasted_iota(jnp.int32, (n_blocks, LANES), 1)
    mine = owner == pencil
    mask = mine.astype(jnp.float32)
    within = jnp.dot(mask, upper, preferred_element_type=jnp.float32)
    total = jnp.broadcast_to(jnp.sum(mask, axis=1, keepdims=True), (n_blocks, LANES))
    base = jnp.dot(lower, total, preferred_element_type=jnp.float32).astype(jnp.int32)
    slot = base + within.astype(jnp.int32) - 1
    spot_ref[...] = jnp.where(mine, slot & (LANES - 1), -1)
    group_ref[...] = base // LANES + jnp.where(lane < (base & (LANES - 1)), 1, 0)


def chunk_kernel(n_tile, own_hbm, owner_hbm, out_ref,
                 own, owner_ref, windows, arrived, fields, mids, slope, final, pieces, landed, spot_ref, group_ref, ordered, band_ref,
                 own_sem, owner_sem, send_sem, recv_sem, recv_two, hand_sem, side_sem, onward_sem):
    g, t = lax.axis_index("grp"), lax.axis_index("tile")
    planes, rows, ny = own.shape
    n_grp = 4
    n_dev = n_grp * n_tile
    nx = rows * n_tile
    half = nx // 2
    me = t * n_grp + g

    load = pltpu.make_async_copy(own_hbm.at[0], own, own_sem)
    load.start()
    load_owner = pltpu.make_async_copy(owner_hbm, owner_ref, owner_sem)
    load_owner.start()
    peers = [(lax.rem(g + k % n_grp, n_grp), lax.rem(t + k // n_grp, n_tile)) for k in range(1, n_dev)]
    barrier = pltpu.get_barrier_semaphore()
    for peer in peers:
        pl.semaphore_signal(barrier, inc=1, device_id=peer, device_id_type=MESH)
    load.wait()
    for z in range(planes):
        value = own[z]
        for odd in range(2):
            turned = pltpu.roll(value, SIDE if odd == 0 else ny - SIDE, 1)
            for m in range(n_dev // 2):
                windows[2 * m + odd, z * rows : (z + 1) * rows] = turned[:, m * LANES : (m + 1) * LANES]
    pl.semaphore_wait(barrier, n_dev - 1)

    def deal(peer, source):
        to = peer[1] * n_grp + peer[0]
        return pltpu.make_async_remote_copy(
            src_ref=windows.at[to], dst_ref=arrived.at[source], send_sem=send_sem.at[to], recv_sem=recv_sem.at[source],
            device_id=peer, device_id_type=MESH)

    for peer in peers:
        deal(peer, me).start()
    arrived[me] = windows[me]

    load_owner.wait()
    pencil_slots(t, owner_ref[...], spot_ref, group_ref)
    out_ref[...] = jnp.zeros_like(out_ref)
    band_ref[...] = column_band(planes)

    for peer in peers:
        deal(peer, peer[1] * n_grp + peer[0]).wait_recv()

    sublane = lax.broadcasted_iota(jnp.int32, (reach, SUB, LANES), 1)

    def flip(value):
        return jnp.where((sublane & 1) == 0, pltpu.roll(value, SUB - 1, 1), pltpu.roll(value, 1, 1))

    def wrap(ref, c):
        ref[c, 0:reach] = flip(ref[c, half : half + reach])
        ref[c, half + reach : half + 2 * reach] = flip(ref[c, reach : 2 * reach])

    for f in range(n_grp):
        for tile in range(n_tile):
            side, first = tile // (n_tile // 2), (tile % (n_tile // 2)) * rows
            for r in range(rows):
                fields[f, reach + first + r, pl.ds(side, planes, stride=2), :] = arrived[tile * n_grp + f, pl.ds(r, planes, stride=rows), :]
        wrap(fields, f)

    z_first, z_second = planes_taps(planes)
    step = rows

    def turn_z(value, m):
        return value if m == 0 else pltpu.roll(value, (-2 * m) % SUB, 1)

    def turn_y(value, k):
        return pltpu.roll(value, (-k) % LANES, 2)

    def gradient(i, direction):
        if direction == 0:
            shift = lambda k: fields[3, reach + i + k : reach + i + k + step]
        else:
            center = fields[3, reach + i : reach + i + step]
            if direction == 1:
                shift = lambda k: turn_y(center, k)
            else:
                total = None
                for m in range(1, planes):
                    if z_first[m] != 0.0:
                        term = z_first[m] * turn_z(center, m)
                        total = term if total is None else total + term
                return total
        value, _ = derivatives(None, shift, True, False)
        return value

    def tendency(ref, c, i, speed, press):
        center = ref[c, reach + i : reach + i + step]
        total = z_second[0] * center
        slope_z = None
        for m in range(1, planes):
            turned = turn_z(center, m)
            total = total + z_second[m] * turned
            if z_first[m] != 0.0:
                term = z_first[m] * turned
                slope_z = term if slope_z is None else slope_z + term
        slope_x, slope_y = None, None
        for k in range(1, reach + 1):
            ahead, behind = ref[c, reach + i + k : reach + i + k + step], ref[c, reach + i - k : reach + i - k + step]
            up, down = turn_y(center, k), turn_y(center, -k)
            term_x, term_y = first_coeffs[k - 1] * (ahead - behind), first_coeffs[k - 1] * (up - down)
            slope_x = term_x if slope_x is None else slope_x + term_x
            slope_y = term_y if slope_y is None else slope_y + term_y
            total = total + second_coeffs[k - 1] * ((ahead + behind) + (up + down))
        advect = speed[0] * slope_x + speed[1] * slope_y + speed[2] * slope_z
        return viscosity * total - advect - press, center

    def first_section(b, _):
        i = b * step
        speed = [fields[f, reach + i : reach + i + step] if isinstance(i, int) else fields[f, pl.ds(reach + i, step)] for f in range(3)]
        for c in range(3):
            press = gradient(i, c)
            slope[c, i : i + step] = press
            change, center = tendency(fields, c, i, speed, press)
            mids[c, reach + i : reach + i + step] = center + time_step * change
        return 0

    def second_section(b, c):
        i = b * step
        speed = [mids[f, reach + i : reach + i + step] for f in range(3)]
        change, center = tendency(mids, c, i, speed, slope[c, i : i + step])
        final[c, i : i + step] = 0.5 * ((fields[c, reach + i : reach + i + step] + center) + time_step * change)

    for b in range(half // step):
        first_section(b, 0)
    for c in range(3):
        wrap(mids, c)
    flat = lax.broadcasted_iota(jnp.int32, (SUB, LANES), 0)

    def flip_one(value):
        return jnp.where((flat & 1) == 0, pltpu.roll(value, SUB - 1, 0), pltpu.roll(value, 1, 0))

    matrix = lift_matrix(planes)
    z_coeffs = []
    for m in range(planes):
        column = jnp.zeros((SUB, LANES), jnp.float32)
        for z in range(planes):
            column = jnp.where(flat // 2 == z, float(matrix[z, (z + m) % planes]), column)
        z_coeffs.append(column)

    def lift_z(value):
        total = z_coeffs[0] * value
        for m in range(1, planes):
            total = total + z_coeffs[m] * pltpu.roll(value, (-2 * m) % SUB, 0)
        return total

    pairs = half // 2
    z, y = t // 2, t % 2
    n_z = n_tile // 2

    def flipped(value, bits):
        result, place = 0, 1
        while place < n_z:
            result = result + place * lax.rem(value // place + bits // place, 2)
            place *= 2
        return result

    partner = flipped(z, 1)

    def source_of(level, column, group):
        return (level * 2 + column) * n_grp + group

    def send(origin, source, sem, group, level, column):
        return pltpu.make_async_remote_copy(
            src_ref=origin, dst_ref=landed.at[source], send_sem=sem, recv_sem=recv_two.at[source],
            device_id=(group, level * 2 + column), device_id_type=MESH)

    kin = [g, g + 1 - 2 * lax.rem(g, 2), lax.rem(g + 2, n_grp), n_grp - 1 - g]
    across = (0, 2, 3, 1)
    routes = ((3, 0), (0, 1), (0, 0), (1, 0))

    def hand(bits, other, c):
        return send(pieces.at[c], me, hand_sem.at[bits + 2 * other, c], c, flipped(z, bits), lax.rem(y + other, 2))

    def each_hand(c, act):
        for bits, other in routes:
            if bits or other:
                act(hand(bits, other, c))
            else:
                @pl.when(g != c)
                def _():
                    act(hand(bits, other, c))

    def side(source):
        return send(landed.at[source], source, side_sem.at[source], g, z, 1 - y)

    def onward(source):
        return send(landed.at[source], source, onward_sem.at[source], g, partner, y)

    def await_piece(source):
        send(pieces.at[g], source, hand_sem.at[0, 0], g, z, 1 - y).wait_recv()

    def finish(c):
        even = [lift_z(final[c, 2 * i]) for i in range(pairs)]
        odd = [lift_z(final[c, 2 * i + 1]) for i in range(pairs)]
        for odd_tap, even_tap in ((lift_alpha, lift_beta), (lift_gamma, lift_delta)):
            after = even[1:] + [flip_one(even[0])]
            odd = [odd[i] + odd_tap * (even[i] + after[i]) for i in range(pairs)]
            before = [flip_one(odd[-1])] + odd[:-1]
            even = [even[i] + even_tap * (odd[i] + before[i]) for i in range(pairs)]
        for i in range(pairs):
            final[c, i] = even[i] * lift_scale
            final[c, pairs + i] = odd[i] * (1.0 / lift_scale)
        flat_ref = final.at[c].reshape(half * SUB, LANES)
        stacked = []
        for high in range(2):
            for a in range(2):
                stacked.append(jnp.concatenate([flat_ref[pl.ds(high * pairs * SUB + 2 * z_at + a, pairs, stride=SUB), :] for z_at in range(planes)], axis=1))
        lines = jnp.dot(jnp.concatenate(stacked, axis=0), band_ref[...], precision=lax.Precision.HIGHEST, preferred_element_type=jnp.float32)
        pieces[c] = lines

    for c in (0, 2, 1):
        for b in range(half // step):
            second_section(b, c)
        finish(c)
        each_hand(c, lambda copy: copy.start())
    pieces[3] = pieces[0] * pieces[0] + pieces[1] * pieces[1] + pieces[2] * pieces[2]
    each_hand(3, lambda copy: copy.start())
    rank = lax.broadcasted_iota(jnp.int32, (LANES, LANES), 0)
    n_groups = n_tile
    lane_part = lax.broadcasted_iota(jnp.int32, (nx, LANES), 1) // (CHUNK // 2)

    def select(tile):
        for high in range(2):
            tiles = [landed[tile * n_grp + m, :, high * LANES : (high + 1) * LANES] for m in range(4)]
            for bit in range(2):
                distance = (CHUNK // 2) << bit
                is_low = (lane_part & (1 << bit)) == 0
                turned = list(tiles)
                for m in range(4):
                    if not m & (1 << bit):
                        other = m | (1 << bit)
                        turned[m] = jnp.where(is_low, tiles[m], pltpu.roll(tiles[other], distance, 1))
                        turned[other] = jnp.where(is_low, pltpu.roll(tiles[m], LANES - distance, 1), tiles[other])
                tiles = turned
            for plane in range(planes):
                block = (plane * 2 + high) * n_groups + tile
                value = tiles[plane]
                first = value.astype(jnp.bfloat16).astype(jnp.float32)
                rest = value - first
                second = rest.astype(jnp.bfloat16).astype(jnp.float32)
                stack = jnp.concatenate([first, second, rest - second], axis=0).astype(jnp.bfloat16)
                chosen = jnp.where(rank == spot_ref[pl.ds(block, 1), :], 1.0, 0.0).astype(jnp.bfloat16)
                placed = lax.dot_general(stack, chosen, (((1,), (1,)), ((), ())), preferred_element_type=jnp.float32)
                ordered[plane * 2 + high] = (placed[0:nx] + placed[nx : 2 * nx]) + placed[2 * nx : 3 * nx]
        labels = [group_ref[pl.ds((plane * 2 + high) * n_groups + tile, 1), :] for plane in range(planes) for high in range(2)]
        for q in range(out_ref.shape[1] // LANES):
            total = out_ref[:, q * LANES : (q + 1) * LANES]
            for n, label in enumerate(labels):
                total = total + jnp.where(label == q, ordered[n], 0.0)
            out_ref[:, q * LANES : (q + 1) * LANES] = total

    landed[me] = pieces[g]

    def sideways(bits, k):
        return bits > 0 and not (bits == 1 and k >= n_grp // 2)

    def receive(bits):
        for k in across:
            source = source_of(flipped(z, bits), y, kin[k])
            if bits or k:
                await_piece(source)
            if bits == 3:
                onward(source).start()
            if sideways(bits, k):
                side(source).start()
        if bits == 0:
            for k in across:
                source = source_of(z, 1 - y, kin[k])
                await_piece(source)
                if k >= n_grp // 2:
                    onward(source).start()

    for bits in (3, 0, 1):
        receive(bits)

    def from_other(bits):
        for k in across:
            await_piece(source_of(flipped(z, bits), 1 - y, kin[k]))

    def pick(bits, other):
        select(flipped(z, bits) * 2 + lax.rem(y + other, 2))

    pick(0, 0)
    receive(2)
    pick(0, 1)
    pick(1, 0)
    pick(3, 0)
    pick(2, 0)
    for bits in (3, 1, 2):
        from_other(bits)
        pick(bits, 1)

    for peer in peers:
        deal(peer, me).wait_send()
    for c in range(n_grp):
        each_hand(c, lambda copy: copy.wait_send())
    for k in across:
        for bits in range(1, n_z):
            source = source_of(flipped(z, bits), y, kin[k])
            if sideways(bits, k):
                side(source).wait_send()
        onward(source_of(flipped(z, 3), y, kin[k])).wait_send()
        if k >= n_grp // 2:
            onward(source_of(z, 1 - y, kin[k])).wait_send()


def chunk_body(flow_state, line_owner, *, n_tile):
    _, planes, rows, ny = flow_state.shape
    n_lines = line_owner.shape[0]
    n_blocks = n_lines // LANES
    nx = rows * n_tile
    half = nx // 2
    n_dev = 4 * n_tile
    cap = 2 * planes * ny // n_tile
    f32 = jnp.float32
    dma = pltpu.SemaphoreType.DMA
    hbm = pl.BlockSpec(memory_space=pltpu.HBM)
    padded = (half + 2 * reach, SUB, LANES)
    record = pl.pallas_call(
        functools.partial(chunk_kernel, n_tile),
        out_shape=jax.ShapeDtypeStruct((nx, cap), f32),
        in_specs=[hbm, hbm], out_specs=pl.BlockSpec(memory_space=pltpu.VMEM),
        scratch_shapes=[
            pltpu.VMEM((planes, rows, ny), f32), pltpu.VMEM((n_blocks, LANES), jnp.int32),
            pltpu.VMEM((n_dev, planes * rows, LANES), f32), pltpu.VMEM((n_dev, planes * rows, LANES), f32),
            pltpu.VMEM((4,) + padded, f32), pltpu.VMEM((3,) + padded, f32),
            pltpu.VMEM((3, half, SUB, LANES), f32), pltpu.VMEM((3, half, SUB, LANES), f32),
            pltpu.VMEM((4, nx, 2 * LANES), f32), pltpu.VMEM((n_dev, nx, 2 * LANES), f32),
            pltpu.VMEM((n_blocks, LANES), jnp.int32), pltpu.VMEM((n_blocks, LANES), jnp.int32),
            pltpu.VMEM((2 * planes, nx, LANES), f32), pltpu.VMEM((planes * LANES, 2 * LANES), f32),
            dma, dma, dma((n_dev,)), dma((n_dev,)), dma((n_dev,)), dma((4, 4)), dma((n_dev,)), dma((n_dev,)),
        ],
        compiler_params=pltpu.CompilerParams(has_side_effects=True, collective_id=0, vmem_limit_bytes=16 * 1024 * 1024), name="record",
    )(pltpu.with_memory_space_constraint(flow_state, pltpu.HBM), pltpu.with_memory_space_constraint(line_owner.reshape(n_blocks, LANES), pltpu.HBM))
    return record[None, None]


def fits_chunks(mesh, planes, rows, ny):
    n_tile = mesh.shape["tile"]
    return 2 * planes == SUB and 2 * rows == SUB and mesh.shape["grp"] == 4 and ny == 4 * n_tile * CHUNK and n_tile == 8


def solution(mesh):
    in_specs = (P("grp", None, "tile", None), P())
    out_specs = P("grp", "tile", None, None)
    n_tile = mesh.shape["tile"]

    def run(flow_state, line_owner):
        _, planes, rows, ny = flow_state.shape
        chosen = chunk_body if fits_chunks(mesh, planes, rows, ny) else tiled_body
        return chosen(flow_state, line_owner, n_tile=n_tile)

    return jax.shard_map(run, mesh=mesh, in_specs=in_specs, out_specs=out_specs, check_vma=False)
```

```python
import functools

import jax
import jax.numpy as jnp
import numpy as np
from jax import lax
from jax.experimental import pallas as pl
from jax.experimental.pallas import tpu as pltpu
from jax.sharding import PartitionSpec as P

time_step = 0.2
viscosity = 0.05
reach = 4
first_coeffs = (0.8, -0.2, 4.0 / 105.0, -1.0 / 280.0)
second_center = -205.0 / 72.0
second_coeffs = (1.6, -0.2, 8.0 / 315.0, -1.0 / 560.0)
lift_alpha = -1.586134342059924
lift_beta = -0.052980118572961
lift_gamma = 0.882911075530934
lift_delta = 0.443506852043971
lift_scale = 1.149604398860241
LANES = 128
MESH = pl.DeviceIdType.MESH


def lift_numpy(signal):
    even, odd = signal[0::2].copy(), signal[1::2].copy()
    odd += lift_alpha * (even + np.roll(even, -1, 0))
    even += lift_beta * (odd + np.roll(odd, 1, 0))
    odd += lift_gamma * (even + np.roll(even, -1, 0))
    even += lift_delta * (odd + np.roll(odd, 1, 0))
    return np.concatenate([even * lift_scale, odd / lift_scale])


def lift_matrix(length):
    return lift_numpy(np.eye(length))


def band_matrix():
    full = lift_matrix(8 * LANES)
    low = full[LANES : 2 * LANES, LANES : 5 * LANES]
    high = full[4 * LANES + LANES : 4 * LANES + 2 * LANES, LANES : 5 * LANES]
    return np.concatenate([low, high]).T.astype(np.float32)


def band_value(taps_low, taps_high):
    row = lax.broadcasted_iota(jnp.int32, (4 * LANES, 2 * LANES), 0)
    column = lax.broadcasted_iota(jnp.int32, (4 * LANES, 2 * LANES), 1)
    distance = row - LANES - 2 * (column & (LANES - 1))
    is_low = column < LANES
    value = jnp.zeros((4 * LANES, 2 * LANES), jnp.float32)
    for offset in range(-4, 5):
        tap = jnp.where(is_low, taps_low[offset + 4], taps_high[offset + 4])
        value = jnp.where(distance == offset, tap, value)
    return value


def band_taps():
    band = band_matrix()
    rows = slice(LANES + LANES // 2 - 4, LANES + LANES // 2 + 5)
    return [float(x) for x in band[rows, LANES // 4]], [float(x) for x in band[rows, LANES + LANES // 4]]


def shifted_y(value, k):
    return pltpu.roll(value, (-k) % value.shape[-1], value.ndim - 1)


def derivatives(center, shift, want_first=True, want_second=True):
    first, second = None, second_center * center if want_second else None
    for k in range(1, reach + 1):
        ahead, behind = shift(k), shift(-k)
        if want_first:
            term = first_coeffs[k - 1] * (ahead - behind)
            first = term if first is None else first + term
        if want_second:
            second = second + second_coeffs[k - 1] * (ahead + behind)
    return first, second


def slots_of(n_tile, owner_ref, place_ref, base_ref, count_ref):
    owner = owner_ref[...]
    n_blocks = owner.shape[0]
    upper = (lax.broadcasted_iota(jnp.int32, (LANES, LANES), 0) <= lax.broadcasted_iota(jnp.int32, (LANES, LANES), 1)).astype(jnp.float32)
    lower = (lax.broadcasted_iota(jnp.int32, (n_blocks, n_blocks), 0) > lax.broadcasted_iota(jnp.int32, (n_blocks, n_blocks), 1)).astype(jnp.float32)
    lane = lax.broadcasted_iota(jnp.int32, (n_blocks, LANES), 1)

    def step(s, carry):
        place, counts, ahead = carry
        mask = (owner == s).astype(jnp.float32)
        within = jnp.dot(mask, upper, preferred_element_type=jnp.float32)
        total = jnp.sum(mask, axis=1, keepdims=True)
        place = place + mask * (ahead + within - 1.0)
        counts = jnp.where(lane == s, total, counts)
        return place, counts, ahead + total

    zeros = jnp.zeros((n_blocks, LANES), jnp.float32)
    carry = (zeros, zeros, jnp.zeros((n_blocks, 1), jnp.float32))
    if n_tile <= 16:
        for s in range(n_tile):
            carry = step(s, carry)
    else:
        carry = lax.fori_loop(0, n_tile, step, carry)
    place, counts, _ = carry
    place_ref[...] = place
    count_ref[...] = counts.astype(jnp.int32)
    base_ref[...] = jnp.dot(lower, counts, preferred_element_type=jnp.float32).astype(jnp.int32)


def flow_kernel(n_tile, own_ref, owner_ref, out_ref, place_ref, base_ref, count_ref,
                fields, mids, halo, mid_halo, pad, ppad, middle, fin, along_y, along_z, lap, send_sem, recv_sem, hsend_sem, hrecv_sem, msend_sem, mrecv_sem, mhsend_sem, mhrecv_sem, relay_sem, band_ref):
    g, t = lax.axis_index("grp"), lax.axis_index("tile")
    right, left = lax.rem(t + 1, n_tile), lax.rem(t + n_tile - 1, n_tile)
    planes, rows, ny = own_ref.shape[1:]
    own = own_ref.at[0]

    barrier = pltpu.get_barrier_semaphore()
    for k in range(1, 4):
        pl.semaphore_signal(barrier, inc=1, device_id=(lax.rem(g + k, 4), t), device_id_type=MESH)
    for side in (right, left):
        pl.semaphore_signal(barrier, inc=1, device_id=(g, side), device_id_type=MESH)

    @pl.when((g == 0) | (g == 3))
    def _():
        for side in (right, left):
            pl.semaphore_signal(barrier, inc=1, device_id=(3 - g, side), device_id_type=MESH)
        pl.semaphore_wait(barrier, 7)

    @pl.when((g == 1) | (g == 2))
    def _():
        pl.semaphore_wait(barrier, 5)

    def gather_copy(src, dst, ssem, rsem, k, slot):
        return pltpu.make_async_remote_copy(
            src_ref=src, dst_ref=dst.at[slot], send_sem=ssem.at[k], recv_sem=rsem.at[slot],
            device_id=(k, t), device_id_type=MESH)

    half = planes // 2

    def whole_copy(k, slot):
        return pltpu.make_async_remote_copy(
            src_ref=own, dst_ref=fields.at[slot], send_sem=send_sem.at[k], recv_sem=recv_sem.at[slot, 0],
            device_id=(k, t), device_id_type=MESH)

    def half_copy(slot, k):
        part = pl.ds(k * half, half)
        return pltpu.make_async_remote_copy(
            src_ref=own.at[part], dst_ref=fields.at[slot, part], send_sem=send_sem.at[k],
            recv_sem=recv_sem.at[slot, k], device_id=(k, t), device_id_type=MESH)

    def relay_copy(slot, k):
        part = pl.ds(k * half, half)
        return pltpu.make_async_remote_copy(
            src_ref=fields.at[slot, part], dst_ref=fields.at[slot, part], send_sem=relay_sem.at[slot],
            recv_sem=recv_sem.at[slot, k], device_id=(1 - k, t), device_id_type=MESH)

    def halo_copy(src, dst, ssem, rsem, side, slot, group):
        return pltpu.make_async_remote_copy(
            src_ref=src, dst_ref=dst.at[slot + side], send_sem=ssem.at[side], recv_sem=rsem.at[slot + side],
            device_id=(group, right if side == 0 else left), device_id_type=MESH)

    @pl.when(g < 3)
    def _():
        for side in range(2):
            halo_copy(own, halo, hsend_sem, hrecv_sem, side, 0, g).start()

    for k in range(3):
        @pl.when((g < 2) & (g != k))
        def _(k=k):
            whole_copy(k, g).start()

    @pl.when(g >= 2)
    def _():
        for k in range(2):
            half_copy(g, k).start()

    @pl.when(g == 3)
    def _():
        whole_copy(2, 3).start()
        for side in range(2):
            halo_copy(own, halo, hsend_sem, hrecv_sem, side, 2, 0).start()

    def local_terms():
        for z in range(planes):
            center = pad[z, reach : reach + rows]
            fy, sy = derivatives(center, lambda k: shifted_y(center, k))
            fz, sz = derivatives(center, lambda k: pad[(z + k) % planes, reach : reach + rows])
            along_y[z], along_z[z], lap[z] = fy, fz, sy + sz

    slots_of(n_tile, owner_ref, place_ref, base_ref, count_ref)
    band_ref[...] = band_value(*band_taps())

    @pl.when(g < 3)
    def _():
        for k in range(3):
            @pl.when(g == k)
            def _(k=k):
                fields[k] = own_ref[0]

        for z in range(planes):
            pad[z, reach : reach + rows] = own_ref[0, z]
        local_terms()

        @pl.when(g < 2)
        def _():
            for slot in (2, 3):
                half_copy(slot, g).wait_recv()
                relay_copy(slot, g).start()
            whole_copy(0, 1 - g).wait_recv()
            for slot in (2, 3):
                half_copy(slot, 1 - g).wait_recv()

        @pl.when(g == 2)
        def _():
            for slot in (0, 1, 3):
                whole_copy(0, slot).wait_recv()

        for side in range(2):
            halo_copy(own, halo, hsend_sem, hrecv_sem, side, 0, g).wait_recv()

        @pl.when(g == 0)
        def _():
            for side in range(2):
                halo_copy(own, halo, hsend_sem, hrecv_sem, side, 2, 0).wait_recv()
            for z in range(planes):
                ppad[z, 0:reach] = halo[2, z, rows - reach : rows]
                ppad[z, reach : reach + rows] = fields[3, z]
                ppad[z, reach + rows : 2 * reach + rows] = halo[3, z, 0:reach]
            for z in range(planes):
                middle[z], _ = derivatives(None, lambda k: ppad[z, reach + k : reach + k + rows], True, False)

        @pl.when(g == 1)
        def _():
            for z in range(planes):
                value = fields[3, z]
                middle[z], _ = derivatives(None, lambda k: shifted_y(value, k), True, False)

        @pl.when(g == 2)
        def _():
            for z in range(planes):
                middle[z], _ = derivatives(None, lambda k: fields[3, (z + k) % planes], True, False)

        def tendency(z, vel, press):
            center = pad[z, reach : reach + rows]
            fx, sx = derivatives(center, lambda k: pad[z, reach + k : reach + k + rows])
            advect = vel[0, z] * fx + vel[1, z] * along_y[z] + vel[2, z] * along_z[z]
            return viscosity * (sx + lap[z]) - advect - press

        for z in range(planes):
            pad[z, 0:reach] = halo[0, z, rows - reach : rows]
            pad[z, reach + rows : 2 * reach + rows] = halo[1, z, 0:reach]
        for z in range(planes):
            press = middle[z]
            ppad[z, 0:rows] = press
        for z in range(planes):
            middle[z] = own_ref[0, z] + time_step * tendency(z, fields, ppad[z, 0:rows])

        for side in range(2):
            halo_copy(middle, mid_halo, mhsend_sem, mhrecv_sem, side, 0, g).start()
        for k in range(3):
            @pl.when(g != k)
            def _(k=k):
                gather_copy(middle, mids, msend_sem, mrecv_sem, k, g).start()

            @pl.when(g == k)
            def _(k=k):
                mids[k] = middle[...]

        for z in range(planes):
            pad[z, reach : reach + rows] = middle[z]
        local_terms()
        for k in range(3):
            @pl.when(g != k)
            def _(k=k):
                gather_copy(middle, mids, msend_sem, mrecv_sem, 0, k).wait_recv()
        for side in range(2):
            halo_copy(middle, mid_halo, mhsend_sem, mhrecv_sem, side, 0, g).wait_recv()
        for z in range(planes):
            pad[z, 0:reach] = mid_halo[0, z, rows - reach : rows]
            pad[z, reach + rows : 2 * reach + rows] = mid_halo[1, z, 0:reach]
        for z in range(planes):
            fin[z] = 0.5 * ((own_ref[0, z] + middle[z]) + time_step * tendency(z, mids, ppad[z, 0:rows]))

        blocks = ny // (2 * LANES)
        groups = ny // LANES
        for z in range(planes):
            value = fin[z]
            pieces = []
            for b in range(blocks):
                window = [value[:, ((2 * b + j) % groups) * LANES : ((2 * b + j) % groups + 1) * LANES] for j in (-1, 0, 1, 2)]
                pieces.append(jnp.concatenate(window, axis=1))
            stacked = jnp.concatenate(pieces, axis=0)
            lifted = jnp.dot(stacked, band_ref[...], precision=lax.Precision.HIGHEST, preferred_element_type=jnp.float32)
            for b in range(blocks):
                piece = lifted[b * rows : (b + 1) * rows]
                fin[z, :, b * LANES : (b + 1) * LANES] = piece[:, 0:LANES]
                fin[z, :, ny // 2 + b * LANES : ny // 2 + (b + 1) * LANES] = piece[:, LANES:]

        even = [fin[2 * i] for i in range(half)]
        odd = [fin[2 * i + 1] for i in range(half)]
        odd = [odd[i] + lift_alpha * (even[i] + even[(i + 1) % half]) for i in range(half)]
        even = [even[i] + lift_beta * (odd[i] + odd[(i - 1) % half]) for i in range(half)]
        odd = [odd[i] + lift_gamma * (even[i] + even[(i + 1) % half]) for i in range(half)]
        even = [even[i] + lift_delta * (odd[i] + odd[(i - 1) % half]) for i in range(half)]
        for i in range(half):
            out_ref[i] = even[i] * lift_scale
            out_ref[half + i] = odd[i] * (1.0 / lift_scale)

        for side in range(2):
            halo_copy(middle, mid_halo, mhsend_sem, mhrecv_sem, side, 0, g).wait_send()
        for k in range(3):
            @pl.when(g != k)
            def _(k=k):
                gather_copy(middle, mids, msend_sem, mrecv_sem, k, g).wait_send()

    @pl.when(g == 3)
    def _():
        out_ref[...] = jnp.zeros_like(out_ref)

    for side in range(2):
        halo_copy(own, halo, hsend_sem, hrecv_sem, side, 0, g).wait_send()
    for k in range(3):
        @pl.when((g < 2) & (g != k))
        def _(k=k):
            whole_copy(k, g).wait_send()

    @pl.when(g < 2)
    def _():
        for slot in (2, 3):
            relay_copy(slot, g).wait_send()

    @pl.when(g >= 2)
    def _():
        for k in range(2):
            half_copy(g, k).wait_send()

    @pl.when(g == 3)
    def _():
        whole_copy(2, 3).wait_send()


def compact_kernel(n_tile, base_ref, count_ref, coeff_ref, place_ref, out_ref, current):
    planes, rows, ny = coeff_ref.shape
    groups = ny // LANES
    out_ref[...] = jnp.zeros_like(out_ref)
    current[...] = jnp.zeros_like(current)
    rank = lax.broadcasted_iota(jnp.int32, (LANES, LANES), 0).astype(jnp.float32)
    lane = lax.broadcasted_iota(jnp.int32, (rows, LANES), 1)

    def sort(b):
        z, y = b // groups, b % groups
        value = coeff_ref[z, :, pl.ds(pl.multiple_of(y * LANES, LANES), LANES)]
        high = value.astype(jnp.bfloat16).astype(jnp.float32)
        rest = value - high
        mid = rest.astype(jnp.bfloat16).astype(jnp.float32)
        low = rest - mid
        parts = jnp.concatenate([high, mid, low], axis=0).astype(jnp.bfloat16)
        chosen = jnp.where(rank == place_ref[pl.ds(b, 1), :], 1.0, 0.0).astype(jnp.bfloat16)
        ordered = lax.dot_general(parts, chosen, (((1,), (1,)), ((), ())), preferred_element_type=jnp.float32)
        return (ordered[0:rows] + ordered[rows : 2 * rows]) + ordered[2 * rows : 3 * rows]

    def pencil(b, ordered, s, ahead):
        base, count = base_ref[b, s], count_ref[b, s]
        start = base & (LANES - 1)
        end = start + count
        turned = pltpu.roll(ordered, (start - ahead) & (LANES - 1), 1)
        now = current[s] + jnp.where((lane >= start) & (lane < end), turned, 0.0)
        group = pl.multiple_of(base - start, LANES)
        after = jnp.where(lane < end - LANES, turned, 0.0)
        current[s] = jnp.where(end >= LANES, after, now)
        out_ref[s, :, pl.ds(group, 2 * LANES)] = jnp.concatenate([now, after], axis=1)
        return ahead + count

    n_blocks = planes * groups
    batch = 8 if n_blocks % 8 == 0 and n_tile <= 16 else 1

    def blocks(i, _):
        ordered = [sort(i * batch + j) for j in range(batch)]
        for j in range(batch):
            b = i * batch + j
            if n_tile <= 16:
                ahead = jnp.int32(0)
                for s in range(n_tile):
                    ahead = pencil(b, ordered[j], s, ahead)
            else:
                lax.fori_loop(0, n_tile, lambda s, ahead: pencil(b, ordered[j], s, ahead), jnp.int32(0))
        return 0

    lax.fori_loop(0, n_blocks // batch, blocks, 0)


def record_kernel(n_tile, chunks, sent_ref, matrix_ref, out_ref, got, records, send_sem, recv_sem, rsend_sem, rrecv_sem):
    g, t = lax.axis_index("grp"), lax.axis_index("tile")
    rows, nx, cap = sent_ref.shape[1], out_ref.shape[0], out_ref.shape[1]
    width = cap // chunks

    barrier = pltpu.get_barrier_semaphore()

    @pl.when(g < 3)
    def _():
        for k in range(1, n_tile):
            pl.semaphore_signal(barrier, inc=1, device_id=(g, lax.rem(t + k, n_tile)), device_id_type=MESH)
        pl.semaphore_signal(barrier, inc=1, device_id=(3, t), device_id_type=MESH)
        pl.semaphore_wait(barrier, n_tile)

    @pl.when(g == 3)
    def _():
        for k in range(3):
            pl.semaphore_signal(barrier, inc=1, device_id=(k, t), device_id_type=MESH)
        pl.semaphore_wait(barrier, 3)

    def exchange(s, slot, c):
        part = pl.ds(c * width, width)
        return pltpu.make_async_remote_copy(
            src_ref=sent_ref.at[s, :, part], dst_ref=got.at[slot, :, part], send_sem=send_sem.at[s, c],
            recv_sem=recv_sem.at[slot, c], device_id=(g, s), device_id_type=MESH)

    def report(c, slot):
        part = pl.ds(c * width, width)
        return pltpu.make_async_remote_copy(
            src_ref=out_ref.at[:, part], dst_ref=records.at[slot, :, part], send_sem=rsend_sem.at[c],
            recv_sem=rrecv_sem.at[slot, c], device_id=(3, t), device_id_type=MESH)

    @pl.when(g < 3)
    def _():
        for c in range(chunks):
            for k in range(1, n_tile):
                exchange(lax.rem(t + k, n_tile), t, c).start()
        got[t] = sent_ref[t, :, 0:cap]
        matrix = matrix_ref[...]
        for c in range(chunks):
            for k in range(1, n_tile):
                exchange(lax.rem(t + k, n_tile), lax.rem(t + k, n_tile), c).wait_recv()
            value = got[:, :, c * width : (c + 1) * width].reshape(nx, width)
            out_ref[:, c * width : (c + 1) * width] = jnp.dot(
                matrix, value, precision=lax.Precision.HIGHEST, preferred_element_type=jnp.float32)
            report(c, g).start()
        for c in range(chunks):
            for k in range(1, n_tile):
                exchange(lax.rem(t + k, n_tile), t, c).wait_send()
            report(c, g).wait_send()

    @pl.when(g == 3)
    def _():
        for c in range(chunks):
            for k in range(3):
                report(c, k).wait_recv()
            part = slice(c * width, (c + 1) * width)
            first, second, third = records[0, :, part], records[1, :, part], records[2, :, part]
            out_ref[:, part] = first * first + second * second + third * third


def tiled_body(flow_state, line_owner, *, n_tile):
    _, planes, rows, ny = flow_state.shape
    n_lines = line_owner.shape[0]
    n_blocks = n_lines // LANES
    nx = rows * n_tile
    cap = 2 * planes * ny // n_tile
    vmem = pl.BlockSpec(memory_space=pltpu.VMEM)
    smem = pl.BlockSpec(memory_space=pltpu.SMEM)
    f32 = jnp.float32
    shape = jax.ShapeDtypeStruct
    limit = 16 * 1024 * 1024
    dma = pltpu.SemaphoreType.DMA
    owner = line_owner.reshape(n_blocks, LANES)
    tile = (planes, rows, ny)
    ints = shape((n_blocks, LANES), jnp.int32)
    coeffs, place, base, count = pl.pallas_call(
        functools.partial(flow_kernel, n_tile),
        out_shape=(shape(tile, f32), shape((n_blocks, LANES), f32), ints, ints),
        in_specs=[vmem, vmem], out_specs=(vmem, vmem, vmem, vmem),
        scratch_shapes=[
            pltpu.VMEM((4,) + tile, f32), pltpu.VMEM((3,) + tile, f32),
            pltpu.VMEM((4,) + tile, f32), pltpu.VMEM((2,) + tile, f32),
            pltpu.VMEM((planes, rows + 2 * reach, ny), f32), pltpu.VMEM((planes, rows + 2 * reach, ny), f32),
            pltpu.VMEM(tile, f32), pltpu.VMEM(tile, f32), pltpu.VMEM(tile, f32), pltpu.VMEM(tile, f32), pltpu.VMEM(tile, f32),
            dma((4,)), dma((4, 2)), dma((2,)), dma((4,)), dma((4,)), dma((4,)), dma((2,)), dma((2,)), dma((4,)),
            pltpu.VMEM((4 * LANES, 2 * LANES), f32),
        ],
        compiler_params=pltpu.CompilerParams(has_side_effects=True, collective_id=0, vmem_limit_bytes=limit), name="flow",
    )(flow_state, owner)
    sent = pl.pallas_call(
        functools.partial(compact_kernel, n_tile),
        out_shape=shape((n_tile, rows, cap + 2 * LANES), f32),
        in_specs=[smem, smem, vmem, vmem], out_specs=vmem,
        scratch_shapes=[pltpu.VMEM((n_tile, rows, LANES), f32)],
        compiler_params=pltpu.CompilerParams(vmem_limit_bytes=limit), name="compact",
    )(base, count, coeffs, place)
    chunks = 4 if cap % (4 * LANES) == 0 else 1
    record = pl.pallas_call(
        functools.partial(record_kernel, n_tile, chunks),
        out_shape=shape((nx, cap), f32),
        in_specs=[vmem, vmem], out_specs=vmem,
        scratch_shapes=[
            pltpu.VMEM((n_tile, rows, cap), f32), pltpu.VMEM((3, nx, cap), f32),
            dma((n_tile, chunks)), dma((n_tile, chunks)), dma((chunks,)), dma((3, chunks)),
        ],
        compiler_params=pltpu.CompilerParams(has_side_effects=True, collective_id=1, vmem_limit_bytes=limit), name="record",
    )(sent, jnp.asarray(lift_matrix(nx).astype(np.float32)))
    return record[None, None]


CHUNK = 64
SIDE = 16
SPARE = LANES - CHUNK - 2 * SIDE
SUB = 8


def planes_taps(planes):
    first, second = [0.0] * planes, [0.0] * planes
    second[0] = 3.0 * second_center
    for k in range(1, reach + 1):
        first[k % planes] += first_coeffs[k - 1]
        first[-k % planes] -= first_coeffs[k - 1]
        second[k % planes] += second_coeffs[k - 1]
        second[-k % planes] += second_coeffs[k - 1]
    return first, second


def column_taps():
    full = lift_matrix(8 * CHUNK)
    middle = 4 * CHUNK
    low = full[middle // 2, middle - 4 : middle + 5]
    high = full[8 * CHUNK // 2 + middle // 2, middle + 1 - 4 : middle + 1 + 5]
    return [float(x) for x in low], [float(x) for x in high]


def column_band(planes):
    taps_low, taps_high = column_taps()
    part = CHUNK // 2
    row = lax.broadcasted_iota(jnp.int32, (planes * LANES, 2 * LANES), 0)
    column = lax.broadcasted_iota(jnp.int32, (planes * LANES, 2 * LANES), 1)
    is_low = column < LANES
    spot = SIDE + 2 * (column & (part - 1)) + jnp.where(is_low, 0, 1)
    same = (row // LANES) == ((column & (LANES - 1)) // part)
    distance = jnp.where(same, (row & (LANES - 1)) - spot, LANES)
    value = jnp.zeros((planes * LANES, 2 * LANES), jnp.float32)
    for offset in range(-4, 5):
        tap = jnp.where(is_low, taps_low[offset + 4], taps_high[offset + 4])
        value = jnp.where(distance == offset, tap, value)
    return value


def pencil_slots(pencil, owner, spot_ref, group_ref):
    n_blocks = owner.shape[0]
    upper = (lax.broadcasted_iota(jnp.int32, (LANES, LANES), 0) <= lax.broadcasted_iota(jnp.int32, (LANES, LANES), 1)).astype(jnp.float32)
    lower = (lax.broadcasted_iota(jnp.int32, (n_blocks, n_blocks), 0) > lax.broadcasted_iota(jnp.int32, (n_blocks, n_blocks), 1)).astype(jnp.float32)
    lane = lax.broadcasted_iota(jnp.int32, (n_blocks, LANES), 1)
    mine = owner == pencil
    mask = mine.astype(jnp.float32)
    within = jnp.dot(mask, upper, preferred_element_type=jnp.float32)
    total = jnp.broadcast_to(jnp.sum(mask, axis=1, keepdims=True), (n_blocks, LANES))
    base = jnp.dot(lower, total, preferred_element_type=jnp.float32).astype(jnp.int32)
    slot = base + within.astype(jnp.int32) - 1
    spot_ref[...] = jnp.where(mine, slot & (LANES - 1), -1)
    group_ref[...] = base // LANES + jnp.where(lane < (base & (LANES - 1)), 1, 0)


def chunk_kernel(n_tile, own_hbm, owner_hbm, out_ref,
                 own, owner_ref, windows, arrived, fields, mids, slope, final, pieces, landed, spot_ref, group_ref, ordered, band_ref,
                 own_sem, owner_sem, send_sem, recv_sem, recv_two, hand_sem, side_sem, onward_sem):
    g, t = lax.axis_index("grp"), lax.axis_index("tile")
    planes, rows, ny = own.shape
    n_grp = 4
    n_dev = n_grp * n_tile
    nx = rows * n_tile
    half = nx // 2
    me = t * n_grp + g

    load = pltpu.make_async_copy(own_hbm.at[0], own, own_sem)
    load.start()
    load_owner = pltpu.make_async_copy(owner_hbm, owner_ref, owner_sem)
    load_owner.start()
    peers = [(lax.rem(g + k % n_grp, n_grp), lax.rem(t + k // n_grp, n_tile)) for k in range(1, n_dev)]
    barrier = pltpu.get_barrier_semaphore()
    for peer in peers:
        pl.semaphore_signal(barrier, inc=1, device_id=peer, device_id_type=MESH)
    load.wait()
    spread = lax.broadcasted_iota(jnp.int32, (rows, ny), 1) & (LANES - 1)
    for odd in range(2):
        turned = [pltpu.roll(own[z], (SIDE - odd * CHUNK) % ny, 1) for z in range(planes)]
        for z in range(planes - 1):
            moved = pltpu.roll(turned[planes - 1], LANES - SPARE * (z + 1), 1)
            mixed = jnp.where(spread < LANES - SPARE, turned[z], moved)
            for m in range(n_dev // 2):
                windows[2 * m + odd, z * rows : (z + 1) * rows] = mixed[:, m * LANES : (m + 1) * LANES]
    pl.semaphore_wait(barrier, n_dev - 1)

    packed = (planes - 1) * rows

    def deal(peer, source):
        to = peer[1] * n_grp + peer[0]
        return pltpu.make_async_remote_copy(
            src_ref=windows.at[to, pl.ds(0, packed)], dst_ref=arrived.at[source, pl.ds(0, packed)], send_sem=send_sem.at[to], recv_sem=recv_sem.at[source],
            device_id=peer, device_id_type=MESH)

    for peer in peers:
        deal(peer, me).start()
    arrived[me] = windows[me]

    load_owner.wait()
    pencil_slots(t, owner_ref[...], spot_ref, group_ref)
    out_ref[...] = jnp.zeros_like(out_ref)
    band_ref[...] = column_band(planes)

    for peer in peers:
        deal(peer, peer[1] * n_grp + peer[0]).wait_recv()

    sublane = lax.broadcasted_iota(jnp.int32, (reach, SUB, LANES), 1)

    def flip(value):
        return jnp.where((sublane & 1) == 0, pltpu.roll(value, SUB - 1, 1), pltpu.roll(value, 1, 1))

    def wrap(ref, c):
        ref[c, 0:reach] = flip(ref[c, half : half + reach])
        ref[c, half + reach : half + 2 * reach] = flip(ref[c, reach : 2 * reach])

    spot = lax.broadcasted_iota(jnp.int32, (rows, LANES), 1)
    for f in range(n_grp):
        for tile in range(n_tile):
            source = tile * n_grp + f
            last = None
            for z in range(planes - 1):
                piece = pltpu.roll(arrived[source, z * rows : (z + 1) * rows], SPARE * (z + 1), 1)
                last = piece if last is None else jnp.where(spot < SPARE * z, last, piece)
            arrived[source, packed : packed + rows] = last
            side, first = tile // (n_tile // 2), (tile % (n_tile // 2)) * rows
            for r in range(rows):
                fields[f, reach + first + r, pl.ds(side, planes, stride=2), :] = arrived[tile * n_grp + f, pl.ds(r, planes, stride=rows), :]
        wrap(fields, f)

    z_first, z_second = planes_taps(planes)
    step = rows

    def turn_z(value, m):
        return value if m == 0 else pltpu.roll(value, (-2 * m) % SUB, 1)

    def turn_y(value, k):
        return pltpu.roll(value, (-k) % LANES, 2)

    def gradient(i, direction):
        if direction == 0:
            shift = lambda k: fields[3, reach + i + k : reach + i + k + step]
        else:
            center = fields[3, reach + i : reach + i + step]
            if direction == 1:
                shift = lambda k: turn_y(center, k)
            else:
                total = None
                for m in range(1, planes):
                    if z_first[m] != 0.0:
                        term = z_first[m] * turn_z(center, m)
                        total = term if total is None else total + term
                return total
        value, _ = derivatives(None, shift, True, False)
        return value

    def tendency(ref, c, i, speed, press):
        center = ref[c, reach + i : reach + i + step]
        total = z_second[0] * center
        slope_z = None
        for m in range(1, planes):
            turned = turn_z(center, m)
            total = total + z_second[m] * turned
            if z_first[m] != 0.0:
                term = z_first[m] * turned
                slope_z = term if slope_z is None else slope_z + term
        slope_x, slope_y = None, None
        for k in range(1, reach + 1):
            ahead, behind = ref[c, reach + i + k : reach + i + k + step], ref[c, reach + i - k : reach + i - k + step]
            up, down = turn_y(center, k), turn_y(center, -k)
            term_x, term_y = first_coeffs[k - 1] * (ahead - behind), first_coeffs[k - 1] * (up - down)
            slope_x = term_x if slope_x is None else slope_x + term_x
            slope_y = term_y if slope_y is None else slope_y + term_y
            total = total + second_coeffs[k - 1] * ((ahead + behind) + (up + down))
        advect = speed[0] * slope_x + speed[1] * slope_y + speed[2] * slope_z
        return viscosity * total - advect - press, center

    def first_section(b, _):
        i = b * step
        speed = [fields[f, reach + i : reach + i + step] if isinstance(i, int) else fields[f, pl.ds(reach + i, step)] for f in range(3)]
        for c in range(3):
            press = gradient(i, c)
            slope[c, i : i + step] = press
            change, center = tendency(fields, c, i, speed, press)
            mids[c, reach + i : reach + i + step] = center + time_step * change
        return 0

    def second_section(b, c):
        i = b * step
        speed = [mids[f, reach + i : reach + i + step] for f in range(3)]
        change, center = tendency(mids, c, i, speed, slope[c, i : i + step])
        final[c, i : i + step] = 0.5 * ((fields[c, reach + i : reach + i + step] + center) + time_step * change)

    for b in range(half // step):
        first_section(b, 0)
    for c in range(3):
        wrap(mids, c)
    flat = lax.broadcasted_iota(jnp.int32, (SUB, LANES), 0)

    def flip_one(value):
        return jnp.where((flat & 1) == 0, pltpu.roll(value, SUB - 1, 0), pltpu.roll(value, 1, 0))

    matrix = lift_matrix(planes)
    z_coeffs = []
    for m in range(planes):
        column = jnp.zeros((SUB, LANES), jnp.float32)
        for z in range(planes):
            column = jnp.where(flat // 2 == z, float(matrix[z, (z + m) % planes]), column)
        z_coeffs.append(column)

    def lift_z(value):
        total = z_coeffs[0] * value
        for m in range(1, planes):
            total = total + z_coeffs[m] * pltpu.roll(value, (-2 * m) % SUB, 0)
        return total

    pairs = half // 2
    z, y = t // 2, t % 2
    n_z = n_tile // 2

    def flipped(value, bits):
        result, place = 0, 1
        while place < n_z:
            result = result + place * lax.rem(value // place + bits // place, 2)
            place *= 2
        return result

    partner = flipped(z, 1)

    def source_of(level, column, group):
        return (level * 2 + column) * n_grp + group

    def send(origin, source, sem, group, level, column):
        return pltpu.make_async_remote_copy(
            src_ref=origin, dst_ref=landed.at[source], send_sem=sem, recv_sem=recv_two.at[source],
            device_id=(group, level * 2 + column), device_id_type=MESH)

    kin = [g, g + 1 - 2 * lax.rem(g, 2), lax.rem(g + 2, n_grp), n_grp - 1 - g]
    across = (0, 2, 3, 1)
    routes = ((3, 0), (0, 1), (0, 0), (1, 0))

    def hand(bits, other, c):
        return send(pieces.at[c], me, hand_sem.at[bits + 2 * other, c], c, flipped(z, bits), lax.rem(y + other, 2))

    def each_hand(c, act):
        for bits, other in routes:
            if bits or other:
                act(hand(bits, other, c))
            else:
                @pl.when(g != c)
                def _():
                    act(hand(bits, other, c))

    def side(source):
        return send(landed.at[source], source, side_sem.at[source], g, z, 1 - y)

    def onward(source):
        return send(landed.at[source], source, onward_sem.at[source], g, partner, y)

    def await_piece(source):
        send(pieces.at[g], source, hand_sem.at[0, 0], g, z, 1 - y).wait_recv()

    def finish(c):
        even = [lift_z(final[c, 2 * i]) for i in range(pairs)]
        odd = [lift_z(final[c, 2 * i + 1]) for i in range(pairs)]
        for odd_tap, even_tap in ((lift_alpha, lift_beta), (lift_gamma, lift_delta)):
            after = even[1:] + [flip_one(even[0])]
            odd = [odd[i] + odd_tap * (even[i] + after[i]) for i in range(pairs)]
            before = [flip_one(odd[-1])] + odd[:-1]
            even = [even[i] + even_tap * (odd[i] + before[i]) for i in range(pairs)]
        for i in range(pairs):
            final[c, i] = even[i] * lift_scale
            final[c, pairs + i] = odd[i] * (1.0 / lift_scale)
        flat_ref = final.at[c].reshape(half * SUB, LANES)
        stacked = []
        for high in range(2):
            for a in range(2):
                stacked.append(jnp.concatenate([flat_ref[pl.ds(high * pairs * SUB + 2 * z_at + a, pairs, stride=SUB), :] for z_at in range(planes)], axis=1))
        lines = jnp.dot(jnp.concatenate(stacked, axis=0), band_ref[...], precision=lax.Precision.HIGHEST, preferred_element_type=jnp.float32)
        pieces[c] = lines

    for c in (0, 2, 1):
        for b in range(half // step):
            second_section(b, c)
        finish(c)
        each_hand(c, lambda copy: copy.start())
    pieces[3] = pieces[0] * pieces[0] + pieces[1] * pieces[1] + pieces[2] * pieces[2]
    each_hand(3, lambda copy: copy.start())
    rank = lax.broadcasted_iota(jnp.int32, (LANES, LANES), 0)
    n_groups = n_tile
    lane_part = lax.broadcasted_iota(jnp.int32, (nx, LANES), 1) // (CHUNK // 2)

    def select(tile):
        for high in range(2):
            tiles = [landed[tile * n_grp + m, :, high * LANES : (high + 1) * LANES] for m in range(4)]
            for bit in range(2):
                distance = (CHUNK // 2) << bit
                is_low = (lane_part & (1 << bit)) == 0
                turned = list(tiles)
                for m in range(4):
                    if not m & (1 << bit):
                        other = m | (1 << bit)
                        turned[m] = jnp.where(is_low, tiles[m], pltpu.roll(tiles[other], distance, 1))
                        turned[other] = jnp.where(is_low, pltpu.roll(tiles[m], LANES - distance, 1), tiles[other])
                tiles = turned
            for plane in range(planes):
                block = (plane * 2 + high) * n_groups + tile
                value = tiles[plane]
                first = value.astype(jnp.bfloat16).astype(jnp.float32)
                rest = value - first
                second = rest.astype(jnp.bfloat16).astype(jnp.float32)
                stack = jnp.concatenate([first, second, rest - second], axis=0).astype(jnp.bfloat16)
                chosen = jnp.where(rank == spot_ref[pl.ds(block, 1), :], 1.0, 0.0).astype(jnp.bfloat16)
                placed = lax.dot_general(stack, chosen, (((1,), (1,)), ((), ())), preferred_element_type=jnp.float32)
                ordered[plane * 2 + high] = (placed[0:nx] + placed[nx : 2 * nx]) + placed[2 * nx : 3 * nx]
        labels = [group_ref[pl.ds((plane * 2 + high) * n_groups + tile, 1), :] for plane in range(planes) for high in range(2)]
        for q in range(out_ref.shape[1] // LANES):
            total = out_ref[:, q * LANES : (q + 1) * LANES]
            for n, label in enumerate(labels):
                total = total + jnp.where(label == q, ordered[n], 0.0)
            out_ref[:, q * LANES : (q + 1) * LANES] = total

    landed[me] = pieces[g]

    def sideways(bits, k):
        return bits > 0 and not (bits == 1 and k >= n_grp // 2)

    def receive(bits):
        for k in across:
            source = source_of(flipped(z, bits), y, kin[k])
            if bits or k:
                await_piece(source)
            if bits == 3:
                onward(source).start()
            if sideways(bits, k):
                side(source).start()
        if bits == 0:
            for k in across:
                source = source_of(z, 1 - y, kin[k])
                await_piece(source)
                if k >= n_grp // 2:
                    onward(source).start()

    for bits in (3, 0, 1):
        receive(bits)

    def from_other(bits):
        for k in across:
            await_piece(source_of(flipped(z, bits), 1 - y, kin[k]))

    def pick(bits, other):
        select(flipped(z, bits) * 2 + lax.rem(y + other, 2))

    pick(0, 0)
    receive(2)
    pick(0, 1)
    pick(1, 0)
    pick(3, 0)
    pick(2, 0)
    for bits in (3, 1, 2):
        from_other(bits)
        pick(bits, 1)

    for peer in peers:
        deal(peer, me).wait_send()
    for c in range(n_grp):
        each_hand(c, lambda copy: copy.wait_send())
    for k in across:
        for bits in range(1, n_z):
            source = source_of(flipped(z, bits), y, kin[k])
            if sideways(bits, k):
                side(source).wait_send()
        onward(source_of(flipped(z, 3), y, kin[k])).wait_send()
        if k >= n_grp // 2:
            onward(source_of(z, 1 - y, kin[k])).wait_send()


def chunk_body(flow_state, line_owner, *, n_tile):
    _, planes, rows, ny = flow_state.shape
    n_lines = line_owner.shape[0]
    n_blocks = n_lines // LANES
    nx = rows * n_tile
    half = nx // 2
    n_dev = 4 * n_tile
    cap = 2 * planes * ny // n_tile
    f32 = jnp.float32
    dma = pltpu.SemaphoreType.DMA
    hbm = pl.BlockSpec(memory_space=pltpu.HBM)
    padded = (half + 2 * reach, SUB, LANES)
    record = pl.pallas_call(
        functools.partial(chunk_kernel, n_tile),
        out_shape=jax.ShapeDtypeStruct((nx, cap), f32),
        in_specs=[hbm, hbm], out_specs=pl.BlockSpec(memory_space=pltpu.VMEM),
        scratch_shapes=[
            pltpu.VMEM((planes, rows, ny), f32), pltpu.VMEM((n_blocks, LANES), jnp.int32),
            pltpu.VMEM((n_dev, planes * rows, LANES), f32), pltpu.VMEM((n_dev, planes * rows, LANES), f32),
            pltpu.VMEM((4,) + padded, f32), pltpu.VMEM((3,) + padded, f32),
            pltpu.VMEM((3, half, SUB, LANES), f32), pltpu.VMEM((3, half, SUB, LANES), f32),
            pltpu.VMEM((4, nx, 2 * LANES), f32), pltpu.VMEM((n_dev, nx, 2 * LANES), f32),
            pltpu.VMEM((n_blocks, LANES), jnp.int32), pltpu.VMEM((n_blocks, LANES), jnp.int32),
            pltpu.VMEM((2 * planes, nx, LANES), f32), pltpu.VMEM((planes * LANES, 2 * LANES), f32),
            dma, dma, dma((n_dev,)), dma((n_dev,)), dma((n_dev,)), dma((4, 4)), dma((n_dev,)), dma((n_dev,)),
        ],
        compiler_params=pltpu.CompilerParams(has_side_effects=True, collective_id=0, vmem_limit_bytes=16 * 1024 * 1024), name="record",
    )(pltpu.with_memory_space_constraint(flow_state, pltpu.HBM), pltpu.with_memory_space_constraint(line_owner.reshape(n_blocks, LANES), pltpu.HBM))
    return record[None, None]


def fits_chunks(mesh, planes, rows, ny):
    n_tile = mesh.shape["tile"]
    return 2 * planes == SUB and 2 * rows == SUB and mesh.shape["grp"] == 4 and ny == 4 * n_tile * CHUNK and n_tile == 8


def solution(mesh):
    in_specs = (P("grp", None, "tile", None), P())
    out_specs = P("grp", "tile", None, None)
    n_tile = mesh.shape["tile"]

    def run(flow_state, line_owner):
        _, planes, rows, ny = flow_state.shape
        chosen = chunk_body if fits_chunks(mesh, planes, rows, ny) else tiled_body
        return chosen(flow_state, line_owner, n_tile=n_tile)

    return jax.shard_map(run, mesh=mesh, in_specs=in_specs, out_specs=out_specs, check_vma=False)
```

```python
import functools

import jax
import jax.numpy as jnp
import numpy as np
from jax import lax
from jax.experimental import pallas as pl
from jax.experimental.pallas import tpu as pltpu
from jax.sharding import PartitionSpec as P

time_step = 0.2
viscosity = 0.05
reach = 4
first_coeffs = (0.8, -0.2, 4.0 / 105.0, -1.0 / 280.0)
second_center = -205.0 / 72.0
second_coeffs = (1.6, -0.2, 8.0 / 315.0, -1.0 / 560.0)
lift_alpha = -1.586134342059924
lift_beta = -0.052980118572961
lift_gamma = 0.882911075530934
lift_delta = 0.443506852043971
lift_scale = 1.149604398860241
LANES = 128
MESH = pl.DeviceIdType.MESH


def lift_numpy(signal):
    even, odd = signal[0::2].copy(), signal[1::2].copy()
    odd += lift_alpha * (even + np.roll(even, -1, 0))
    even += lift_beta * (odd + np.roll(odd, 1, 0))
    odd += lift_gamma * (even + np.roll(even, -1, 0))
    even += lift_delta * (odd + np.roll(odd, 1, 0))
    return np.concatenate([even * lift_scale, odd / lift_scale])


def lift_matrix(length):
    return lift_numpy(np.eye(length))


def band_matrix():
    full = lift_matrix(8 * LANES)
    low = full[LANES : 2 * LANES, LANES : 5 * LANES]
    high = full[4 * LANES + LANES : 4 * LANES + 2 * LANES, LANES : 5 * LANES]
    return np.concatenate([low, high]).T.astype(np.float32)


def band_value(taps_low, taps_high):
    row = lax.broadcasted_iota(jnp.int32, (4 * LANES, 2 * LANES), 0)
    column = lax.broadcasted_iota(jnp.int32, (4 * LANES, 2 * LANES), 1)
    distance = row - LANES - 2 * (column & (LANES - 1))
    is_low = column < LANES
    value = jnp.zeros((4 * LANES, 2 * LANES), jnp.float32)
    for offset in range(-4, 5):
        tap = jnp.where(is_low, taps_low[offset + 4], taps_high[offset + 4])
        value = jnp.where(distance == offset, tap, value)
    return value


def band_taps():
    band = band_matrix()
    rows = slice(LANES + LANES // 2 - 4, LANES + LANES // 2 + 5)
    return [float(x) for x in band[rows, LANES // 4]], [float(x) for x in band[rows, LANES + LANES // 4]]


def shifted_y(value, k):
    return pltpu.roll(value, (-k) % value.shape[-1], value.ndim - 1)


def derivatives(center, shift, want_first=True, want_second=True):
    first, second = None, second_center * center if want_second else None
    for k in range(1, reach + 1):
        ahead, behind = shift(k), shift(-k)
        if want_first:
            term = first_coeffs[k - 1] * (ahead - behind)
            first = term if first is None else first + term
        if want_second:
            second = second + second_coeffs[k - 1] * (ahead + behind)
    return first, second


def slots_of(n_tile, owner_ref, place_ref, base_ref, count_ref):
    owner = owner_ref[...]
    n_blocks = owner.shape[0]
    upper = (lax.broadcasted_iota(jnp.int32, (LANES, LANES), 0) <= lax.broadcasted_iota(jnp.int32, (LANES, LANES), 1)).astype(jnp.float32)
    lower = (lax.broadcasted_iota(jnp.int32, (n_blocks, n_blocks), 0) > lax.broadcasted_iota(jnp.int32, (n_blocks, n_blocks), 1)).astype(jnp.float32)
    lane = lax.broadcasted_iota(jnp.int32, (n_blocks, LANES), 1)

    def step(s, carry):
        place, counts, ahead = carry
        mask = (owner == s).astype(jnp.float32)
        within = jnp.dot(mask, upper, preferred_element_type=jnp.float32)
        total = jnp.sum(mask, axis=1, keepdims=True)
        place = place + mask * (ahead + within - 1.0)
        counts = jnp.where(lane == s, total, counts)
        return place, counts, ahead + total

    zeros = jnp.zeros((n_blocks, LANES), jnp.float32)
    carry = (zeros, zeros, jnp.zeros((n_blocks, 1), jnp.float32))
    if n_tile <= 16:
        for s in range(n_tile):
            carry = step(s, carry)
    else:
        carry = lax.fori_loop(0, n_tile, step, carry)
    place, counts, _ = carry
    place_ref[...] = place
    count_ref[...] = counts.astype(jnp.int32)
    base_ref[...] = jnp.dot(lower, counts, preferred_element_type=jnp.float32).astype(jnp.int32)


def flow_kernel(n_tile, own_ref, owner_ref, out_ref, place_ref, base_ref, count_ref,
                fields, mids, halo, mid_halo, pad, ppad, middle, fin, along_y, along_z, lap, send_sem, recv_sem, hsend_sem, hrecv_sem, msend_sem, mrecv_sem, mhsend_sem, mhrecv_sem, relay_sem, band_ref):
    g, t = lax.axis_index("grp"), lax.axis_index("tile")
    right, left = lax.rem(t + 1, n_tile), lax.rem(t + n_tile - 1, n_tile)
    planes, rows, ny = own_ref.shape[1:]
    own = own_ref.at[0]

    barrier = pltpu.get_barrier_semaphore()
    for k in range(1, 4):
        pl.semaphore_signal(barrier, inc=1, device_id=(lax.rem(g + k, 4), t), device_id_type=MESH)
    for side in (right, left):
        pl.semaphore_signal(barrier, inc=1, device_id=(g, side), device_id_type=MESH)

    @pl.when((g == 0) | (g == 3))
    def _():
        for side in (right, left):
            pl.semaphore_signal(barrier, inc=1, device_id=(3 - g, side), device_id_type=MESH)
        pl.semaphore_wait(barrier, 7)

    @pl.when((g == 1) | (g == 2))
    def _():
        pl.semaphore_wait(barrier, 5)

    def gather_copy(src, dst, ssem, rsem, k, slot):
        return pltpu.make_async_remote_copy(
            src_ref=src, dst_ref=dst.at[slot], send_sem=ssem.at[k], recv_sem=rsem.at[slot],
            device_id=(k, t), device_id_type=MESH)

    half = planes // 2

    def whole_copy(k, slot):
        return pltpu.make_async_remote_copy(
            src_ref=own, dst_ref=fields.at[slot], send_sem=send_sem.at[k], recv_sem=recv_sem.at[slot, 0],
            device_id=(k, t), device_id_type=MESH)

    def half_copy(slot, k):
        part = pl.ds(k * half, half)
        return pltpu.make_async_remote_copy(
            src_ref=own.at[part], dst_ref=fields.at[slot, part], send_sem=send_sem.at[k],
            recv_sem=recv_sem.at[slot, k], device_id=(k, t), device_id_type=MESH)

    def relay_copy(slot, k):
        part = pl.ds(k * half, half)
        return pltpu.make_async_remote_copy(
            src_ref=fields.at[slot, part], dst_ref=fields.at[slot, part], send_sem=relay_sem.at[slot],
            recv_sem=recv_sem.at[slot, k], device_id=(1 - k, t), device_id_type=MESH)

    def halo_copy(src, dst, ssem, rsem, side, slot, group):
        return pltpu.make_async_remote_copy(
            src_ref=src, dst_ref=dst.at[slot + side], send_sem=ssem.at[side], recv_sem=rsem.at[slot + side],
            device_id=(group, right if side == 0 else left), device_id_type=MESH)

    @pl.when(g < 3)
    def _():
        for side in range(2):
            halo_copy(own, halo, hsend_sem, hrecv_sem, side, 0, g).start()

    for k in range(3):
        @pl.when((g < 2) & (g != k))
        def _(k=k):
            whole_copy(k, g).start()

    @pl.when(g >= 2)
    def _():
        for k in range(2):
            half_copy(g, k).start()

    @pl.when(g == 3)
    def _():
        whole_copy(2, 3).start()
        for side in range(2):
            halo_copy(own, halo, hsend_sem, hrecv_sem, side, 2, 0).start()

    def local_terms():
        for z in range(planes):
            center = pad[z, reach : reach + rows]
            fy, sy = derivatives(center, lambda k: shifted_y(center, k))
            fz, sz = derivatives(center, lambda k: pad[(z + k) % planes, reach : reach + rows])
            along_y[z], along_z[z], lap[z] = fy, fz, sy + sz

    slots_of(n_tile, owner_ref, place_ref, base_ref, count_ref)
    band_ref[...] = band_value(*band_taps())

    @pl.when(g < 3)
    def _():
        for k in range(3):
            @pl.when(g == k)
            def _(k=k):
                fields[k] = own_ref[0]

        for z in range(planes):
            pad[z, reach : reach + rows] = own_ref[0, z]
        local_terms()

        @pl.when(g < 2)
        def _():
            for slot in (2, 3):
                half_copy(slot, g).wait_recv()
                relay_copy(slot, g).start()
            whole_copy(0, 1 - g).wait_recv()
            for slot in (2, 3):
                half_copy(slot, 1 - g).wait_recv()

        @pl.when(g == 2)
        def _():
            for slot in (0, 1, 3):
                whole_copy(0, slot).wait_recv()

        for side in range(2):
            halo_copy(own, halo, hsend_sem, hrecv_sem, side, 0, g).wait_recv()

        @pl.when(g == 0)
        def _():
            for side in range(2):
                halo_copy(own, halo, hsend_sem, hrecv_sem, side, 2, 0).wait_recv()
            for z in range(planes):
                ppad[z, 0:reach] = halo[2, z, rows - reach : rows]
                ppad[z, reach : reach + rows] = fields[3, z]
                ppad[z, reach + rows : 2 * reach + rows] = halo[3, z, 0:reach]
            for z in range(planes):
                middle[z], _ = derivatives(None, lambda k: ppad[z, reach + k : reach + k + rows], True, False)

        @pl.when(g == 1)
        def _():
            for z in range(planes):
                value = fields[3, z]
                middle[z], _ = derivatives(None, lambda k: shifted_y(value, k), True, False)

        @pl.when(g == 2)
        def _():
            for z in range(planes):
                middle[z], _ = derivatives(None, lambda k: fields[3, (z + k) % planes], True, False)

        def tendency(z, vel, press):
            center = pad[z, reach : reach + rows]
            fx, sx = derivatives(center, lambda k: pad[z, reach + k : reach + k + rows])
            advect = vel[0, z] * fx + vel[1, z] * along_y[z] + vel[2, z] * along_z[z]
            return viscosity * (sx + lap[z]) - advect - press

        for z in range(planes):
            pad[z, 0:reach] = halo[0, z, rows - reach : rows]
            pad[z, reach + rows : 2 * reach + rows] = halo[1, z, 0:reach]
        for z in range(planes):
            press = middle[z]
            ppad[z, 0:rows] = press
        for z in range(planes):
            middle[z] = own_ref[0, z] + time_step * tendency(z, fields, ppad[z, 0:rows])

        for side in range(2):
            halo_copy(middle, mid_halo, mhsend_sem, mhrecv_sem, side, 0, g).start()
        for k in range(3):
            @pl.when(g != k)
            def _(k=k):
                gather_copy(middle, mids, msend_sem, mrecv_sem, k, g).start()

            @pl.when(g == k)
            def _(k=k):
                mids[k] = middle[...]

        for z in range(planes):
            pad[z, reach : reach + rows] = middle[z]
        local_terms()
        for k in range(3):
            @pl.when(g != k)
            def _(k=k):
                gather_copy(middle, mids, msend_sem, mrecv_sem, 0, k).wait_recv()
        for side in range(2):
            halo_copy(middle, mid_halo, mhsend_sem, mhrecv_sem, side, 0, g).wait_recv()
        for z in range(planes):
            pad[z, 0:reach] = mid_halo[0, z, rows - reach : rows]
            pad[z, reach + rows : 2 * reach + rows] = mid_halo[1, z, 0:reach]
        for z in range(planes):
            fin[z] = 0.5 * ((own_ref[0, z] + middle[z]) + time_step * tendency(z, mids, ppad[z, 0:rows]))

        blocks = ny // (2 * LANES)
        groups = ny // LANES
        for z in range(planes):
            value = fin[z]
            pieces = []
            for b in range(blocks):
                window = [value[:, ((2 * b + j) % groups) * LANES : ((2 * b + j) % groups + 1) * LANES] for j in (-1, 0, 1, 2)]
                pieces.append(jnp.concatenate(window, axis=1))
            stacked = jnp.concatenate(pieces, axis=0)
            lifted = jnp.dot(stacked, band_ref[...], precision=lax.Precision.HIGHEST, preferred_element_type=jnp.float32)
            for b in range(blocks):
                piece = lifted[b * rows : (b + 1) * rows]
                fin[z, :, b * LANES : (b + 1) * LANES] = piece[:, 0:LANES]
                fin[z, :, ny // 2 + b * LANES : ny // 2 + (b + 1) * LANES] = piece[:, LANES:]

        even = [fin[2 * i] for i in range(half)]
        odd = [fin[2 * i + 1] for i in range(half)]
        odd = [odd[i] + lift_alpha * (even[i] + even[(i + 1) % half]) for i in range(half)]
        even = [even[i] + lift_beta * (odd[i] + odd[(i - 1) % half]) for i in range(half)]
        odd = [odd[i] + lift_gamma * (even[i] + even[(i + 1) % half]) for i in range(half)]
        even = [even[i] + lift_delta * (odd[i] + odd[(i - 1) % half]) for i in range(half)]
        for i in range(half):
            out_ref[i] = even[i] * lift_scale
            out_ref[half + i] = odd[i] * (1.0 / lift_scale)

        for side in range(2):
            halo_copy(middle, mid_halo, mhsend_sem, mhrecv_sem, side, 0, g).wait_send()
        for k in range(3):
            @pl.when(g != k)
            def _(k=k):
                gather_copy(middle, mids, msend_sem, mrecv_sem, k, g).wait_send()

    @pl.when(g == 3)
    def _():
        out_ref[...] = jnp.zeros_like(out_ref)

    for side in range(2):
        halo_copy(own, halo, hsend_sem, hrecv_sem, side, 0, g).wait_send()
    for k in range(3):
        @pl.when((g < 2) & (g != k))
        def _(k=k):
            whole_copy(k, g).wait_send()

    @pl.when(g < 2)
    def _():
        for slot in (2, 3):
            relay_copy(slot, g).wait_send()

    @pl.when(g >= 2)
    def _():
        for k in range(2):
            half_copy(g, k).wait_send()

    @pl.when(g == 3)
    def _():
        whole_copy(2, 3).wait_send()


def compact_kernel(n_tile, base_ref, count_ref, coeff_ref, place_ref, out_ref, current):
    planes, rows, ny = coeff_ref.shape
    groups = ny // LANES
    out_ref[...] = jnp.zeros_like(out_ref)
    current[...] = jnp.zeros_like(current)
    rank = lax.broadcasted_iota(jnp.int32, (LANES, LANES), 0).astype(jnp.float32)
    lane = lax.broadcasted_iota(jnp.int32, (rows, LANES), 1)

    def sort(b):
        z, y = b // groups, b % groups
        value = coeff_ref[z, :, pl.ds(pl.multiple_of(y * LANES, LANES), LANES)]
        high = value.astype(jnp.bfloat16).astype(jnp.float32)
        rest = value - high
        mid = rest.astype(jnp.bfloat16).astype(jnp.float32)
        low = rest - mid
        parts = jnp.concatenate([high, mid, low], axis=0).astype(jnp.bfloat16)
        chosen = jnp.where(rank == place_ref[pl.ds(b, 1), :], 1.0, 0.0).astype(jnp.bfloat16)
        ordered = lax.dot_general(parts, chosen, (((1,), (1,)), ((), ())), preferred_element_type=jnp.float32)
        return (ordered[0:rows] + ordered[rows : 2 * rows]) + ordered[2 * rows : 3 * rows]

    def pencil(b, ordered, s, ahead):
        base, count = base_ref[b, s], count_ref[b, s]
        start = base & (LANES - 1)
        end = start + count
        turned = pltpu.roll(ordered, (start - ahead) & (LANES - 1), 1)
        now = current[s] + jnp.where((lane >= start) & (lane < end), turned, 0.0)
        group = pl.multiple_of(base - start, LANES)
        after = jnp.where(lane < end - LANES, turned, 0.0)
        current[s] = jnp.where(end >= LANES, after, now)
        out_ref[s, :, pl.ds(group, 2 * LANES)] = jnp.concatenate([now, after], axis=1)
        return ahead + count

    n_blocks = planes * groups
    batch = 8 if n_blocks % 8 == 0 and n_tile <= 16 else 1

    def blocks(i, _):
        ordered = [sort(i * batch + j) for j in range(batch)]
        for j in range(batch):
            b = i * batch + j
            if n_tile <= 16:
                ahead = jnp.int32(0)
                for s in range(n_tile):
                    ahead = pencil(b, ordered[j], s, ahead)
            else:
                lax.fori_loop(0, n_tile, lambda s, ahead: pencil(b, ordered[j], s, ahead), jnp.int32(0))
        return 0

    lax.fori_loop(0, n_blocks // batch, blocks, 0)


def record_kernel(n_tile, chunks, sent_ref, matrix_ref, out_ref, got, records, send_sem, recv_sem, rsend_sem, rrecv_sem):
    g, t = lax.axis_index("grp"), lax.axis_index("tile")
    rows, nx, cap = sent_ref.shape[1], out_ref.shape[0], out_ref.shape[1]
    width = cap // chunks

    barrier = pltpu.get_barrier_semaphore()

    @pl.when(g < 3)
    def _():
        for k in range(1, n_tile):
            pl.semaphore_signal(barrier, inc=1, device_id=(g, lax.rem(t + k, n_tile)), device_id_type=MESH)
        pl.semaphore_signal(barrier, inc=1, device_id=(3, t), device_id_type=MESH)
        pl.semaphore_wait(barrier, n_tile)

    @pl.when(g == 3)
    def _():
        for k in range(3):
            pl.semaphore_signal(barrier, inc=1, device_id=(k, t), device_id_type=MESH)
        pl.semaphore_wait(barrier, 3)

    def exchange(s, slot, c):
        part = pl.ds(c * width, width)
        return pltpu.make_async_remote_copy(
            src_ref=sent_ref.at[s, :, part], dst_ref=got.at[slot, :, part], send_sem=send_sem.at[s, c],
            recv_sem=recv_sem.at[slot, c], device_id=(g, s), device_id_type=MESH)

    def report(c, slot):
        part = pl.ds(c * width, width)
        return pltpu.make_async_remote_copy(
            src_ref=out_ref.at[:, part], dst_ref=records.at[slot, :, part], send_sem=rsend_sem.at[c],
            recv_sem=rrecv_sem.at[slot, c], device_id=(3, t), device_id_type=MESH)

    @pl.when(g < 3)
    def _():
        for c in range(chunks):
            for k in range(1, n_tile):
                exchange(lax.rem(t + k, n_tile), t, c).start()
        got[t] = sent_ref[t, :, 0:cap]
        matrix = matrix_ref[...]
        for c in range(chunks):
            for k in range(1, n_tile):
                exchange(lax.rem(t + k, n_tile), lax.rem(t + k, n_tile), c).wait_recv()
            value = got[:, :, c * width : (c + 1) * width].reshape(nx, width)
            out_ref[:, c * width : (c + 1) * width] = jnp.dot(
                matrix, value, precision=lax.Precision.HIGHEST, preferred_element_type=jnp.float32)
            report(c, g).start()
        for c in range(chunks):
            for k in range(1, n_tile):
                exchange(lax.rem(t + k, n_tile), t, c).wait_send()
            report(c, g).wait_send()

    @pl.when(g == 3)
    def _():
        for c in range(chunks):
            for k in range(3):
                report(c, k).wait_recv()
            part = slice(c * width, (c + 1) * width)
            first, second, third = records[0, :, part], records[1, :, part], records[2, :, part]
            out_ref[:, part] = first * first + second * second + third * third


def tiled_body(flow_state, line_owner, *, n_tile):
    _, planes, rows, ny = flow_state.shape
    n_lines = line_owner.shape[0]
    n_blocks = n_lines // LANES
    nx = rows * n_tile
    cap = 2 * planes * ny // n_tile
    vmem = pl.BlockSpec(memory_space=pltpu.VMEM)
    smem = pl.BlockSpec(memory_space=pltpu.SMEM)
    f32 = jnp.float32
    shape = jax.ShapeDtypeStruct
    limit = 16 * 1024 * 1024
    dma = pltpu.SemaphoreType.DMA
    owner = line_owner.reshape(n_blocks, LANES)
    tile = (planes, rows, ny)
    ints = shape((n_blocks, LANES), jnp.int32)
    coeffs, place, base, count = pl.pallas_call(
        functools.partial(flow_kernel, n_tile),
        out_shape=(shape(tile, f32), shape((n_blocks, LANES), f32), ints, ints),
        in_specs=[vmem, vmem], out_specs=(vmem, vmem, vmem, vmem),
        scratch_shapes=[
            pltpu.VMEM((4,) + tile, f32), pltpu.VMEM((3,) + tile, f32),
            pltpu.VMEM((4,) + tile, f32), pltpu.VMEM((2,) + tile, f32),
            pltpu.VMEM((planes, rows + 2 * reach, ny), f32), pltpu.VMEM((planes, rows + 2 * reach, ny), f32),
            pltpu.VMEM(tile, f32), pltpu.VMEM(tile, f32), pltpu.VMEM(tile, f32), pltpu.VMEM(tile, f32), pltpu.VMEM(tile, f32),
            dma((4,)), dma((4, 2)), dma((2,)), dma((4,)), dma((4,)), dma((4,)), dma((2,)), dma((2,)), dma((4,)),
            pltpu.VMEM((4 * LANES, 2 * LANES), f32),
        ],
        compiler_params=pltpu.CompilerParams(has_side_effects=True, collective_id=0, vmem_limit_bytes=limit), name="flow",
    )(flow_state, owner)
    sent = pl.pallas_call(
        functools.partial(compact_kernel, n_tile),
        out_shape=shape((n_tile, rows, cap + 2 * LANES), f32),
        in_specs=[smem, smem, vmem, vmem], out_specs=vmem,
        scratch_shapes=[pltpu.VMEM((n_tile, rows, LANES), f32)],
        compiler_params=pltpu.CompilerParams(vmem_limit_bytes=limit), name="compact",
    )(base, count, coeffs, place)
    chunks = 4 if cap % (4 * LANES) == 0 else 1
    record = pl.pallas_call(
        functools.partial(record_kernel, n_tile, chunks),
        out_shape=shape((nx, cap), f32),
        in_specs=[vmem, vmem], out_specs=vmem,
        scratch_shapes=[
            pltpu.VMEM((n_tile, rows, cap), f32), pltpu.VMEM((3, nx, cap), f32),
            dma((n_tile, chunks)), dma((n_tile, chunks)), dma((chunks,)), dma((3, chunks)),
        ],
        compiler_params=pltpu.CompilerParams(has_side_effects=True, collective_id=1, vmem_limit_bytes=limit), name="record",
    )(sent, jnp.asarray(lift_matrix(nx).astype(np.float32)))
    return record[None, None]


CHUNK = 64
SIDE = 16
SPARE = LANES - CHUNK - 2 * SIDE
SUB = 8


def planes_taps(planes):
    first, second = [0.0] * planes, [0.0] * planes
    second[0] = 3.0 * second_center
    for k in range(1, reach + 1):
        first[k % planes] += first_coeffs[k - 1]
        first[-k % planes] -= first_coeffs[k - 1]
        second[k % planes] += second_coeffs[k - 1]
        second[-k % planes] += second_coeffs[k - 1]
    return first, second


def column_taps():
    full = lift_matrix(8 * CHUNK)
    middle = 4 * CHUNK
    low = full[middle // 2, middle - 4 : middle + 5]
    high = full[8 * CHUNK // 2 + middle // 2, middle + 1 - 4 : middle + 1 + 5]
    return [float(x) for x in low], [float(x) for x in high]


def column_band():
    taps_low, taps_high = column_taps()
    part = CHUNK // 2
    row = lax.broadcasted_iota(jnp.int32, (2 * LANES, LANES), 0)
    column = lax.broadcasted_iota(jnp.int32, (2 * LANES, LANES), 1)
    is_low = column < CHUNK
    spot = SIDE + 2 * (column & (part - 1)) + jnp.where(is_low, 0, 1)
    same = (row // LANES) == ((column & (CHUNK - 1)) // part)
    distance = jnp.where(same, (row & (LANES - 1)) - spot, LANES)
    value = jnp.zeros((2 * LANES, LANES), jnp.float32)
    for offset in range(-4, 5):
        tap = jnp.where(is_low, taps_low[offset + 4], taps_high[offset + 4])
        value = jnp.where(distance == offset, tap, value)
    return value


def pencil_slots(pencil, owner, spot_ref, group_ref):
    n_blocks = owner.shape[0]
    upper = (lax.broadcasted_iota(jnp.int32, (LANES, LANES), 0) <= lax.broadcasted_iota(jnp.int32, (LANES, LANES), 1)).astype(jnp.float32)
    lower = (lax.broadcasted_iota(jnp.int32, (n_blocks, n_blocks), 0) > lax.broadcasted_iota(jnp.int32, (n_blocks, n_blocks), 1)).astype(jnp.float32)
    lane = lax.broadcasted_iota(jnp.int32, (n_blocks, LANES), 1)
    mine = owner == pencil
    mask = mine.astype(jnp.float32)
    within = jnp.dot(mask, upper, preferred_element_type=jnp.float32)
    total = jnp.broadcast_to(jnp.sum(mask, axis=1, keepdims=True), (n_blocks, LANES))
    base = jnp.dot(lower, total, preferred_element_type=jnp.float32).astype(jnp.int32)
    slot = base + within.astype(jnp.int32) - 1
    spot_ref[...] = jnp.where(mine, slot & (LANES - 1), -1)
    taken = ((lane - base) & (LANES - 1)) < total.astype(jnp.int32)
    group_ref[...] = jnp.where(taken, base // LANES + jnp.where(lane < (base & (LANES - 1)), 1, 0), -1)


def chunk_kernel(n_tile, own_hbm, owner_hbm, out_ref,
                 own, owner_ref, windows, arrived, fields, mids, slope, final, pieces, landed, spot_ref, group_ref, ordered, band_ref,
                 own_sem, owner_sem, send_sem, recv_sem, recv_two, hand_sem, side_sem, onward_sem, corner_sem):
    g, t = lax.axis_index("grp"), lax.axis_index("tile")
    planes, rows, ny = own.shape
    n_grp = 4
    n_dev = n_grp * n_tile
    nx = rows * n_tile
    half = nx // 2
    me = t * n_grp + g

    load = pltpu.make_async_copy(own_hbm.at[0], own, own_sem)
    load.start()
    load_owner = pltpu.make_async_copy(owner_hbm, owner_ref, owner_sem)
    load_owner.start()
    peers = [(lax.rem(g + k % n_grp, n_grp), lax.rem(t + k // n_grp, n_tile)) for k in range(1, n_dev)]
    barrier = pltpu.get_barrier_semaphore()
    for peer in peers:
        pl.semaphore_signal(barrier, inc=1, device_id=peer, device_id_type=MESH)
    load.wait()
    spread = lax.broadcasted_iota(jnp.int32, (rows, ny), 1) & (LANES - 1)
    for odd in range(2):
        turned = [pltpu.roll(own[z], (SIDE - odd * CHUNK) % ny, 1) for z in range(planes)]
        for z in range(planes - 1):
            moved = pltpu.roll(turned[planes - 1], LANES - SPARE * (z + 1), 1)
            mixed = jnp.where(spread < LANES - SPARE, turned[z], moved)
            for m in range(n_dev // 2):
                windows[2 * m + odd, z * rows : (z + 1) * rows] = mixed[:, m * LANES : (m + 1) * LANES]
    pl.semaphore_wait(barrier, n_dev - 1)

    packed = (planes - 1) * rows

    def deal(peer, source):
        to = peer[1] * n_grp + peer[0]
        return pltpu.make_async_remote_copy(
            src_ref=windows.at[to, pl.ds(0, packed)], dst_ref=arrived.at[source, pl.ds(0, packed)], send_sem=send_sem.at[to], recv_sem=recv_sem.at[source],
            device_id=peer, device_id_type=MESH)

    for peer in peers:
        deal(peer, me).start()
    arrived[me] = windows[me]

    load_owner.wait()
    pencil_slots(t, owner_ref[...], spot_ref, group_ref)
    out_ref[...] = jnp.zeros_like(out_ref)
    band_ref[...] = column_band()

    for peer in peers:
        deal(peer, peer[1] * n_grp + peer[0]).wait_recv()

    sublane = lax.broadcasted_iota(jnp.int32, (reach, SUB, LANES), 1)

    def flip(value):
        return jnp.where((sublane & 1) == 0, pltpu.roll(value, SUB - 1, 1), pltpu.roll(value, 1, 1))

    def wrap(ref, c):
        ref[c, 0:reach] = flip(ref[c, half : half + reach])
        ref[c, half + reach : half + 2 * reach] = flip(ref[c, reach : 2 * reach])

    spot = lax.broadcasted_iota(jnp.int32, (rows, LANES), 1)
    for f in range(n_grp):
        for tile in range(n_tile):
            source = tile * n_grp + f
            last = None
            for z in range(planes - 1):
                piece = pltpu.roll(arrived[source, z * rows : (z + 1) * rows], SPARE * (z + 1), 1)
                last = piece if last is None else jnp.where(spot < SPARE * z, last, piece)
            arrived[source, packed : packed + rows] = last
            side, first = tile // (n_tile // 2), (tile % (n_tile // 2)) * rows
            for r in range(rows):
                fields[f, reach + first + r, pl.ds(side, planes, stride=2), :] = arrived[tile * n_grp + f, pl.ds(r, planes, stride=rows), :]
        wrap(fields, f)

    z_first, z_second = planes_taps(planes)
    step = rows * 2

    def turn_z(value, m):
        return value if m == 0 else pltpu.roll(value, (-2 * m) % SUB, 1)

    def turn_y(value, k):
        return pltpu.roll(value, (-k) % LANES, 2)

    def gradient(i, direction):
        if direction == 0:
            shift = lambda k: fields[3, reach + i + k : reach + i + k + step]
        else:
            center = fields[3, reach + i : reach + i + step]
            if direction == 1:
                shift = lambda k: turn_y(center, k)
            else:
                total = None
                for m in range(1, planes):
                    if z_first[m] != 0.0:
                        term = z_first[m] * turn_z(center, m)
                        total = term if total is None else total + term
                return total
        value, _ = derivatives(None, shift, True, False)
        return value

    def tendency(ref, c, i, speed, press):
        center = ref[c, reach + i : reach + i + step]
        total = z_second[0] * center
        slope_z = None
        for m in range(1, planes):
            turned = turn_z(center, m)
            total = total + z_second[m] * turned
            if z_first[m] != 0.0:
                term = z_first[m] * turned
                slope_z = term if slope_z is None else slope_z + term
        slope_x, slope_y = None, None
        for k in range(1, reach + 1):
            ahead, behind = ref[c, reach + i + k : reach + i + k + step], ref[c, reach + i - k : reach + i - k + step]
            up, down = turn_y(center, k), turn_y(center, -k)
            term_x, term_y = first_coeffs[k - 1] * (ahead - behind), first_coeffs[k - 1] * (up - down)
            slope_x = term_x if slope_x is None else slope_x + term_x
            slope_y = term_y if slope_y is None else slope_y + term_y
            total = total + second_coeffs[k - 1] * ((ahead + behind) + (up + down))
        advect = speed[0] * slope_x + speed[1] * slope_y + speed[2] * slope_z
        return viscosity * total - advect - press, center

    def first_section(b, _):
        i = b * step
        speed = [fields[f, reach + i : reach + i + step] if isinstance(i, int) else fields[f, pl.ds(reach + i, step)] for f in range(3)]
        for c in range(3):
            press = gradient(i, c)
            slope[c, i : i + step] = press
            change, center = tendency(fields, c, i, speed, press)
            mids[c, reach + i : reach + i + step] = center + time_step * change
        return 0

    def second_section(b, c):
        i = b * step
        speed = [mids[f, reach + i : reach + i + step] for f in range(3)]
        change, center = tendency(mids, c, i, speed, slope[c, i : i + step])
        final[c, i : i + step] = 0.5 * ((fields[c, reach + i : reach + i + step] + center) + time_step * change)

    for b in range(half // step):
        first_section(b, 0)
    for c in range(3):
        wrap(mids, c)
    flat = lax.broadcasted_iota(jnp.int32, (SUB, LANES), 0)

    def flip_one(value):
        return jnp.where((flat & 1) == 0, pltpu.roll(value, SUB - 1, 0), pltpu.roll(value, 1, 0))

    matrix = lift_matrix(planes)
    z_coeffs = []
    for m in range(planes):
        column = jnp.zeros((SUB, LANES), jnp.float32)
        for z in range(planes):
            column = jnp.where(flat // 2 == z, float(matrix[z, (z + m) % planes]), column)
        z_coeffs.append(column)

    def lift_z(value):
        total = z_coeffs[0] * value
        for m in range(1, planes):
            total = total + z_coeffs[m] * pltpu.roll(value, (-2 * m) % SUB, 0)
        return total

    pairs = half // 2
    z, y = t // 2, t % 2
    n_z = n_tile // 2

    def flipped(value, bits):
        result, place = 0, 1
        while place < n_z:
            result = result + place * lax.rem(value // place + bits // place, 2)
            place *= 2
        return result

    partner = flipped(z, 1)

    def source_of(level, column, group):
        return (level * 2 + column) * n_grp + group

    def send(origin, source, sem, group, level, column):
        return pltpu.make_async_remote_copy(
            src_ref=origin, dst_ref=landed.at[source], send_sem=sem, recv_sem=recv_two.at[source],
            device_id=(group, level * 2 + column), device_id_type=MESH)

    kin = [g, g + 1 - 2 * lax.rem(g, 2), lax.rem(g + 2, n_grp), n_grp - 1 - g]
    across = (0, 2, 3, 1)
    routes = ((3, 0), (0, 1), (1, 0), (0, 0))

    def hand(bits, other, c):
        return send(pieces.at[c], me, hand_sem.at[bits + 2 * other, c], c, flipped(z, bits), lax.rem(y + other, 2))

    def each_hand(c, act):
        for bits, other in routes:
            if bits or other:
                act(hand(bits, other, c))
            else:
                @pl.when(g != c)
                def _():
                    act(hand(bits, other, c))

    def side(source):
        return send(landed.at[source], source, side_sem.at[source], g, z, 1 - y)

    def onward(source):
        return send(landed.at[source], source, onward_sem.at[source], g, partner, y)

    skipped, crossed = (), (1, 2, 3)

    def corner(source):
        return send(landed.at[source], source, corner_sem.at[source], g, partner, 1 - y)

    def await_piece(source):
        send(pieces.at[g], source, hand_sem.at[0, 0], g, z, 1 - y).wait_recv()

    def finish(c):
        even = [lift_z(final[c, 2 * i]) for i in range(pairs)]
        odd = [lift_z(final[c, 2 * i + 1]) for i in range(pairs)]
        for odd_tap, even_tap in ((lift_alpha, lift_beta), (lift_gamma, lift_delta)):
            after = even[1:] + [flip_one(even[0])]
            odd = [odd[i] + odd_tap * (even[i] + after[i]) for i in range(pairs)]
            before = [flip_one(odd[-1])] + odd[:-1]
            even = [even[i] + even_tap * (odd[i] + before[i]) for i in range(pairs)]
        for i in range(pairs):
            final[c, i] = even[i] * lift_scale
            final[c, pairs + i] = odd[i] * (1.0 / lift_scale)
        flat_ref = final.at[c].reshape(half * SUB, LANES)
        stacked = []
        for pair in range(2):
            for high in range(2):
                for a in range(2):
                    stacked.append(jnp.concatenate([flat_ref[pl.ds(high * pairs * SUB + 2 * z_at + a, pairs, stride=SUB), :] for z_at in (2 * pair, 2 * pair + 1)], axis=1))
        lines = jnp.dot(jnp.concatenate(stacked, axis=0), band_ref[...], precision=lax.Precision.HIGHEST, preferred_element_type=jnp.float32)
        near, beyond = lines[0:nx], lines[nx : 2 * nx]
        is_near = lax.broadcasted_iota(jnp.int32, (nx, LANES), 1) < CHUNK
        pieces[c, :, 0:LANES] = jnp.where(is_near, near, pltpu.roll(beyond, CHUNK, 1))
        pieces[c, :, LANES : 2 * LANES] = jnp.where(is_near, pltpu.roll(near, CHUNK, 1), beyond)

    for c in (0, 2, 1):
        for b in range(half // step):
            second_section(b, c)
        finish(c)
        each_hand(c, lambda copy: copy.start())
    pieces[3] = pieces[0] * pieces[0] + pieces[1] * pieces[1] + pieces[2] * pieces[2]
    each_hand(3, lambda copy: copy.start())
    rank = lax.broadcasted_iota(jnp.int32, (LANES, LANES), 0)
    n_groups = n_tile
    lane_part = lax.broadcasted_iota(jnp.int32, (nx, LANES), 1) // (CHUNK // 2)

    def select(tile):
        for high in range(2):
            tiles = [landed[tile * n_grp + m, :, high * LANES : (high + 1) * LANES] for m in range(4)]
            for bit in range(2):
                distance = (CHUNK // 2) << bit
                is_low = (lane_part & (1 << bit)) == 0
                turned = list(tiles)
                for m in range(4):
                    if not m & (1 << bit):
                        other = m | (1 << bit)
                        turned[m] = jnp.where(is_low, tiles[m], pltpu.roll(tiles[other], distance, 1))
                        turned[other] = jnp.where(is_low, pltpu.roll(tiles[m], LANES - distance, 1), tiles[other])
                tiles = turned
            for plane in range(planes):
                block = (plane * 2 + high) * n_groups + tile
                value = tiles[plane]
                first = value.astype(jnp.bfloat16).astype(jnp.float32)
                rest = value - first
                second = rest.astype(jnp.bfloat16).astype(jnp.float32)
                stack = jnp.concatenate([first, second, rest - second], axis=0).astype(jnp.bfloat16)
                chosen = jnp.where(rank == spot_ref[pl.ds(block, 1), :], 1.0, 0.0).astype(jnp.bfloat16)
                placed = lax.dot_general(stack, chosen, (((1,), (1,)), ((), ())), preferred_element_type=jnp.float32)
                ordered[plane * 2 + high] = (placed[0:nx] + placed[nx : 2 * nx]) + placed[2 * nx : 3 * nx]
        labels = [group_ref[pl.ds((plane * 2 + high) * n_groups + tile, 1), :] for plane in range(planes) for high in range(2)]
        for q in range(out_ref.shape[1] // LANES):
            total = out_ref[:, q * LANES : (q + 1) * LANES]
            for n, label in enumerate(labels):
                total = jnp.where(label == q, ordered[n], total)
            out_ref[:, q * LANES : (q + 1) * LANES] = total

    landed[me] = pieces[g]

    def sideways(bits, k):
        return bits == 3 or (bits == 2 and k not in skipped) or (bits == 1 and k not in crossed)

    def receive(bits):
        for k in across:
            source = source_of(flipped(z, bits), y, kin[k])
            if bits or k:
                await_piece(source)
            if bits == 3:
                onward(source).start()
                if k in skipped:
                    corner(source).start()
            if sideways(bits, k):
                side(source).start()
        if bits == 0:
            for k in across:
                source = source_of(z, 1 - y, kin[k])
                await_piece(source)
                if k in crossed:
                    onward(source).start()

    for peer in peers:
        deal(peer, me).wait_send()

    for bits in (3, 0, 1):
        receive(bits)

    def from_other(bits):
        for k in across:
            await_piece(source_of(flipped(z, bits), 1 - y, kin[k]))

    def pick(bits, other):
        select(flipped(z, bits) * 2 + lax.rem(y + other, 2))

    pick(0, 0)
    receive(2)
    pick(0, 1)
    pick(1, 0)
    pick(3, 0)
    pick(2, 0)
    for bits in (3, 1):
        from_other(bits)
        pick(bits, 1)
    for c in range(n_grp):
        each_hand(c, lambda copy: copy.wait_send())
    for k in across:
        for bits in range(1, n_z):
            source = source_of(flipped(z, bits), y, kin[k])
            if sideways(bits, k):
                side(source).wait_send()
        onward(source_of(flipped(z, 3), y, kin[k])).wait_send()
        if k in skipped:
            corner(source_of(flipped(z, 3), y, kin[k])).wait_send()
        if k in crossed:
            onward(source_of(z, 1 - y, kin[k])).wait_send()
    from_other(2)
    pick(2, 1)


def chunk_body(flow_state, line_owner, *, n_tile):
    _, planes, rows, ny = flow_state.shape
    n_lines = line_owner.shape[0]
    n_blocks = n_lines // LANES
    nx = rows * n_tile
    half = nx // 2
    n_dev = 4 * n_tile
    cap = 2 * planes * ny // n_tile
    f32 = jnp.float32
    dma = pltpu.SemaphoreType.DMA
    hbm = pl.BlockSpec(memory_space=pltpu.HBM)
    padded = (half + 2 * reach, SUB, LANES)
    record = pl.pallas_call(
        functools.partial(chunk_kernel, n_tile),
        out_shape=jax.ShapeDtypeStruct((nx, cap), f32),
        in_specs=[hbm, hbm], out_specs=pl.BlockSpec(memory_space=pltpu.VMEM),
        scratch_shapes=[
            pltpu.VMEM((planes, rows, ny), f32), pltpu.VMEM((n_blocks, LANES), jnp.int32),
            pltpu.VMEM((n_dev, planes * rows, LANES), f32), pltpu.VMEM((n_dev, planes * rows, LANES), f32),
            pltpu.VMEM((4,) + padded, f32), pltpu.VMEM((3,) + padded, f32),
            pltpu.VMEM((3, half, SUB, LANES), f32), pltpu.VMEM((3, half, SUB, LANES), f32),
            pltpu.VMEM((4, nx, 2 * LANES), f32), pltpu.VMEM((n_dev, nx, 2 * LANES), f32),
            pltpu.VMEM((n_blocks, LANES), jnp.int32), pltpu.VMEM((n_blocks, LANES), jnp.int32),
            pltpu.VMEM((2 * planes, nx, LANES), f32), pltpu.VMEM((2 * LANES, LANES), f32),
            dma, dma, dma((n_dev,)), dma((n_dev,)), dma((n_dev,)), dma((4, 4)), dma((n_dev,)), dma((n_dev,)), dma((n_dev,)),
        ],
        compiler_params=pltpu.CompilerParams(has_side_effects=True, collective_id=0, vmem_limit_bytes=16 * 1024 * 1024), name="record",
    )(pltpu.with_memory_space_constraint(flow_state, pltpu.HBM), pltpu.with_memory_space_constraint(line_owner.reshape(n_blocks, LANES), pltpu.HBM))
    return record[None, None]


def fits_chunks(mesh, planes, rows, ny):
    n_tile = mesh.shape["tile"]
    return 2 * planes == SUB and 2 * rows == SUB and mesh.shape["grp"] == 4 and ny == 4 * n_tile * CHUNK and n_tile == 8


def solution(mesh):
    in_specs = (P("grp", None, "tile", None), P())
    out_specs = P("grp", "tile", None, None)
    n_tile = mesh.shape["tile"]

    def run(flow_state, line_owner):
        _, planes, rows, ny = flow_state.shape
        chosen = chunk_body if fits_chunks(mesh, planes, rows, ny) else tiled_body
        return chosen(flow_state, line_owner, n_tile=n_tile)

    return jax.shard_map(run, mesh=mesh, in_specs=in_specs, out_specs=out_specs, check_vma=False)
```

```python
import functools

import jax
import jax.numpy as jnp
import numpy as np
from jax import lax
from jax.experimental import pallas as pl
from jax.experimental.pallas import tpu as pltpu
from jax.sharding import PartitionSpec as P

time_step = 0.2
viscosity = 0.05
reach = 4
first_coeffs = (0.8, -0.2, 4.0 / 105.0, -1.0 / 280.0)
second_center = -205.0 / 72.0
second_coeffs = (1.6, -0.2, 8.0 / 315.0, -1.0 / 560.0)
lift_alpha = -1.586134342059924
lift_beta = -0.052980118572961
lift_gamma = 0.882911075530934
lift_delta = 0.443506852043971
lift_scale = 1.149604398860241
LANES = 128
MESH = pl.DeviceIdType.MESH


def lift_numpy(signal):
    even, odd = signal[0::2].copy(), signal[1::2].copy()
    odd += lift_alpha * (even + np.roll(even, -1, 0))
    even += lift_beta * (odd + np.roll(odd, 1, 0))
    odd += lift_gamma * (even + np.roll(even, -1, 0))
    even += lift_delta * (odd + np.roll(odd, 1, 0))
    return np.concatenate([even * lift_scale, odd / lift_scale])


def lift_matrix(length):
    return lift_numpy(np.eye(length))


def band_matrix():
    full = lift_matrix(8 * LANES)
    low = full[LANES : 2 * LANES, LANES : 5 * LANES]
    high = full[4 * LANES + LANES : 4 * LANES + 2 * LANES, LANES : 5 * LANES]
    return np.concatenate([low, high]).T.astype(np.float32)


def band_value(taps_low, taps_high):
    row = lax.broadcasted_iota(jnp.int32, (4 * LANES, 2 * LANES), 0)
    column = lax.broadcasted_iota(jnp.int32, (4 * LANES, 2 * LANES), 1)
    distance = row - LANES - 2 * (column & (LANES - 1))
    is_low = column < LANES
    value = jnp.zeros((4 * LANES, 2 * LANES), jnp.float32)
    for offset in range(-4, 5):
        tap = jnp.where(is_low, taps_low[offset + 4], taps_high[offset + 4])
        value = jnp.where(distance == offset, tap, value)
    return value


def band_taps():
    band = band_matrix()
    rows = slice(LANES + LANES // 2 - 4, LANES + LANES // 2 + 5)
    return [float(x) for x in band[rows, LANES // 4]], [float(x) for x in band[rows, LANES + LANES // 4]]


def shifted_y(value, k):
    return pltpu.roll(value, (-k) % value.shape[-1], value.ndim - 1)


def derivatives(center, shift, want_first=True, want_second=True):
    first, second = None, second_center * center if want_second else None
    for k in range(1, reach + 1):
        ahead, behind = shift(k), shift(-k)
        if want_first:
            term = first_coeffs[k - 1] * (ahead - behind)
            first = term if first is None else first + term
        if want_second:
            second = second + second_coeffs[k - 1] * (ahead + behind)
    return first, second


def slots_of(n_tile, owner_ref, place_ref, base_ref, count_ref):
    owner = owner_ref[...]
    n_blocks = owner.shape[0]
    upper = (lax.broadcasted_iota(jnp.int32, (LANES, LANES), 0) <= lax.broadcasted_iota(jnp.int32, (LANES, LANES), 1)).astype(jnp.float32)
    lower = (lax.broadcasted_iota(jnp.int32, (n_blocks, n_blocks), 0) > lax.broadcasted_iota(jnp.int32, (n_blocks, n_blocks), 1)).astype(jnp.float32)
    lane = lax.broadcasted_iota(jnp.int32, (n_blocks, LANES), 1)

    def step(s, carry):
        place, counts, ahead = carry
        mask = (owner == s).astype(jnp.float32)
        within = jnp.dot(mask, upper, preferred_element_type=jnp.float32)
        total = jnp.sum(mask, axis=1, keepdims=True)
        place = place + mask * (ahead + within - 1.0)
        counts = jnp.where(lane == s, total, counts)
        return place, counts, ahead + total

    zeros = jnp.zeros((n_blocks, LANES), jnp.float32)
    carry = (zeros, zeros, jnp.zeros((n_blocks, 1), jnp.float32))
    if n_tile <= 16:
        for s in range(n_tile):
            carry = step(s, carry)
    else:
        carry = lax.fori_loop(0, n_tile, step, carry)
    place, counts, _ = carry
    place_ref[...] = place
    count_ref[...] = counts.astype(jnp.int32)
    base_ref[...] = jnp.dot(lower, counts, preferred_element_type=jnp.float32).astype(jnp.int32)


def flow_kernel(n_tile, own_ref, owner_ref, out_ref, place_ref, base_ref, count_ref,
                fields, mids, halo, mid_halo, pad, ppad, middle, fin, along_y, along_z, lap, send_sem, recv_sem, hsend_sem, hrecv_sem, msend_sem, mrecv_sem, mhsend_sem, mhrecv_sem, relay_sem, band_ref):
    g, t = lax.axis_index("grp"), lax.axis_index("tile")
    right, left = lax.rem(t + 1, n_tile), lax.rem(t + n_tile - 1, n_tile)
    planes, rows, ny = own_ref.shape[1:]
    own = own_ref.at[0]

    barrier = pltpu.get_barrier_semaphore()
    for k in range(1, 4):
        pl.semaphore_signal(barrier, inc=1, device_id=(lax.rem(g + k, 4), t), device_id_type=MESH)
    for side in (right, left):
        pl.semaphore_signal(barrier, inc=1, device_id=(g, side), device_id_type=MESH)

    @pl.when((g == 0) | (g == 3))
    def _():
        for side in (right, left):
            pl.semaphore_signal(barrier, inc=1, device_id=(3 - g, side), device_id_type=MESH)
        pl.semaphore_wait(barrier, 7)

    @pl.when((g == 1) | (g == 2))
    def _():
        pl.semaphore_wait(barrier, 5)

    def gather_copy(src, dst, ssem, rsem, k, slot):
        return pltpu.make_async_remote_copy(
            src_ref=src, dst_ref=dst.at[slot], send_sem=ssem.at[k], recv_sem=rsem.at[slot],
            device_id=(k, t), device_id_type=MESH)

    half = planes // 2

    def whole_copy(k, slot):
        return pltpu.make_async_remote_copy(
            src_ref=own, dst_ref=fields.at[slot], send_sem=send_sem.at[k], recv_sem=recv_sem.at[slot, 0],
            device_id=(k, t), device_id_type=MESH)

    def half_copy(slot, k):
        part = pl.ds(k * half, half)
        return pltpu.make_async_remote_copy(
            src_ref=own.at[part], dst_ref=fields.at[slot, part], send_sem=send_sem.at[k],
            recv_sem=recv_sem.at[slot, k], device_id=(k, t), device_id_type=MESH)

    def relay_copy(slot, k):
        part = pl.ds(k * half, half)
        return pltpu.make_async_remote_copy(
            src_ref=fields.at[slot, part], dst_ref=fields.at[slot, part], send_sem=relay_sem.at[slot],
            recv_sem=recv_sem.at[slot, k], device_id=(1 - k, t), device_id_type=MESH)

    def halo_copy(src, dst, ssem, rsem, side, slot, group):
        return pltpu.make_async_remote_copy(
            src_ref=src, dst_ref=dst.at[slot + side], send_sem=ssem.at[side], recv_sem=rsem.at[slot + side],
            device_id=(group, right if side == 0 else left), device_id_type=MESH)

    @pl.when(g < 3)
    def _():
        for side in range(2):
            halo_copy(own, halo, hsend_sem, hrecv_sem, side, 0, g).start()

    for k in range(3):
        @pl.when((g < 2) & (g != k))
        def _(k=k):
            whole_copy(k, g).start()

    @pl.when(g >= 2)
    def _():
        for k in range(2):
            half_copy(g, k).start()

    @pl.when(g == 3)
    def _():
        whole_copy(2, 3).start()
        for side in range(2):
            halo_copy(own, halo, hsend_sem, hrecv_sem, side, 2, 0).start()

    def local_terms():
        for z in range(planes):
            center = pad[z, reach : reach + rows]
            fy, sy = derivatives(center, lambda k: shifted_y(center, k))
            fz, sz = derivatives(center, lambda k: pad[(z + k) % planes, reach : reach + rows])
            along_y[z], along_z[z], lap[z] = fy, fz, sy + sz

    slots_of(n_tile, owner_ref, place_ref, base_ref, count_ref)
    band_ref[...] = band_value(*band_taps())

    @pl.when(g < 3)
    def _():
        for k in range(3):
            @pl.when(g == k)
            def _(k=k):
                fields[k] = own_ref[0]

        for z in range(planes):
            pad[z, reach : reach + rows] = own_ref[0, z]
        local_terms()

        @pl.when(g < 2)
        def _():
            for slot in (2, 3):
                half_copy(slot, g).wait_recv()
                relay_copy(slot, g).start()
            whole_copy(0, 1 - g).wait_recv()
            for slot in (2, 3):
                half_copy(slot, 1 - g).wait_recv()

        @pl.when(g == 2)
        def _():
            for slot in (0, 1, 3):
                whole_copy(0, slot).wait_recv()

        for side in range(2):
            halo_copy(own, halo, hsend_sem, hrecv_sem, side, 0, g).wait_recv()

        @pl.when(g == 0)
        def _():
            for side in range(2):
                halo_copy(own, halo, hsend_sem, hrecv_sem, side, 2, 0).wait_recv()
            for z in range(planes):
                ppad[z, 0:reach] = halo[2, z, rows - reach : rows]
                ppad[z, reach : reach + rows] = fields[3, z]
                ppad[z, reach + rows : 2 * reach + rows] = halo[3, z, 0:reach]
            for z in range(planes):
                middle[z], _ = derivatives(None, lambda k: ppad[z, reach + k : reach + k + rows], True, False)

        @pl.when(g == 1)
        def _():
            for z in range(planes):
                value = fields[3, z]
                middle[z], _ = derivatives(None, lambda k: shifted_y(value, k), True, False)

        @pl.when(g == 2)
        def _():
            for z in range(planes):
                middle[z], _ = derivatives(None, lambda k: fields[3, (z + k) % planes], True, False)

        def tendency(z, vel, press):
            center = pad[z, reach : reach + rows]
            fx, sx = derivatives(center, lambda k: pad[z, reach + k : reach + k + rows])
            advect = vel[0, z] * fx + vel[1, z] * along_y[z] + vel[2, z] * along_z[z]
            return viscosity * (sx + lap[z]) - advect - press

        for z in range(planes):
            pad[z, 0:reach] = halo[0, z, rows - reach : rows]
            pad[z, reach + rows : 2 * reach + rows] = halo[1, z, 0:reach]
        for z in range(planes):
            press = middle[z]
            ppad[z, 0:rows] = press
        for z in range(planes):
            middle[z] = own_ref[0, z] + time_step * tendency(z, fields, ppad[z, 0:rows])

        for side in range(2):
            halo_copy(middle, mid_halo, mhsend_sem, mhrecv_sem, side, 0, g).start()
        for k in range(3):
            @pl.when(g != k)
            def _(k=k):
                gather_copy(middle, mids, msend_sem, mrecv_sem, k, g).start()

            @pl.when(g == k)
            def _(k=k):
                mids[k] = middle[...]

        for z in range(planes):
            pad[z, reach : reach + rows] = middle[z]
        local_terms()
        for k in range(3):
            @pl.when(g != k)
            def _(k=k):
                gather_copy(middle, mids, msend_sem, mrecv_sem, 0, k).wait_recv()
        for side in range(2):
            halo_copy(middle, mid_halo, mhsend_sem, mhrecv_sem, side, 0, g).wait_recv()
        for z in range(planes):
            pad[z, 0:reach] = mid_halo[0, z, rows - reach : rows]
            pad[z, reach + rows : 2 * reach + rows] = mid_halo[1, z, 0:reach]
        for z in range(planes):
            fin[z] = 0.5 * ((own_ref[0, z] + middle[z]) + time_step * tendency(z, mids, ppad[z, 0:rows]))

        blocks = ny // (2 * LANES)
        groups = ny // LANES
        for z in range(planes):
            value = fin[z]
            pieces = []
            for b in range(blocks):
                window = [value[:, ((2 * b + j) % groups) * LANES : ((2 * b + j) % groups + 1) * LANES] for j in (-1, 0, 1, 2)]
                pieces.append(jnp.concatenate(window, axis=1))
            stacked = jnp.concatenate(pieces, axis=0)
            lifted = jnp.dot(stacked, band_ref[...], precision=lax.Precision.HIGHEST, preferred_element_type=jnp.float32)
            for b in range(blocks):
                piece = lifted[b * rows : (b + 1) * rows]
                fin[z, :, b * LANES : (b + 1) * LANES] = piece[:, 0:LANES]
                fin[z, :, ny // 2 + b * LANES : ny // 2 + (b + 1) * LANES] = piece[:, LANES:]

        even = [fin[2 * i] for i in range(half)]
        odd = [fin[2 * i + 1] for i in range(half)]
        odd = [odd[i] + lift_alpha * (even[i] + even[(i + 1) % half]) for i in range(half)]
        even = [even[i] + lift_beta * (odd[i] + odd[(i - 1) % half]) for i in range(half)]
        odd = [odd[i] + lift_gamma * (even[i] + even[(i + 1) % half]) for i in range(half)]
        even = [even[i] + lift_delta * (odd[i] + odd[(i - 1) % half]) for i in range(half)]
        for i in range(half):
            out_ref[i] = even[i] * lift_scale
            out_ref[half + i] = odd[i] * (1.0 / lift_scale)

        for side in range(2):
            halo_copy(middle, mid_halo, mhsend_sem, mhrecv_sem, side, 0, g).wait_send()
        for k in range(3):
            @pl.when(g != k)
            def _(k=k):
                gather_copy(middle, mids, msend_sem, mrecv_sem, k, g).wait_send()

    @pl.when(g == 3)
    def _():
        out_ref[...] = jnp.zeros_like(out_ref)

    for side in range(2):
        halo_copy(own, halo, hsend_sem, hrecv_sem, side, 0, g).wait_send()
    for k in range(3):
        @pl.when((g < 2) & (g != k))
        def _(k=k):
            whole_copy(k, g).wait_send()

    @pl.when(g < 2)
    def _():
        for slot in (2, 3):
            relay_copy(slot, g).wait_send()

    @pl.when(g >= 2)
    def _():
        for k in range(2):
            half_copy(g, k).wait_send()

    @pl.when(g == 3)
    def _():
        whole_copy(2, 3).wait_send()


def compact_kernel(n_tile, base_ref, count_ref, coeff_ref, place_ref, out_ref, current):
    planes, rows, ny = coeff_ref.shape
    groups = ny // LANES
    out_ref[...] = jnp.zeros_like(out_ref)
    current[...] = jnp.zeros_like(current)
    rank = lax.broadcasted_iota(jnp.int32, (LANES, LANES), 0).astype(jnp.float32)
    lane = lax.broadcasted_iota(jnp.int32, (rows, LANES), 1)

    def sort(b):
        z, y = b // groups, b % groups
        value = coeff_ref[z, :, pl.ds(pl.multiple_of(y * LANES, LANES), LANES)]
        high = value.astype(jnp.bfloat16).astype(jnp.float32)
        rest = value - high
        mid = rest.astype(jnp.bfloat16).astype(jnp.float32)
        low = rest - mid
        parts = jnp.concatenate([high, mid, low], axis=0).astype(jnp.bfloat16)
        chosen = jnp.where(rank == place_ref[pl.ds(b, 1), :], 1.0, 0.0).astype(jnp.bfloat16)
        ordered = lax.dot_general(parts, chosen, (((1,), (1,)), ((), ())), preferred_element_type=jnp.float32)
        return (ordered[0:rows] + ordered[rows : 2 * rows]) + ordered[2 * rows : 3 * rows]

    def pencil(b, ordered, s, ahead):
        base, count = base_ref[b, s], count_ref[b, s]
        start = base & (LANES - 1)
        end = start + count
        turned = pltpu.roll(ordered, (start - ahead) & (LANES - 1), 1)
        now = current[s] + jnp.where((lane >= start) & (lane < end), turned, 0.0)
        group = pl.multiple_of(base - start, LANES)
        after = jnp.where(lane < end - LANES, turned, 0.0)
        current[s] = jnp.where(end >= LANES, after, now)
        out_ref[s, :, pl.ds(group, 2 * LANES)] = jnp.concatenate([now, after], axis=1)
        return ahead + count

    n_blocks = planes * groups
    batch = 8 if n_blocks % 8 == 0 and n_tile <= 16 else 1

    def blocks(i, _):
        ordered = [sort(i * batch + j) for j in range(batch)]
        for j in range(batch):
            b = i * batch + j
            if n_tile <= 16:
                ahead = jnp.int32(0)
                for s in range(n_tile):
                    ahead = pencil(b, ordered[j], s, ahead)
            else:
                lax.fori_loop(0, n_tile, lambda s, ahead: pencil(b, ordered[j], s, ahead), jnp.int32(0))
        return 0

    lax.fori_loop(0, n_blocks // batch, blocks, 0)


def record_kernel(n_tile, chunks, sent_ref, matrix_ref, out_ref, got, records, send_sem, recv_sem, rsend_sem, rrecv_sem):
    g, t = lax.axis_index("grp"), lax.axis_index("tile")
    rows, nx, cap = sent_ref.shape[1], out_ref.shape[0], out_ref.shape[1]
    width = cap // chunks

    barrier = pltpu.get_barrier_semaphore()

    @pl.when(g < 3)
    def _():
        for k in range(1, n_tile):
            pl.semaphore_signal(barrier, inc=1, device_id=(g, lax.rem(t + k, n_tile)), device_id_type=MESH)
        pl.semaphore_signal(barrier, inc=1, device_id=(3, t), device_id_type=MESH)
        pl.semaphore_wait(barrier, n_tile)

    @pl.when(g == 3)
    def _():
        for k in range(3):
            pl.semaphore_signal(barrier, inc=1, device_id=(k, t), device_id_type=MESH)
        pl.semaphore_wait(barrier, 3)

    def exchange(s, slot, c):
        part = pl.ds(c * width, width)
        return pltpu.make_async_remote_copy(
            src_ref=sent_ref.at[s, :, part], dst_ref=got.at[slot, :, part], send_sem=send_sem.at[s, c],
            recv_sem=recv_sem.at[slot, c], device_id=(g, s), device_id_type=MESH)

    def report(c, slot):
        part = pl.ds(c * width, width)
        return pltpu.make_async_remote_copy(
            src_ref=out_ref.at[:, part], dst_ref=records.at[slot, :, part], send_sem=rsend_sem.at[c],
            recv_sem=rrecv_sem.at[slot, c], device_id=(3, t), device_id_type=MESH)

    @pl.when(g < 3)
    def _():
        for c in range(chunks):
            for k in range(1, n_tile):
                exchange(lax.rem(t + k, n_tile), t, c).start()
        got[t] = sent_ref[t, :, 0:cap]
        matrix = matrix_ref[...]
        for c in range(chunks):
            for k in range(1, n_tile):
                exchange(lax.rem(t + k, n_tile), lax.rem(t + k, n_tile), c).wait_recv()
            value = got[:, :, c * width : (c + 1) * width].reshape(nx, width)
            out_ref[:, c * width : (c + 1) * width] = jnp.dot(
                matrix, value, precision=lax.Precision.HIGHEST, preferred_element_type=jnp.float32)
            report(c, g).start()
        for c in range(chunks):
            for k in range(1, n_tile):
                exchange(lax.rem(t + k, n_tile), t, c).wait_send()
            report(c, g).wait_send()

    @pl.when(g == 3)
    def _():
        for c in range(chunks):
            for k in range(3):
                report(c, k).wait_recv()
            part = slice(c * width, (c + 1) * width)
            first, second, third = records[0, :, part], records[1, :, part], records[2, :, part]
            out_ref[:, part] = first * first + second * second + third * third


def tiled_body(flow_state, line_owner, *, n_tile):
    _, planes, rows, ny = flow_state.shape
    n_lines = line_owner.shape[0]
    n_blocks = n_lines // LANES
    nx = rows * n_tile
    cap = 2 * planes * ny // n_tile
    vmem = pl.BlockSpec(memory_space=pltpu.VMEM)
    smem = pl.BlockSpec(memory_space=pltpu.SMEM)
    f32 = jnp.float32
    shape = jax.ShapeDtypeStruct
    limit = 16 * 1024 * 1024
    dma = pltpu.SemaphoreType.DMA
    owner = line_owner.reshape(n_blocks, LANES)
    tile = (planes, rows, ny)
    ints = shape((n_blocks, LANES), jnp.int32)
    coeffs, place, base, count = pl.pallas_call(
        functools.partial(flow_kernel, n_tile),
        out_shape=(shape(tile, f32), shape((n_blocks, LANES), f32), ints, ints),
        in_specs=[vmem, vmem], out_specs=(vmem, vmem, vmem, vmem),
        scratch_shapes=[
            pltpu.VMEM((4,) + tile, f32), pltpu.VMEM((3,) + tile, f32),
            pltpu.VMEM((4,) + tile, f32), pltpu.VMEM((2,) + tile, f32),
            pltpu.VMEM((planes, rows + 2 * reach, ny), f32), pltpu.VMEM((planes, rows + 2 * reach, ny), f32),
            pltpu.VMEM(tile, f32), pltpu.VMEM(tile, f32), pltpu.VMEM(tile, f32), pltpu.VMEM(tile, f32), pltpu.VMEM(tile, f32),
            dma((4,)), dma((4, 2)), dma((2,)), dma((4,)), dma((4,)), dma((4,)), dma((2,)), dma((2,)), dma((4,)),
            pltpu.VMEM((4 * LANES, 2 * LANES), f32),
        ],
        compiler_params=pltpu.CompilerParams(has_side_effects=True, collective_id=0, vmem_limit_bytes=limit), name="flow",
    )(flow_state, owner)
    sent = pl.pallas_call(
        functools.partial(compact_kernel, n_tile),
        out_shape=shape((n_tile, rows, cap + 2 * LANES), f32),
        in_specs=[smem, smem, vmem, vmem], out_specs=vmem,
        scratch_shapes=[pltpu.VMEM((n_tile, rows, LANES), f32)],
        compiler_params=pltpu.CompilerParams(vmem_limit_bytes=limit), name="compact",
    )(base, count, coeffs, place)
    chunks = 4 if cap % (4 * LANES) == 0 else 1
    record = pl.pallas_call(
        functools.partial(record_kernel, n_tile, chunks),
        out_shape=shape((nx, cap), f32),
        in_specs=[vmem, vmem], out_specs=vmem,
        scratch_shapes=[
            pltpu.VMEM((n_tile, rows, cap), f32), pltpu.VMEM((3, nx, cap), f32),
            dma((n_tile, chunks)), dma((n_tile, chunks)), dma((chunks,)), dma((3, chunks)),
        ],
        compiler_params=pltpu.CompilerParams(has_side_effects=True, collective_id=1, vmem_limit_bytes=limit), name="record",
    )(sent, jnp.asarray(lift_matrix(nx).astype(np.float32)))
    return record[None, None]


CHUNK = 64
SIDE = 16
SPARE = LANES - CHUNK - 2 * SIDE
SUB = 8


def planes_taps(planes):
    first, second = [0.0] * planes, [0.0] * planes
    second[0] = 3.0 * second_center
    for k in range(1, reach + 1):
        first[k % planes] += first_coeffs[k - 1]
        first[-k % planes] -= first_coeffs[k - 1]
        second[k % planes] += second_coeffs[k - 1]
        second[-k % planes] += second_coeffs[k - 1]
    return first, second


def column_taps():
    full = lift_matrix(8 * CHUNK)
    middle = 4 * CHUNK
    low = full[middle // 2, middle - 4 : middle + 5]
    high = full[8 * CHUNK // 2 + middle // 2, middle + 1 - 4 : middle + 1 + 5]
    return [float(x) for x in low], [float(x) for x in high]


def column_band():
    taps_low, taps_high = column_taps()
    part = CHUNK // 2
    row = lax.broadcasted_iota(jnp.int32, (2 * LANES, LANES), 0)
    column = lax.broadcasted_iota(jnp.int32, (2 * LANES, LANES), 1)
    is_low = column < CHUNK
    spot = SIDE + 2 * (column & (part - 1)) + jnp.where(is_low, 0, 1)
    same = (row // LANES) == ((column & (CHUNK - 1)) // part)
    distance = jnp.where(same, (row & (LANES - 1)) - spot, LANES)
    value = jnp.zeros((2 * LANES, LANES), jnp.float32)
    for offset in range(-4, 5):
        tap = jnp.where(is_low, taps_low[offset + 4], taps_high[offset + 4])
        value = jnp.where(distance == offset, tap, value)
    return value


def pencil_slots(pencil, owner, spot_ref, group_ref):
    n_blocks = owner.shape[0]
    upper = (lax.broadcasted_iota(jnp.int32, (LANES, LANES), 0) <= lax.broadcasted_iota(jnp.int32, (LANES, LANES), 1)).astype(jnp.float32)
    lower = (lax.broadcasted_iota(jnp.int32, (n_blocks, n_blocks), 0) > lax.broadcasted_iota(jnp.int32, (n_blocks, n_blocks), 1)).astype(jnp.float32)
    lane = lax.broadcasted_iota(jnp.int32, (n_blocks, LANES), 1)
    mine = owner == pencil
    mask = mine.astype(jnp.float32)
    within = jnp.dot(mask, upper, preferred_element_type=jnp.float32)
    total = jnp.broadcast_to(jnp.sum(mask, axis=1, keepdims=True), (n_blocks, LANES))
    base = jnp.dot(lower, total, preferred_element_type=jnp.float32).astype(jnp.int32)
    slot = base + within.astype(jnp.int32) - 1
    spot_ref[...] = jnp.where(mine, slot & (LANES - 1), -1)
    taken = ((lane - base) & (LANES - 1)) < total.astype(jnp.int32)
    group_ref[...] = jnp.where(taken, base // LANES + jnp.where(lane < (base & (LANES - 1)), 1, 0), -1)


def chunk_kernel(n_tile, own_hbm, owner_hbm, out_ref,
                 own, owner_ref, windows, arrived, fields, mids, slope, final, pieces, landed, spot_ref, group_ref, ordered, band_ref,
                 own_sem, owner_sem, send_sem, recv_sem, recv_two, hand_sem, side_sem, onward_sem, leap_sem):
    g, t = lax.axis_index("grp"), lax.axis_index("tile")
    planes, rows, ny = own.shape
    n_grp = 4
    n_dev = n_grp * n_tile
    nx = rows * n_tile
    half = nx // 2
    me = t * n_grp + g

    load = pltpu.make_async_copy(own_hbm.at[0], own, own_sem)
    load.start()
    load_owner = pltpu.make_async_copy(owner_hbm, owner_ref, owner_sem)
    load_owner.start()
    peers = [(lax.rem(g + k % n_grp, n_grp), lax.rem(t + k // n_grp, n_tile)) for k in range(1, n_dev)]
    barrier = pltpu.get_barrier_semaphore()
    for peer in peers:
        pl.semaphore_signal(barrier, inc=1, device_id=peer, device_id_type=MESH)
    load.wait()
    spread = lax.broadcasted_iota(jnp.int32, (rows, ny), 1) & (LANES - 1)
    for odd in range(2):
        turned = [pltpu.roll(own[z], (SIDE - odd * CHUNK) % ny, 1) for z in range(planes)]
        for z in range(planes - 1):
            moved = pltpu.roll(turned[planes - 1], LANES - SPARE * (z + 1), 1)
            mixed = jnp.where(spread < LANES - SPARE, turned[z], moved)
            for m in range(n_dev // 2):
                windows[2 * m + odd, z * rows : (z + 1) * rows] = mixed[:, m * LANES : (m + 1) * LANES]
    pl.semaphore_wait(barrier, n_dev - 1)

    packed = (planes - 1) * rows

    def deal(peer, source):
        to = peer[1] * n_grp + peer[0]
        return pltpu.make_async_remote_copy(
            src_ref=windows.at[to, pl.ds(0, packed)], dst_ref=arrived.at[source, pl.ds(0, packed)], send_sem=send_sem.at[to], recv_sem=recv_sem.at[source],
            device_id=peer, device_id_type=MESH)

    for peer in peers:
        deal(peer, me).start()
    arrived[me] = windows[me]

    load_owner.wait()
    pencil_slots(t, owner_ref[...], spot_ref, group_ref)
    out_ref[...] = jnp.zeros_like(out_ref)
    band_ref[...] = column_band()

    for peer in peers:
        deal(peer, peer[1] * n_grp + peer[0]).wait_recv()

    sublane = lax.broadcasted_iota(jnp.int32, (reach, SUB, LANES), 1)

    def flip(value):
        return jnp.where((sublane & 1) == 0, pltpu.roll(value, SUB - 1, 1), pltpu.roll(value, 1, 1))

    def wrap(ref, c):
        ref[c, 0:reach] = flip(ref[c, half : half + reach])
        ref[c, half + reach : half + 2 * reach] = flip(ref[c, reach : 2 * reach])

    spot = lax.broadcasted_iota(jnp.int32, (rows, LANES), 1)
    for f in range(n_grp):
        for tile in range(n_tile):
            source = tile * n_grp + f
            last = None
            for z in range(planes - 1):
                piece = pltpu.roll(arrived[source, z * rows : (z + 1) * rows], SPARE * (z + 1), 1)
                last = piece if last is None else jnp.where(spot < SPARE * z, last, piece)
            arrived[source, packed : packed + rows] = last
            side, first = tile // (n_tile // 2), (tile % (n_tile // 2)) * rows
            for r in range(rows):
                fields[f, reach + first + r, pl.ds(side, planes, stride=2), :] = arrived[tile * n_grp + f, pl.ds(r, planes, stride=rows), :]
        wrap(fields, f)

    z_first, z_second = planes_taps(planes)
    step = rows * 2

    def turn_z(value, m):
        return value if m == 0 else pltpu.roll(value, (-2 * m) % SUB, 1)

    def turn_y(value, k):
        return pltpu.roll(value, (-k) % LANES, 2)

    def gradient(i, direction):
        if direction == 0:
            shift = lambda k: fields[3, reach + i + k : reach + i + k + step]
        else:
            center = fields[3, reach + i : reach + i + step]
            if direction == 1:
                shift = lambda k: turn_y(center, k)
            else:
                total = None
                for m in range(1, planes):
                    if z_first[m] != 0.0:
                        term = z_first[m] * turn_z(center, m)
                        total = term if total is None else total + term
                return total
        value, _ = derivatives(None, shift, True, False)
        return value

    def tendency(ref, c, i, speed, press):
        center = ref[c, reach + i : reach + i + step]
        total = z_second[0] * center
        slope_z = None
        for m in range(1, planes):
            turned = turn_z(center, m)
            total = total + z_second[m] * turned
            if z_first[m] != 0.0:
                term = z_first[m] * turned
                slope_z = term if slope_z is None else slope_z + term
        slope_x, slope_y = None, None
        for k in range(1, reach + 1):
            ahead, behind = ref[c, reach + i + k : reach + i + k + step], ref[c, reach + i - k : reach + i - k + step]
            up, down = turn_y(center, k), turn_y(center, -k)
            term_x, term_y = first_coeffs[k - 1] * (ahead - behind), first_coeffs[k - 1] * (up - down)
            slope_x = term_x if slope_x is None else slope_x + term_x
            slope_y = term_y if slope_y is None else slope_y + term_y
            total = total + second_coeffs[k - 1] * ((ahead + behind) + (up + down))
        advect = speed[0] * slope_x + speed[1] * slope_y + speed[2] * slope_z
        return viscosity * total - advect - press, center

    def first_section(b, _):
        i = b * step
        speed = [fields[f, reach + i : reach + i + step] if isinstance(i, int) else fields[f, pl.ds(reach + i, step)] for f in range(3)]
        for c in range(3):
            press = gradient(i, c)
            slope[c, i : i + step] = press
            change, center = tendency(fields, c, i, speed, press)
            mids[c, reach + i : reach + i + step] = center + time_step * change
        return 0

    def second_section(b, c):
        i = b * step
        speed = [mids[f, reach + i : reach + i + step] for f in range(3)]
        change, center = tendency(mids, c, i, speed, slope[c, i : i + step])
        final[c, i : i + step] = 0.5 * ((fields[c, reach + i : reach + i + step] + center) + time_step * change)

    for b in range(half // step):
        first_section(b, 0)
    for c in range(3):
        wrap(mids, c)
    flat = lax.broadcasted_iota(jnp.int32, (SUB, LANES), 0)

    def flip_one(value):
        return jnp.where((flat & 1) == 0, pltpu.roll(value, SUB - 1, 0), pltpu.roll(value, 1, 0))

    matrix = lift_matrix(planes)
    z_coeffs = []
    for m in range(planes):
        column = jnp.zeros((SUB, LANES), jnp.float32)
        for z in range(planes):
            column = jnp.where(flat // 2 == z, float(matrix[z, (z + m) % planes]), column)
        z_coeffs.append(column)

    def lift_z(value):
        total = z_coeffs[0] * value
        for m in range(1, planes):
            total = total + z_coeffs[m] * pltpu.roll(value, (-2 * m) % SUB, 0)
        return total

    pairs = half // 2
    z, y = t // 2, t % 2
    n_z = n_tile // 2

    def flipped(value, bits):
        result, place = 0, 1
        while place < n_z:
            result = result + place * lax.rem(value // place + bits // place, 2)
            place *= 2
        return result

    partner = flipped(z, 1)

    def source_of(level, column, group):
        return (level * 2 + column) * n_grp + group

    def send(origin, source, sem, group, level, column):
        return pltpu.make_async_remote_copy(
            src_ref=origin, dst_ref=landed.at[source], send_sem=sem, recv_sem=recv_two.at[source],
            device_id=(group, level * 2 + column), device_id_type=MESH)

    kin = [g, g + 1 - 2 * lax.rem(g, 2), lax.rem(g + 2, n_grp), n_grp - 1 - g]
    across = (0, 2, 3, 1)
    routes = ((3, 0), (0, 1), (1, 0), (0, 0))

    def hand(bits, other, c):
        return send(pieces.at[c], me, hand_sem.at[bits + 2 * other, c], c, flipped(z, bits), lax.rem(y + other, 2))

    def each_hand(c, act):
        for bits, other in routes:
            if bits or other:
                act(hand(bits, other, c))
            else:
                @pl.when(g != c)
                def _():
                    act(hand(bits, other, c))

    def side(source):
        return send(landed.at[source], source, side_sem.at[source], g, z, 1 - y)

    def onward(source):
        return send(landed.at[source], source, onward_sem.at[source], g, partner, y)

    crossed = (1, 2, 3)

    inner = (z > 0) & (z + 1 < n_z)

    def leap(source):
        return send(landed.at[source], source, leap_sem.at[source], g, flipped(z, 3), y)

    def await_piece(source):
        send(pieces.at[g], source, hand_sem.at[0, 0], g, z, 1 - y).wait_recv()

    def finish(c):
        even = [lift_z(final[c, 2 * i]) for i in range(pairs)]
        odd = [lift_z(final[c, 2 * i + 1]) for i in range(pairs)]
        for odd_tap, even_tap in ((lift_alpha, lift_beta), (lift_gamma, lift_delta)):
            after = even[1:] + [flip_one(even[0])]
            odd = [odd[i] + odd_tap * (even[i] + after[i]) for i in range(pairs)]
            before = [flip_one(odd[-1])] + odd[:-1]
            even = [even[i] + even_tap * (odd[i] + before[i]) for i in range(pairs)]
        for i in range(pairs):
            final[c, i] = even[i] * lift_scale
            final[c, pairs + i] = odd[i] * (1.0 / lift_scale)
        flat_ref = final.at[c].reshape(half * SUB, LANES)
        stacked = []
        for pair in range(2):
            for high in range(2):
                for a in range(2):
                    stacked.append(jnp.concatenate([flat_ref[pl.ds(high * pairs * SUB + 2 * z_at + a, pairs, stride=SUB), :] for z_at in (2 * pair, 2 * pair + 1)], axis=1))
        lines = jnp.dot(jnp.concatenate(stacked, axis=0), band_ref[...], precision=lax.Precision.HIGHEST, preferred_element_type=jnp.float32)
        near, beyond = lines[0:nx], lines[nx : 2 * nx]
        is_near = lax.broadcasted_iota(jnp.int32, (nx, LANES), 1) < CHUNK
        pieces[c, :, 0:LANES] = jnp.where(is_near, near, pltpu.roll(beyond, CHUNK, 1))
        pieces[c, :, LANES : 2 * LANES] = jnp.where(is_near, pltpu.roll(near, CHUNK, 1), beyond)

    for c in (0, 2, 1):
        for b in range(half // step):
            second_section(b, c)
        finish(c)
        each_hand(c, lambda copy: copy.start())
    pieces[3] = pieces[0] * pieces[0] + pieces[1] * pieces[1] + pieces[2] * pieces[2]
    each_hand(3, lambda copy: copy.start())
    rank = lax.broadcasted_iota(jnp.int32, (LANES, LANES), 0)
    n_groups = n_tile
    lane_part = lax.broadcasted_iota(jnp.int32, (nx, LANES), 1) // (CHUNK // 2)

    def select(tile):
        for high in range(2):
            tiles = [landed[tile * n_grp + m, :, high * LANES : (high + 1) * LANES] for m in range(4)]
            for bit in range(2):
                distance = (CHUNK // 2) << bit
                is_low = (lane_part & (1 << bit)) == 0
                turned = list(tiles)
                for m in range(4):
                    if not m & (1 << bit):
                        other = m | (1 << bit)
                        turned[m] = jnp.where(is_low, tiles[m], pltpu.roll(tiles[other], distance, 1))
                        turned[other] = jnp.where(is_low, pltpu.roll(tiles[m], LANES - distance, 1), tiles[other])
                tiles = turned
            for plane in range(planes):
                block = (plane * 2 + high) * n_groups + tile
                value = tiles[plane]
                first = value.astype(jnp.bfloat16).astype(jnp.float32)
                rest = value - first
                second = rest.astype(jnp.bfloat16).astype(jnp.float32)
                stack = jnp.concatenate([first, second, rest - second], axis=0).astype(jnp.bfloat16)
                chosen = jnp.where(rank == spot_ref[pl.ds(block, 1), :], 1.0, 0.0).astype(jnp.bfloat16)
                placed = lax.dot_general(stack, chosen, (((1,), (1,)), ((), ())), preferred_element_type=jnp.float32)
                ordered[plane * 2 + high] = (placed[0:nx] + placed[nx : 2 * nx]) + placed[2 * nx : 3 * nx]
        labels = [group_ref[pl.ds((plane * 2 + high) * n_groups + tile, 1), :] for plane in range(planes) for high in range(2)]
        for q in range(out_ref.shape[1] // LANES):
            total = out_ref[:, q * LANES : (q + 1) * LANES]
            for n, label in enumerate(labels):
                total = jnp.where(label == q, ordered[n], total)
            out_ref[:, q * LANES : (q + 1) * LANES] = total

    landed[me] = pieces[g]

    def sideways(bits, k):
        return bits == 3 or bits == 2 or (bits == 1 and k not in crossed)

    def receive(bits):
        for k in across:
            source = source_of(flipped(z, bits), y, kin[k])
            if bits or k:
                await_piece(source)
            if bits == 3 or bits == 1:
                @pl.when(inner)
                def _():
                    (onward if bits == 3 else leap)(source).start()
            if sideways(bits, k):
                side(source).start()
        if bits == 0:
            for k in across:
                source = source_of(z, 1 - y, kin[k])
                await_piece(source)
                if k in crossed:
                    onward(source).start()

    for peer in peers:
        deal(peer, me).wait_send()

    for bits in (1, 3, 0):
        receive(bits)

    def from_other(bits):
        for k in across:
            await_piece(source_of(flipped(z, bits), 1 - y, kin[k]))

    def pick(bits, other):
        select(flipped(z, bits) * 2 + lax.rem(y + other, 2))

    pick(0, 0)
    receive(2)
    pick(0, 1)
    pick(1, 0)
    pick(3, 0)
    pick(2, 0)
    for bits in (3, 1):
        from_other(bits)
        pick(bits, 1)
    for c in range(n_grp):
        each_hand(c, lambda copy: copy.wait_send())
    for k in across:
        for bits in range(1, n_z):
            source = source_of(flipped(z, bits), y, kin[k])
            if sideways(bits, k):
                side(source).wait_send()
        @pl.when(inner)
        def _():
            onward(source_of(flipped(z, 3), y, kin[k])).wait_send()
            leap(source_of(partner, y, kin[k])).wait_send()

        if k in crossed:
            onward(source_of(z, 1 - y, kin[k])).wait_send()
    from_other(2)
    pick(2, 1)


def chunk_body(flow_state, line_owner, *, n_tile):
    _, planes, rows, ny = flow_state.shape
    n_lines = line_owner.shape[0]
    n_blocks = n_lines // LANES
    nx = rows * n_tile
    half = nx // 2
    n_dev = 4 * n_tile
    cap = 2 * planes * ny // n_tile
    f32 = jnp.float32
    dma = pltpu.SemaphoreType.DMA
    hbm = pl.BlockSpec(memory_space=pltpu.HBM)
    padded = (half + 2 * reach, SUB, LANES)
    record = pl.pallas_call(
        functools.partial(chunk_kernel, n_tile),
        out_shape=jax.ShapeDtypeStruct((nx, cap), f32),
        in_specs=[hbm, hbm], out_specs=pl.BlockSpec(memory_space=pltpu.VMEM),
        scratch_shapes=[
            pltpu.VMEM((planes, rows, ny), f32), pltpu.VMEM((n_blocks, LANES), jnp.int32),
            pltpu.VMEM((n_dev, planes * rows, LANES), f32), pltpu.VMEM((n_dev, planes * rows, LANES), f32),
            pltpu.VMEM((4,) + padded, f32), pltpu.VMEM((3,) + padded, f32),
            pltpu.VMEM((3, half, SUB, LANES), f32), pltpu.VMEM((3, half, SUB, LANES), f32),
            pltpu.VMEM((4, nx, 2 * LANES), f32), pltpu.VMEM((n_dev, nx, 2 * LANES), f32),
            pltpu.VMEM((n_blocks, LANES), jnp.int32), pltpu.VMEM((n_blocks, LANES), jnp.int32),
            pltpu.VMEM((2 * planes, nx, LANES), f32), pltpu.VMEM((2 * LANES, LANES), f32),
            dma, dma, dma((n_dev,)), dma((n_dev,)), dma((n_dev,)), dma((4, 4)), dma((n_dev,)), dma((n_dev,)), dma((n_dev,)),
        ],
        compiler_params=pltpu.CompilerParams(has_side_effects=True, collective_id=0, vmem_limit_bytes=16 * 1024 * 1024), name="record",
    )(pltpu.with_memory_space_constraint(flow_state, pltpu.HBM), pltpu.with_memory_space_constraint(line_owner.reshape(n_blocks, LANES), pltpu.HBM))
    return record[None, None]


def fits_chunks(mesh, planes, rows, ny):
    n_tile = mesh.shape["tile"]
    return 2 * planes == SUB and 2 * rows == SUB and mesh.shape["grp"] == 4 and ny == 4 * n_tile * CHUNK and n_tile == 8


def solution(mesh):
    in_specs = (P("grp", None, "tile", None), P())
    out_specs = P("grp", "tile", None, None)
    n_tile = mesh.shape["tile"]

    def run(flow_state, line_owner):
        _, planes, rows, ny = flow_state.shape
        chosen = chunk_body if fits_chunks(mesh, planes, rows, ny) else tiled_body
        return chosen(flow_state, line_owner, n_tile=n_tile)

    return jax.shard_map(run, mesh=mesh, in_specs=in_specs, out_specs=out_specs, check_vma=False)
```

```python
import functools

import jax
import jax.numpy as jnp
import numpy as np
from jax import lax
from jax.experimental import pallas as pl
from jax.experimental.pallas import tpu as pltpu
from jax.sharding import PartitionSpec as P

time_step = 0.2
viscosity = 0.05
reach = 4
first_coeffs = (0.8, -0.2, 4.0 / 105.0, -1.0 / 280.0)
second_center = -205.0 / 72.0
second_coeffs = (1.6, -0.2, 8.0 / 315.0, -1.0 / 560.0)
lift_alpha = -1.586134342059924
lift_beta = -0.052980118572961
lift_gamma = 0.882911075530934
lift_delta = 0.443506852043971
lift_scale = 1.149604398860241
LANES = 128
MESH = pl.DeviceIdType.MESH


def lift_numpy(signal):
    even, odd = signal[0::2].copy(), signal[1::2].copy()
    odd += lift_alpha * (even + np.roll(even, -1, 0))
    even += lift_beta * (odd + np.roll(odd, 1, 0))
    odd += lift_gamma * (even + np.roll(even, -1, 0))
    even += lift_delta * (odd + np.roll(odd, 1, 0))
    return np.concatenate([even * lift_scale, odd / lift_scale])


def lift_matrix(length):
    return lift_numpy(np.eye(length))


def band_matrix():
    full = lift_matrix(8 * LANES)
    low = full[LANES : 2 * LANES, LANES : 5 * LANES]
    high = full[4 * LANES + LANES : 4 * LANES + 2 * LANES, LANES : 5 * LANES]
    return np.concatenate([low, high]).T.astype(np.float32)


def band_value(taps_low, taps_high):
    row = lax.broadcasted_iota(jnp.int32, (4 * LANES, 2 * LANES), 0)
    column = lax.broadcasted_iota(jnp.int32, (4 * LANES, 2 * LANES), 1)
    distance = row - LANES - 2 * (column & (LANES - 1))
    is_low = column < LANES
    value = jnp.zeros((4 * LANES, 2 * LANES), jnp.float32)
    for offset in range(-4, 5):
        tap = jnp.where(is_low, taps_low[offset + 4], taps_high[offset + 4])
        value = jnp.where(distance == offset, tap, value)
    return value


def band_taps():
    band = band_matrix()
    rows = slice(LANES + LANES // 2 - 4, LANES + LANES // 2 + 5)
    return [float(x) for x in band[rows, LANES // 4]], [float(x) for x in band[rows, LANES + LANES // 4]]


def shifted_y(value, k):
    return pltpu.roll(value, (-k) % value.shape[-1], value.ndim - 1)


def derivatives(center, shift, want_first=True, want_second=True):
    first, second = None, second_center * center if want_second else None
    for k in range(1, reach + 1):
        ahead, behind = shift(k), shift(-k)
        if want_first:
            term = first_coeffs[k - 1] * (ahead - behind)
            first = term if first is None else first + term
        if want_second:
            second = second + second_coeffs[k - 1] * (ahead + behind)
    return first, second


def slots_of(n_tile, owner_ref, place_ref, base_ref, count_ref):
    owner = owner_ref[...]
    n_blocks = owner.shape[0]
    upper = (lax.broadcasted_iota(jnp.int32, (LANES, LANES), 0) <= lax.broadcasted_iota(jnp.int32, (LANES, LANES), 1)).astype(jnp.float32)
    lower = (lax.broadcasted_iota(jnp.int32, (n_blocks, n_blocks), 0) > lax.broadcasted_iota(jnp.int32, (n_blocks, n_blocks), 1)).astype(jnp.float32)
    lane = lax.broadcasted_iota(jnp.int32, (n_blocks, LANES), 1)

    def step(s, carry):
        place, counts, ahead = carry
        mask = (owner == s).astype(jnp.float32)
        within = jnp.dot(mask, upper, preferred_element_type=jnp.float32)
        total = jnp.sum(mask, axis=1, keepdims=True)
        place = place + mask * (ahead + within - 1.0)
        counts = jnp.where(lane == s, total, counts)
        return place, counts, ahead + total

    zeros = jnp.zeros((n_blocks, LANES), jnp.float32)
    carry = (zeros, zeros, jnp.zeros((n_blocks, 1), jnp.float32))
    if n_tile <= 16:
        for s in range(n_tile):
            carry = step(s, carry)
    else:
        carry = lax.fori_loop(0, n_tile, step, carry)
    place, counts, _ = carry
    place_ref[...] = place
    count_ref[...] = counts.astype(jnp.int32)
    base_ref[...] = jnp.dot(lower, counts, preferred_element_type=jnp.float32).astype(jnp.int32)


def flow_kernel(n_tile, own_ref, owner_ref, out_ref, place_ref, base_ref, count_ref,
                fields, mids, halo, mid_halo, pad, ppad, middle, fin, along_y, along_z, lap, send_sem, recv_sem, hsend_sem, hrecv_sem, msend_sem, mrecv_sem, mhsend_sem, mhrecv_sem, relay_sem, band_ref):
    g, t = lax.axis_index("grp"), lax.axis_index("tile")
    right, left = lax.rem(t + 1, n_tile), lax.rem(t + n_tile - 1, n_tile)
    planes, rows, ny = own_ref.shape[1:]
    own = own_ref.at[0]

    barrier = pltpu.get_barrier_semaphore()
    for k in range(1, 4):
        pl.semaphore_signal(barrier, inc=1, device_id=(lax.rem(g + k, 4), t), device_id_type=MESH)
    for side in (right, left):
        pl.semaphore_signal(barrier, inc=1, device_id=(g, side), device_id_type=MESH)

    @pl.when((g == 0) | (g == 3))
    def _():
        for side in (right, left):
            pl.semaphore_signal(barrier, inc=1, device_id=(3 - g, side), device_id_type=MESH)
        pl.semaphore_wait(barrier, 7)

    @pl.when((g == 1) | (g == 2))
    def _():
        pl.semaphore_wait(barrier, 5)

    def gather_copy(src, dst, ssem, rsem, k, slot):
        return pltpu.make_async_remote_copy(
            src_ref=src, dst_ref=dst.at[slot], send_sem=ssem.at[k], recv_sem=rsem.at[slot],
            device_id=(k, t), device_id_type=MESH)

    half = planes // 2

    def whole_copy(k, slot):
        return pltpu.make_async_remote_copy(
            src_ref=own, dst_ref=fields.at[slot], send_sem=send_sem.at[k], recv_sem=recv_sem.at[slot, 0],
            device_id=(k, t), device_id_type=MESH)

    def half_copy(slot, k):
        part = pl.ds(k * half, half)
        return pltpu.make_async_remote_copy(
            src_ref=own.at[part], dst_ref=fields.at[slot, part], send_sem=send_sem.at[k],
            recv_sem=recv_sem.at[slot, k], device_id=(k, t), device_id_type=MESH)

    def relay_copy(slot, k):
        part = pl.ds(k * half, half)
        return pltpu.make_async_remote_copy(
            src_ref=fields.at[slot, part], dst_ref=fields.at[slot, part], send_sem=relay_sem.at[slot],
            recv_sem=recv_sem.at[slot, k], device_id=(1 - k, t), device_id_type=MESH)

    def halo_copy(src, dst, ssem, rsem, side, slot, group):
        return pltpu.make_async_remote_copy(
            src_ref=src, dst_ref=dst.at[slot + side], send_sem=ssem.at[side], recv_sem=rsem.at[slot + side],
            device_id=(group, right if side == 0 else left), device_id_type=MESH)

    @pl.when(g < 3)
    def _():
        for side in range(2):
            halo_copy(own, halo, hsend_sem, hrecv_sem, side, 0, g).start()

    for k in range(3):
        @pl.when((g < 2) & (g != k))
        def _(k=k):
            whole_copy(k, g).start()

    @pl.when(g >= 2)
    def _():
        for k in range(2):
            half_copy(g, k).start()

    @pl.when(g == 3)
    def _():
        whole_copy(2, 3).start()
        for side in range(2):
            halo_copy(own, halo, hsend_sem, hrecv_sem, side, 2, 0).start()

    def local_terms():
        for z in range(planes):
            center = pad[z, reach : reach + rows]
            fy, sy = derivatives(center, lambda k: shifted_y(center, k))
            fz, sz = derivatives(center, lambda k: pad[(z + k) % planes, reach : reach + rows])
            along_y[z], along_z[z], lap[z] = fy, fz, sy + sz

    slots_of(n_tile, owner_ref, place_ref, base_ref, count_ref)
    band_ref[...] = band_value(*band_taps())

    @pl.when(g < 3)
    def _():
        for k in range(3):
            @pl.when(g == k)
            def _(k=k):
                fields[k] = own_ref[0]

        for z in range(planes):
            pad[z, reach : reach + rows] = own_ref[0, z]
        local_terms()

        @pl.when(g < 2)
        def _():
            for slot in (2, 3):
                half_copy(slot, g).wait_recv()
                relay_copy(slot, g).start()
            whole_copy(0, 1 - g).wait_recv()
            for slot in (2, 3):
                half_copy(slot, 1 - g).wait_recv()

        @pl.when(g == 2)
        def _():
            for slot in (0, 1, 3):
                whole_copy(0, slot).wait_recv()

        for side in range(2):
            halo_copy(own, halo, hsend_sem, hrecv_sem, side, 0, g).wait_recv()

        @pl.when(g == 0)
        def _():
            for side in range(2):
                halo_copy(own, halo, hsend_sem, hrecv_sem, side, 2, 0).wait_recv()
            for z in range(planes):
                ppad[z, 0:reach] = halo[2, z, rows - reach : rows]
                ppad[z, reach : reach + rows] = fields[3, z]
                ppad[z, reach + rows : 2 * reach + rows] = halo[3, z, 0:reach]
            for z in range(planes):
                middle[z], _ = derivatives(None, lambda k: ppad[z, reach + k : reach + k + rows], True, False)

        @pl.when(g == 1)
        def _():
            for z in range(planes):
                value = fields[3, z]
                middle[z], _ = derivatives(None, lambda k: shifted_y(value, k), True, False)

        @pl.when(g == 2)
        def _():
            for z in range(planes):
                middle[z], _ = derivatives(None, lambda k: fields[3, (z + k) % planes], True, False)

        def tendency(z, vel, press):
            center = pad[z, reach : reach + rows]
            fx, sx = derivatives(center, lambda k: pad[z, reach + k : reach + k + rows])
            advect = vel[0, z] * fx + vel[1, z] * along_y[z] + vel[2, z] * along_z[z]
            return viscosity * (sx + lap[z]) - advect - press

        for z in range(planes):
            pad[z, 0:reach] = halo[0, z, rows - reach : rows]
            pad[z, reach + rows : 2 * reach + rows] = halo[1, z, 0:reach]
        for z in range(planes):
            press = middle[z]
            ppad[z, 0:rows] = press
        for z in range(planes):
            middle[z] = own_ref[0, z] + time_step * tendency(z, fields, ppad[z, 0:rows])

        for side in range(2):
            halo_copy(middle, mid_halo, mhsend_sem, mhrecv_sem, side, 0, g).start()
        for k in range(3):
            @pl.when(g != k)
            def _(k=k):
                gather_copy(middle, mids, msend_sem, mrecv_sem, k, g).start()

            @pl.when(g == k)
            def _(k=k):
                mids[k] = middle[...]

        for z in range(planes):
            pad[z, reach : reach + rows] = middle[z]
        local_terms()
        for k in range(3):
            @pl.when(g != k)
            def _(k=k):
                gather_copy(middle, mids, msend_sem, mrecv_sem, 0, k).wait_recv()
        for side in range(2):
            halo_copy(middle, mid_halo, mhsend_sem, mhrecv_sem, side, 0, g).wait_recv()
        for z in range(planes):
            pad[z, 0:reach] = mid_halo[0, z, rows - reach : rows]
            pad[z, reach + rows : 2 * reach + rows] = mid_halo[1, z, 0:reach]
        for z in range(planes):
            fin[z] = 0.5 * ((own_ref[0, z] + middle[z]) + time_step * tendency(z, mids, ppad[z, 0:rows]))

        blocks = ny // (2 * LANES)
        groups = ny // LANES
        for z in range(planes):
            value = fin[z]
            pieces = []
            for b in range(blocks):
                window = [value[:, ((2 * b + j) % groups) * LANES : ((2 * b + j) % groups + 1) * LANES] for j in (-1, 0, 1, 2)]
                pieces.append(jnp.concatenate(window, axis=1))
            stacked = jnp.concatenate(pieces, axis=0)
            lifted = jnp.dot(stacked, band_ref[...], precision=lax.Precision.HIGHEST, preferred_element_type=jnp.float32)
            for b in range(blocks):
                piece = lifted[b * rows : (b + 1) * rows]
                fin[z, :, b * LANES : (b + 1) * LANES] = piece[:, 0:LANES]
                fin[z, :, ny // 2 + b * LANES : ny // 2 + (b + 1) * LANES] = piece[:, LANES:]

        even = [fin[2 * i] for i in range(half)]
        odd = [fin[2 * i + 1] for i in range(half)]
        odd = [odd[i] + lift_alpha * (even[i] + even[(i + 1) % half]) for i in range(half)]
        even = [even[i] + lift_beta * (odd[i] + odd[(i - 1) % half]) for i in range(half)]
        odd = [odd[i] + lift_gamma * (even[i] + even[(i + 1) % half]) for i in range(half)]
        even = [even[i] + lift_delta * (odd[i] + odd[(i - 1) % half]) for i in range(half)]
        for i in range(half):
            out_ref[i] = even[i] * lift_scale
            out_ref[half + i] = odd[i] * (1.0 / lift_scale)

        for side in range(2):
            halo_copy(middle, mid_halo, mhsend_sem, mhrecv_sem, side, 0, g).wait_send()
        for k in range(3):
            @pl.when(g != k)
            def _(k=k):
                gather_copy(middle, mids, msend_sem, mrecv_sem, k, g).wait_send()

    @pl.when(g == 3)
    def _():
        out_ref[...] = jnp.zeros_like(out_ref)

    for side in range(2):
        halo_copy(own, halo, hsend_sem, hrecv_sem, side, 0, g).wait_send()
    for k in range(3):
        @pl.when((g < 2) & (g != k))
        def _(k=k):
            whole_copy(k, g).wait_send()

    @pl.when(g < 2)
    def _():
        for slot in (2, 3):
            relay_copy(slot, g).wait_send()

    @pl.when(g >= 2)
    def _():
        for k in range(2):
            half_copy(g, k).wait_send()

    @pl.when(g == 3)
    def _():
        whole_copy(2, 3).wait_send()


def compact_kernel(n_tile, base_ref, count_ref, coeff_ref, place_ref, out_ref, current):
    planes, rows, ny = coeff_ref.shape
    groups = ny // LANES
    out_ref[...] = jnp.zeros_like(out_ref)
    current[...] = jnp.zeros_like(current)
    rank = lax.broadcasted_iota(jnp.int32, (LANES, LANES), 0).astype(jnp.float32)
    lane = lax.broadcasted_iota(jnp.int32, (rows, LANES), 1)

    def sort(b):
        z, y = b // groups, b % groups
        value = coeff_ref[z, :, pl.ds(pl.multiple_of(y * LANES, LANES), LANES)]
        high = value.astype(jnp.bfloat16).astype(jnp.float32)
        rest = value - high
        mid = rest.astype(jnp.bfloat16).astype(jnp.float32)
        low = rest - mid
        parts = jnp.concatenate([high, mid, low], axis=0).astype(jnp.bfloat16)
        chosen = jnp.where(rank == place_ref[pl.ds(b, 1), :], 1.0, 0.0).astype(jnp.bfloat16)
        ordered = lax.dot_general(parts, chosen, (((1,), (1,)), ((), ())), preferred_element_type=jnp.float32)
        return (ordered[0:rows] + ordered[rows : 2 * rows]) + ordered[2 * rows : 3 * rows]

    def pencil(b, ordered, s, ahead):
        base, count = base_ref[b, s], count_ref[b, s]
        start = base & (LANES - 1)
        end = start + count
        turned = pltpu.roll(ordered, (start - ahead) & (LANES - 1), 1)
        now = current[s] + jnp.where((lane >= start) & (lane < end), turned, 0.0)
        group = pl.multiple_of(base - start, LANES)
        after = jnp.where(lane < end - LANES, turned, 0.0)
        current[s] = jnp.where(end >= LANES, after, now)
        out_ref[s, :, pl.ds(group, 2 * LANES)] = jnp.concatenate([now, after], axis=1)
        return ahead + count

    n_blocks = planes * groups
    batch = 8 if n_blocks % 8 == 0 and n_tile <= 16 else 1

    def blocks(i, _):
        ordered = [sort(i * batch + j) for j in range(batch)]
        for j in range(batch):
            b = i * batch + j
            if n_tile <= 16:
                ahead = jnp.int32(0)
                for s in range(n_tile):
                    ahead = pencil(b, ordered[j], s, ahead)
            else:
                lax.fori_loop(0, n_tile, lambda s, ahead: pencil(b, ordered[j], s, ahead), jnp.int32(0))
        return 0

    lax.fori_loop(0, n_blocks // batch, blocks, 0)


def record_kernel(n_tile, chunks, sent_ref, matrix_ref, out_ref, got, records, send_sem, recv_sem, rsend_sem, rrecv_sem):
    g, t = lax.axis_index("grp"), lax.axis_index("tile")
    rows, nx, cap = sent_ref.shape[1], out_ref.shape[0], out_ref.shape[1]
    width = cap // chunks

    barrier = pltpu.get_barrier_semaphore()

    @pl.when(g < 3)
    def _():
        for k in range(1, n_tile):
            pl.semaphore_signal(barrier, inc=1, device_id=(g, lax.rem(t + k, n_tile)), device_id_type=MESH)
        pl.semaphore_signal(barrier, inc=1, device_id=(3, t), device_id_type=MESH)
        pl.semaphore_wait(barrier, n_tile)

    @pl.when(g == 3)
    def _():
        for k in range(3):
            pl.semaphore_signal(barrier, inc=1, device_id=(k, t), device_id_type=MESH)
        pl.semaphore_wait(barrier, 3)

    def exchange(s, slot, c):
        part = pl.ds(c * width, width)
        return pltpu.make_async_remote_copy(
            src_ref=sent_ref.at[s, :, part], dst_ref=got.at[slot, :, part], send_sem=send_sem.at[s, c],
            recv_sem=recv_sem.at[slot, c], device_id=(g, s), device_id_type=MESH)

    def report(c, slot):
        part = pl.ds(c * width, width)
        return pltpu.make_async_remote_copy(
            src_ref=out_ref.at[:, part], dst_ref=records.at[slot, :, part], send_sem=rsend_sem.at[c],
            recv_sem=rrecv_sem.at[slot, c], device_id=(3, t), device_id_type=MESH)

    @pl.when(g < 3)
    def _():
        for c in range(chunks):
            for k in range(1, n_tile):
                exchange(lax.rem(t + k, n_tile), t, c).start()
        got[t] = sent_ref[t, :, 0:cap]
        matrix = matrix_ref[...]
        for c in range(chunks):
            for k in range(1, n_tile):
                exchange(lax.rem(t + k, n_tile), lax.rem(t + k, n_tile), c).wait_recv()
            value = got[:, :, c * width : (c + 1) * width].reshape(nx, width)
            out_ref[:, c * width : (c + 1) * width] = jnp.dot(
                matrix, value, precision=lax.Precision.HIGHEST, preferred_element_type=jnp.float32)
            report(c, g).start()
        for c in range(chunks):
            for k in range(1, n_tile):
                exchange(lax.rem(t + k, n_tile), t, c).wait_send()
            report(c, g).wait_send()

    @pl.when(g == 3)
    def _():
        for c in range(chunks):
            for k in range(3):
                report(c, k).wait_recv()
            part = slice(c * width, (c + 1) * width)
            first, second, third = records[0, :, part], records[1, :, part], records[2, :, part]
            out_ref[:, part] = first * first + second * second + third * third


def tiled_body(flow_state, line_owner, *, n_tile):
    _, planes, rows, ny = flow_state.shape
    n_lines = line_owner.shape[0]
    n_blocks = n_lines // LANES
    nx = rows * n_tile
    cap = 2 * planes * ny // n_tile
    vmem = pl.BlockSpec(memory_space=pltpu.VMEM)
    smem = pl.BlockSpec(memory_space=pltpu.SMEM)
    f32 = jnp.float32
    shape = jax.ShapeDtypeStruct
    limit = 16 * 1024 * 1024
    dma = pltpu.SemaphoreType.DMA
    owner = line_owner.reshape(n_blocks, LANES)
    tile = (planes, rows, ny)
    ints = shape((n_blocks, LANES), jnp.int32)
    coeffs, place, base, count = pl.pallas_call(
        functools.partial(flow_kernel, n_tile),
        out_shape=(shape(tile, f32), shape((n_blocks, LANES), f32), ints, ints),
        in_specs=[vmem, vmem], out_specs=(vmem, vmem, vmem, vmem),
        scratch_shapes=[
            pltpu.VMEM((4,) + tile, f32), pltpu.VMEM((3,) + tile, f32),
            pltpu.VMEM((4,) + tile, f32), pltpu.VMEM((2,) + tile, f32),
            pltpu.VMEM((planes, rows + 2 * reach, ny), f32), pltpu.VMEM((planes, rows + 2 * reach, ny), f32),
            pltpu.VMEM(tile, f32), pltpu.VMEM(tile, f32), pltpu.VMEM(tile, f32), pltpu.VMEM(tile, f32), pltpu.VMEM(tile, f32),
            dma((4,)), dma((4, 2)), dma((2,)), dma((4,)), dma((4,)), dma((4,)), dma((2,)), dma((2,)), dma((4,)),
            pltpu.VMEM((4 * LANES, 2 * LANES), f32),
        ],
        compiler_params=pltpu.CompilerParams(has_side_effects=True, collective_id=0, vmem_limit_bytes=limit), name="flow",
    )(flow_state, owner)
    sent = pl.pallas_call(
        functools.partial(compact_kernel, n_tile),
        out_shape=shape((n_tile, rows, cap + 2 * LANES), f32),
        in_specs=[smem, smem, vmem, vmem], out_specs=vmem,
        scratch_shapes=[pltpu.VMEM((n_tile, rows, LANES), f32)],
        compiler_params=pltpu.CompilerParams(vmem_limit_bytes=limit), name="compact",
    )(base, count, coeffs, place)
    chunks = 4 if cap % (4 * LANES) == 0 else 1
    record = pl.pallas_call(
        functools.partial(record_kernel, n_tile, chunks),
        out_shape=shape((nx, cap), f32),
        in_specs=[vmem, vmem], out_specs=vmem,
        scratch_shapes=[
            pltpu.VMEM((n_tile, rows, cap), f32), pltpu.VMEM((3, nx, cap), f32),
            dma((n_tile, chunks)), dma((n_tile, chunks)), dma((chunks,)), dma((3, chunks)),
        ],
        compiler_params=pltpu.CompilerParams(has_side_effects=True, collective_id=1, vmem_limit_bytes=limit), name="record",
    )(sent, jnp.asarray(lift_matrix(nx).astype(np.float32)))
    return record[None, None]


CHUNK = 64
SIDE = 16
SPARE = LANES - CHUNK - 2 * SIDE
SUB = 8


def planes_taps(planes):
    first, second = [0.0] * planes, [0.0] * planes
    second[0] = 3.0 * second_center
    for k in range(1, reach + 1):
        first[k % planes] += first_coeffs[k - 1]
        first[-k % planes] -= first_coeffs[k - 1]
        second[k % planes] += second_coeffs[k - 1]
        second[-k % planes] += second_coeffs[k - 1]
    return first, second


def column_taps():
    full = lift_matrix(8 * CHUNK)
    middle = 4 * CHUNK
    low = full[middle // 2, middle - 4 : middle + 5]
    high = full[8 * CHUNK // 2 + middle // 2, middle + 1 - 4 : middle + 1 + 5]
    return [float(x) for x in low], [float(x) for x in high]


def column_band():
    taps_low, taps_high = column_taps()
    part = CHUNK // 2
    row = lax.broadcasted_iota(jnp.int32, (2 * LANES, LANES), 0)
    column = lax.broadcasted_iota(jnp.int32, (2 * LANES, LANES), 1)
    is_low = column < CHUNK
    spot = SIDE + 2 * (column & (part - 1)) + jnp.where(is_low, 0, 1)
    same = (row // LANES) == ((column & (CHUNK - 1)) // part)
    distance = jnp.where(same, (row & (LANES - 1)) - spot, LANES)
    value = jnp.zeros((2 * LANES, LANES), jnp.float32)
    for offset in range(-4, 5):
        tap = jnp.where(is_low, taps_low[offset + 4], taps_high[offset + 4])
        value = jnp.where(distance == offset, tap, value)
    return value


def pencil_slots(pencil, owner, spot_ref, group_ref):
    n_blocks = owner.shape[0]
    upper = (lax.broadcasted_iota(jnp.int32, (LANES, LANES), 0) <= lax.broadcasted_iota(jnp.int32, (LANES, LANES), 1)).astype(jnp.float32)
    lower = (lax.broadcasted_iota(jnp.int32, (n_blocks, n_blocks), 0) > lax.broadcasted_iota(jnp.int32, (n_blocks, n_blocks), 1)).astype(jnp.float32)
    lane = lax.broadcasted_iota(jnp.int32, (n_blocks, LANES), 1)
    mine = owner == pencil
    mask = mine.astype(jnp.float32)
    within = jnp.dot(mask, upper, preferred_element_type=jnp.float32)
    total = jnp.broadcast_to(jnp.sum(mask, axis=1, keepdims=True), (n_blocks, LANES))
    base = jnp.dot(lower, total, preferred_element_type=jnp.float32).astype(jnp.int32)
    slot = base + within.astype(jnp.int32) - 1
    spot_ref[...] = jnp.where(mine, slot & (LANES - 1), -1)
    taken = ((lane - base) & (LANES - 1)) < total.astype(jnp.int32)
    group_ref[...] = jnp.where(taken, base // LANES + jnp.where(lane < (base & (LANES - 1)), 1, 0), -1)


def chunk_kernel(n_tile, own_hbm, owner_hbm, out_ref,
                 own, owner_ref, windows, arrived, fields, mids, slope, final, pieces, landed, spot_ref, group_ref, ordered, band_ref,
                 own_sem, owner_sem, send_sem, recv_sem, recv_two, hand_sem, side_sem, onward_sem, leap_sem):
    g, t = lax.axis_index("grp"), lax.axis_index("tile")
    planes, rows, ny = own.shape
    n_grp = 4
    n_dev = n_grp * n_tile
    nx = rows * n_tile
    half = nx // 2
    me = t * n_grp + g

    load = pltpu.make_async_copy(own_hbm.at[0], own, own_sem)
    load.start()
    load_owner = pltpu.make_async_copy(owner_hbm, owner_ref, owner_sem)
    load_owner.start()
    peers = [(lax.rem(g + k % n_grp, n_grp), lax.rem(t + k // n_grp, n_tile)) for k in range(1, n_dev)]
    barrier = pltpu.get_barrier_semaphore()
    for peer in peers:
        pl.semaphore_signal(barrier, inc=1, device_id=peer, device_id_type=MESH)
    load.wait()
    spread = lax.broadcasted_iota(jnp.int32, (rows, ny), 1) & (LANES - 1)
    for odd in range(2):
        turned = [pltpu.roll(own[z], (SIDE - odd * CHUNK) % ny, 1) for z in range(planes)]
        for z in range(planes - 1):
            moved = pltpu.roll(turned[planes - 1], LANES - SPARE * (z + 1), 1)
            mixed = jnp.where(spread < LANES - SPARE, turned[z], moved)
            for m in range(n_dev // 2):
                windows[2 * m + odd, z * rows : (z + 1) * rows] = mixed[:, m * LANES : (m + 1) * LANES]
    pl.semaphore_wait(barrier, n_dev - 1)

    packed = (planes - 1) * rows

    def deal(peer, source):
        to = peer[1] * n_grp + peer[0]
        return pltpu.make_async_remote_copy(
            src_ref=windows.at[to, pl.ds(0, packed)], dst_ref=arrived.at[source, pl.ds(0, packed)], send_sem=send_sem.at[to], recv_sem=recv_sem.at[source],
            device_id=peer, device_id_type=MESH)

    for peer in peers:
        deal(peer, me).start()
    arrived[me] = windows[me]

    load_owner.wait()
    pencil_slots(t, owner_ref[...], spot_ref, group_ref)
    out_ref[...] = jnp.zeros_like(out_ref)
    band_ref[...] = column_band()

    for peer in peers:
        deal(peer, peer[1] * n_grp + peer[0]).wait_recv()

    sublane = lax.broadcasted_iota(jnp.int32, (reach, SUB, LANES), 1)

    def flip(value):
        return jnp.where((sublane & 1) == 0, pltpu.roll(value, SUB - 1, 1), pltpu.roll(value, 1, 1))

    def wrap(ref, c):
        ref[c, 0:reach] = flip(ref[c, half : half + reach])
        ref[c, half + reach : half + 2 * reach] = flip(ref[c, reach : 2 * reach])

    spot = lax.broadcasted_iota(jnp.int32, (rows, LANES), 1)
    for f in range(n_grp):
        for tile in range(n_tile):
            source = tile * n_grp + f
            last = None
            for z in range(planes - 1):
                piece = pltpu.roll(arrived[source, z * rows : (z + 1) * rows], SPARE * (z + 1), 1)
                last = piece if last is None else jnp.where(spot < SPARE * z, last, piece)
            arrived[source, packed : packed + rows] = last
            side, first = tile // (n_tile // 2), (tile % (n_tile // 2)) * rows
            for r in range(rows):
                fields[f, reach + first + r, pl.ds(side, planes, stride=2), :] = arrived[tile * n_grp + f, pl.ds(r, planes, stride=rows), :]
        wrap(fields, f)

    z_first, z_second = planes_taps(planes)
    step = rows * 2

    def turn_z(value, m):
        return value if m == 0 else pltpu.roll(value, (-2 * m) % SUB, 1)

    def turn_y(value, k):
        return pltpu.roll(value, (-k) % LANES, 2)

    def gradient(i, direction):
        if direction == 0:
            shift = lambda k: fields[3, reach + i + k : reach + i + k + step]
        else:
            center = fields[3, reach + i : reach + i + step]
            if direction == 1:
                shift = lambda k: turn_y(center, k)
            else:
                total = None
                for m in range(1, planes):
                    if z_first[m] != 0.0:
                        term = z_first[m] * turn_z(center, m)
                        total = term if total is None else total + term
                return total
        value, _ = derivatives(None, shift, True, False)
        return value

    def tendency(ref, c, i, speed, press):
        center = ref[c, reach + i : reach + i + step]
        total = z_second[0] * center
        slope_z = None
        for m in range(1, planes):
            turned = turn_z(center, m)
            total = total + z_second[m] * turned
            if z_first[m] != 0.0:
                term = z_first[m] * turned
                slope_z = term if slope_z is None else slope_z + term
        slope_x, slope_y = None, None
        for k in range(1, reach + 1):
            ahead, behind = ref[c, reach + i + k : reach + i + k + step], ref[c, reach + i - k : reach + i - k + step]
            up, down = turn_y(center, k), turn_y(center, -k)
            term_x, term_y = first_coeffs[k - 1] * (ahead - behind), first_coeffs[k - 1] * (up - down)
            slope_x = term_x if slope_x is None else slope_x + term_x
            slope_y = term_y if slope_y is None else slope_y + term_y
            total = total + second_coeffs[k - 1] * ((ahead + behind) + (up + down))
        advect = speed[0] * slope_x + speed[1] * slope_y + speed[2] * slope_z
        return viscosity * total - advect - press, center

    def first_section(b, _):
        i = b * step
        speed = [fields[f, reach + i : reach + i + step] if isinstance(i, int) else fields[f, pl.ds(reach + i, step)] for f in range(3)]
        for c in range(3):
            press = gradient(i, c)
            slope[c, i : i + step] = press
            change, center = tendency(fields, c, i, speed, press)
            mids[c, reach + i : reach + i + step] = center + time_step * change
        return 0

    def second_section(b, c):
        i = b * step
        speed = [mids[f, reach + i : reach + i + step] for f in range(3)]
        change, center = tendency(mids, c, i, speed, slope[c, i : i + step])
        final[c, i : i + step] = 0.5 * ((fields[c, reach + i : reach + i + step] + center) + time_step * change)

    for b in range(half // step):
        first_section(b, 0)
    for c in range(3):
        wrap(mids, c)
    flat = lax.broadcasted_iota(jnp.int32, (SUB, LANES), 0)

    def flip_one(value):
        return jnp.where((flat & 1) == 0, pltpu.roll(value, SUB - 1, 0), pltpu.roll(value, 1, 0))

    matrix = lift_matrix(planes)
    z_coeffs = []
    for m in range(planes):
        column = jnp.zeros((SUB, LANES), jnp.float32)
        for z in range(planes):
            column = jnp.where(flat // 2 == z, float(matrix[z, (z + m) % planes]), column)
        z_coeffs.append(column)

    def lift_z(value):
        total = z_coeffs[0] * value
        for m in range(1, planes):
            total = total + z_coeffs[m] * pltpu.roll(value, (-2 * m) % SUB, 0)
        return total

    pairs = half // 2
    z, y = t // 2, t % 2
    n_z = n_tile // 2

    def flipped(value, bits):
        result, place = 0, 1
        while place < n_z:
            result = result + place * lax.rem(value // place + bits // place, 2)
            place *= 2
        return result

    partner = flipped(z, 1)

    def source_of(level, column, group):
        return (level * 2 + column) * n_grp + group

    def send(origin, source, sem, group, level, column):
        return pltpu.make_async_remote_copy(
            src_ref=origin, dst_ref=landed.at[source], send_sem=sem, recv_sem=recv_two.at[source],
            device_id=(group, level * 2 + column), device_id_type=MESH)

    kin = [g, g + 1 - 2 * lax.rem(g, 2), lax.rem(g + 2, n_grp), n_grp - 1 - g]
    across = (0, 2, 3, 1)
    routes = ((3, 0), (0, 1), (1, 0), (0, 0))

    def hand(bits, other, c):
        return send(pieces.at[c], me, hand_sem.at[bits + 2 * other, c], c, flipped(z, bits), lax.rem(y + other, 2))

    def each_hand(c, act):
        for bits, other in routes:
            if bits or other:
                act(hand(bits, other, c))
            else:
                @pl.when(g != c)
                def _():
                    act(hand(bits, other, c))

    def side(source):
        return send(landed.at[source], source, side_sem.at[source], g, z, 1 - y)

    def onward(source):
        return send(landed.at[source], source, onward_sem.at[source], g, partner, y)

    crossed = (2, 3)

    inner = (z > 0) & (z + 1 < n_z)

    def leap(source):
        return send(landed.at[source], source, leap_sem.at[source], g, flipped(z, 3), y)

    def await_piece(source):
        send(pieces.at[g], source, hand_sem.at[0, 0], g, z, 1 - y).wait_recv()

    def finish(c):
        even = [lift_z(final[c, 2 * i]) for i in range(pairs)]
        odd = [lift_z(final[c, 2 * i + 1]) for i in range(pairs)]
        for odd_tap, even_tap in ((lift_alpha, lift_beta), (lift_gamma, lift_delta)):
            after = even[1:] + [flip_one(even[0])]
            odd = [odd[i] + odd_tap * (even[i] + after[i]) for i in range(pairs)]
            before = [flip_one(odd[-1])] + odd[:-1]
            even = [even[i] + even_tap * (odd[i] + before[i]) for i in range(pairs)]
        for i in range(pairs):
            final[c, i] = even[i] * lift_scale
            final[c, pairs + i] = odd[i] * (1.0 / lift_scale)
        flat_ref = final.at[c].reshape(half * SUB, LANES)
        stacked = []
        for pair in range(2):
            for high in range(2):
                for a in range(2):
                    stacked.append(jnp.concatenate([flat_ref[pl.ds(high * pairs * SUB + 2 * z_at + a, pairs, stride=SUB), :] for z_at in (2 * pair, 2 * pair + 1)], axis=1))
        lines = jnp.dot(jnp.concatenate(stacked, axis=0), band_ref[...], precision=lax.Precision.HIGHEST, preferred_element_type=jnp.float32)
        near, beyond = lines[0:nx], lines[nx : 2 * nx]
        is_near = lax.broadcasted_iota(jnp.int32, (nx, LANES), 1) < CHUNK
        pieces[c, :, 0:LANES] = jnp.where(is_near, near, pltpu.roll(beyond, CHUNK, 1))
        pieces[c, :, LANES : 2 * LANES] = jnp.where(is_near, pltpu.roll(near, CHUNK, 1), beyond)

    for c in (0, 2, 1):
        for b in range(half // step):
            second_section(b, c)
        finish(c)
        each_hand(c, lambda copy: copy.start())
    pieces[3] = pieces[0] * pieces[0] + pieces[1] * pieces[1] + pieces[2] * pieces[2]
    each_hand(3, lambda copy: copy.start())
    rank = lax.broadcasted_iota(jnp.int32, (LANES, LANES), 0)
    n_groups = n_tile
    lane_part = lax.broadcasted_iota(jnp.int32, (nx, LANES), 1) // (CHUNK // 2)

    def select(tile):
        for high in range(2):
            tiles = [landed[tile * n_grp + m, :, high * LANES : (high + 1) * LANES] for m in range(4)]
            for bit in range(2):
                distance = (CHUNK // 2) << bit
                is_low = (lane_part & (1 << bit)) == 0
                turned = list(tiles)
                for m in range(4):
                    if not m & (1 << bit):
                        other = m | (1 << bit)
                        turned[m] = jnp.where(is_low, tiles[m], pltpu.roll(tiles[other], distance, 1))
                        turned[other] = jnp.where(is_low, pltpu.roll(tiles[m], LANES - distance, 1), tiles[other])
                tiles = turned
            for plane in range(planes):
                block = (plane * 2 + high) * n_groups + tile
                value = tiles[plane]
                first = value.astype(jnp.bfloat16).astype(jnp.float32)
                rest = value - first
                second = rest.astype(jnp.bfloat16).astype(jnp.float32)
                stack = jnp.concatenate([first, second, rest - second], axis=0).astype(jnp.bfloat16)
                chosen = jnp.where(rank == spot_ref[pl.ds(block, 1), :], 1.0, 0.0).astype(jnp.bfloat16)
                placed = lax.dot_general(stack, chosen, (((1,), (1,)), ((), ())), preferred_element_type=jnp.float32)
                ordered[plane * 2 + high] = (placed[0:nx] + placed[nx : 2 * nx]) + placed[2 * nx : 3 * nx]
        labels = [group_ref[pl.ds((plane * 2 + high) * n_groups + tile, 1), :] for plane in range(planes) for high in range(2)]
        for q in range(out_ref.shape[1] // LANES):
            total = out_ref[:, q * LANES : (q + 1) * LANES]
            for n, label in enumerate(labels):
                total = jnp.where(label == q, ordered[n], total)
            out_ref[:, q * LANES : (q + 1) * LANES] = total

    landed[me] = pieces[g]

    def sideways(bits, k):
        return bits == 3 or bits == 2 or (bits == 1 and k not in crossed)

    def receive(bits):
        for k in across:
            source = source_of(flipped(z, bits), y, kin[k])
            if bits or k:
                await_piece(source)
            if bits == 3 or bits == 1:
                @pl.when(inner)
                def _():
                    (onward if bits == 3 else leap)(source).start()
            if sideways(bits, k):
                side(source).start()
        if bits == 0:
            for k in across:
                source = source_of(z, 1 - y, kin[k])
                await_piece(source)
                if k in crossed:
                    onward(source).start()

    for peer in peers:
        deal(peer, me).wait_send()

    for bits in (1, 3, 0):
        receive(bits)

    def from_other(bits):
        for k in across:
            await_piece(source_of(flipped(z, bits), 1 - y, kin[k]))

    def pick(bits, other):
        select(flipped(z, bits) * 2 + lax.rem(y + other, 2))

    pick(0, 0)
    pick(0, 1)
    pick(1, 0)
    receive(2)
    pick(3, 0)
    pick(2, 0)
    for bits in (3, 1):
        from_other(bits)
        pick(bits, 1)
    for c in range(n_grp):
        each_hand(c, lambda copy: copy.wait_send())
    for k in across:
        for bits in range(1, n_z):
            source = source_of(flipped(z, bits), y, kin[k])
            if sideways(bits, k):
                side(source).wait_send()
        @pl.when(inner)
        def _():
            onward(source_of(flipped(z, 3), y, kin[k])).wait_send()
            leap(source_of(partner, y, kin[k])).wait_send()

        if k in crossed:
            onward(source_of(z, 1 - y, kin[k])).wait_send()
    from_other(2)
    pick(2, 1)


def chunk_body(flow_state, line_owner, *, n_tile):
    _, planes, rows, ny = flow_state.shape
    n_lines = line_owner.shape[0]
    n_blocks = n_lines // LANES
    nx = rows * n_tile
    half = nx // 2
    n_dev = 4 * n_tile
    cap = 2 * planes * ny // n_tile
    f32 = jnp.float32
    dma = pltpu.SemaphoreType.DMA
    hbm = pl.BlockSpec(memory_space=pltpu.HBM)
    padded = (half + 2 * reach, SUB, LANES)
    record = pl.pallas_call(
        functools.partial(chunk_kernel, n_tile),
        out_shape=jax.ShapeDtypeStruct((nx, cap), f32),
        in_specs=[hbm, hbm], out_specs=pl.BlockSpec(memory_space=pltpu.VMEM),
        scratch_shapes=[
            pltpu.VMEM((planes, rows, ny), f32), pltpu.VMEM((n_blocks, LANES), jnp.int32),
            pltpu.VMEM((n_dev, planes * rows, LANES), f32), pltpu.VMEM((n_dev, planes * rows, LANES), f32),
            pltpu.VMEM((4,) + padded, f32), pltpu.VMEM((3,) + padded, f32),
            pltpu.VMEM((3, half, SUB, LANES), f32), pltpu.VMEM((3, half, SUB, LANES), f32),
            pltpu.VMEM((4, nx, 2 * LANES), f32), pltpu.VMEM((n_dev, nx, 2 * LANES), f32),
            pltpu.VMEM((n_blocks, LANES), jnp.int32), pltpu.VMEM((n_blocks, LANES), jnp.int32),
            pltpu.VMEM((2 * planes, nx, LANES), f32), pltpu.VMEM((2 * LANES, LANES), f32),
            dma, dma, dma((n_dev,)), dma((n_dev,)), dma((n_dev,)), dma((4, 4)), dma((n_dev,)), dma((n_dev,)), dma((n_dev,)),
        ],
        compiler_params=pltpu.CompilerParams(has_side_effects=True, collective_id=0, vmem_limit_bytes=16 * 1024 * 1024), name="record",
    )(pltpu.with_memory_space_constraint(flow_state, pltpu.HBM), pltpu.with_memory_space_constraint(line_owner.reshape(n_blocks, LANES), pltpu.HBM))
    return record[None, None]


def fits_chunks(mesh, planes, rows, ny):
    n_tile = mesh.shape["tile"]
    return 2 * planes == SUB and 2 * rows == SUB and mesh.shape["grp"] == 4 and ny == 4 * n_tile * CHUNK and n_tile == 8


def solution(mesh):
    in_specs = (P("grp", None, "tile", None), P())
    out_specs = P("grp", "tile", None, None)
    n_tile = mesh.shape["tile"]

    def run(flow_state, line_owner):
        _, planes, rows, ny = flow_state.shape
        chosen = chunk_body if fits_chunks(mesh, planes, rows, ny) else tiled_body
        return chosen(flow_state, line_owner, n_tile=n_tile)

    return jax.shard_map(run, mesh=mesh, in_specs=in_specs, out_specs=out_specs, check_vma=False)
```
